256 devices in a mesh: rep: 4 (over y), row: 4 (over z_hi), col: 16 (over z_lo, x, core).
Axes of the slice: x: 4, y: 4, z: 8 (z_hi: 4, z_lo: 2; z = z_hi * 2 + z_lo), core: 2. Of those that a mesh axis runs over, the one named last changes fastest.
Arguments:
- patches: bfloat16 [4096, 588], P(('rep', 'col')), may hold values from -20 to 20
- embed_weight: bfloat16 [588, 6144], P(None, 'row'), may hold values from -1 to 1
- embed_bias: float32 [6144], P('row'), may hold values from -3 to 3
- old_in: bfloat16 [64, 768, 1536], P(('row', 'col')), may hold values from -0.078125 to 0.078125
- old_out: bfloat16 [64, 1536, 768], P(('row', 'col')), may hold values from -0.0546875 to 0.0546875
- restore_id: int32 [1], replicated, may hold values from 0 to 47
- norm_gains: float32 [48, 6144], P(None, 'row'), may hold values from 0.1 to 1.9
- in_biases: float32 [48, 12288], P(None, 'col'), may hold values from -3 to 3
- out_biases: float32 [48, 6144], P(None, 'row'), may hold values from -3 to 3
- final_gain: float32 [6144], P('row'), may hold values from 0.1 to 1.9
- check_weight: bfloat16 [6144, 128], P('row'), may hold values from -0.078125 to 0.078125
Outputs:
- in_weight: bfloat16 [6144, 12288], P('row', 'col')
- out_weight: bfloat16 [12288, 6144], P('col', 'row')
- check_logits: float32 [4096, 128], P(('rep', 'col'))
The draws below stay inside these ranges and needn't reach their ends.
All inputs are finite; a program needn't handle non-finite values.
Results may differ from the reference program's by a relative error of at most 0.0062.
Values may be sent and summed in bfloat16 or wider, within the bound.
A program may use at most 64 MiB of HBM per device.

```python
import math
import jax
import jax.numpy as jnp
from jax import lax

D = 6144
PATCH = 588
LAYERS_ALL = 48
FF = 12288
OLD_GRID = 8
CHECK = 128
TOKENS = 4096


def draw_patches(key, part):
    base_key, scale_key = jax.random.split(key, 2)
    row_scale = jnp.exp(jax.random.uniform(scale_key, (TOKENS, 1), jnp.float32, math.log(0.5), math.log(5.0)))
    noise_part = jax.random.truncated_normal(base_key, -4.0, 4.0, (TOKENS, PATCH), jnp.float32)
    values = row_scale * noise_part
    return values.astype(jnp.bfloat16)


def draw_embed_weight(key, part):
    entry_key, column_key = jax.random.split(key, 2)
    position = jnp.arange(D, dtype=jnp.float32) / D
    trend_part = math.log(3.0) * (position - 0.5)
    jitter = jax.random.uniform(column_key, (D,), jnp.float32, -1.15, 1.15)
    entries = jax.random.truncated_normal(entry_key, -4.0, 4.0, (PATCH, D), jnp.float32)
    column_scale = jnp.exp(trend_part + jitter)
    return (entries * column_scale[None, :] / math.sqrt(PATCH)).astype(jnp.bfloat16)


def block_levels(key, extent, cuts, smallest, largest):
    factor_of, own = 1.0, jax.random.fold_in(key, 6)
    for dim, parts in cuts:
        draws = jnp.exp(jax.random.uniform(jax.random.fold_in(own, dim), (parts,), jnp.float32, smallest / len(cuts), largest / len(cuts)))
        factor_of = factor_of * jnp.repeat(draws, extent[dim] // parts).reshape([-1 if axis == dim else 1 for axis in range(len(extent))])
    return factor_of


def normal_values(rng, extent, deviation, reach, cuts=(), held_as=jnp.bfloat16):
    values = jax.random.normal(rng, extent, jnp.float32) * deviation
    if len(cuts) > 0:
        values = block_levels(rng, extent, cuts, -0.22, 0.18) * values
    return jnp.clip(values, min=-reach, max=reach).astype(held_as)


def setup_inputs(seed: int = 0) -> dict:
    key_of = jax.random.split(jax.random.key(seed), 12)
    return {
        "patches": draw_patches(jax.random.fold_in(key_of[11], 71), 0),
        "embed_weight": draw_embed_weight(jax.random.fold_in(key_of[11], 71), 0),
        "embed_bias": normal_values(key_of[2], (D,), 0.5, 3.0, ((0, 4),), jnp.float32),
        "old_in": normal_values(key_of[3], (OLD_GRID * OLD_GRID, D // OLD_GRID, FF // OLD_GRID), D ** -0.5, 0.078125, ((0, 64),)),
        "old_out": normal_values(key_of[4], (OLD_GRID * OLD_GRID, FF // OLD_GRID, D // OLD_GRID), FF ** -0.5, 0.0546875, ((0, 64),)),
        "restore_id": jax.random.randint(key_of[5], (1,), 0, LAYERS_ALL).astype(jnp.int32),
        "norm_gains": jnp.clip(1.0 + 0.18 * jax.random.normal(key_of[6], (LAYERS_ALL, D), jnp.float32), 0.1, 1.9),
        "in_biases": normal_values(key_of[7], (LAYERS_ALL, FF), 0.5, 3.0, ((1, 16),), jnp.float32),
        "out_biases": normal_values(key_of[8], (LAYERS_ALL, D), 0.5, 3.0, ((1, 4),), jnp.float32),
        "final_gain": jnp.clip(1.0 + 0.18 * jax.random.normal(key_of[9], (D,), jnp.float32), 0.1, 1.9),
        "check_weight": normal_values(key_of[10], (D, CHECK), D ** -0.5, 0.078125, ((0, 4),)),
    }


EPSILON = 1e-06

def assemble_in(old_tiles):
    tile_grid = old_tiles.reshape(OLD_GRID, OLD_GRID, D // OLD_GRID, FF // OLD_GRID)
    return tile_grid.transpose(0, 2, 1, 3).reshape(D, FF)

def assemble_out(old_tiles):
    tile_grid = old_tiles.reshape(OLD_GRID, OLD_GRID, FF // OLD_GRID, D // OLD_GRID)
    return tile_grid.transpose(1, 2, 0, 3).reshape(FF, D)

def pick_rows(restore_id, param_table):
    selector = (jnp.arange(param_table.shape[0], dtype=jnp.int32)[None, :] == restore_id[:, None]).astype(jnp.float32)
    return jnp.dot(selector, param_table, precision=lax.Precision.HIGHEST)[0]

def norm_rows(values, gain_row):
    feature_count = values.shape[1]
    average = lax.optimization_barrier(jnp.sum(values, axis=1, keepdims=True)) / feature_count
    square_mean = lax.optimization_barrier(jnp.sum(values * values, axis=1, keepdims=True)) / feature_count
    inverse_scale = lax.rsqrt(square_mean - average * average + EPSILON)
    return ((values - average) * inverse_scale * gain_row).astype(jnp.bfloat16)

def reference(patches, embed_weight, embed_bias, old_in, old_out, restore_id, norm_gains, in_biases, out_biases, final_gain, check_weight):
    in_weight = assemble_in(old_in)
    out_weight = assemble_out(old_out)
    layer_gain = pick_rows(restore_id, norm_gains)
    layer_in_bias = pick_rows(restore_id, in_biases)
    layer_out_bias = pick_rows(restore_id, out_biases)
    embedded = jnp.dot(patches, embed_weight, preferred_element_type=jnp.float32) + embed_bias
    normed = norm_rows(embedded, layer_gain)
    pre = jnp.dot(normed, in_weight, preferred_element_type=jnp.float32) + layer_in_bias
    hidden = jax.nn.gelu(pre, approximate=False).astype(jnp.bfloat16)
    updated = embedded + jnp.dot(hidden, out_weight, preferred_element_type=jnp.float32) + layer_out_bias
    final_normed = norm_rows(updated, final_gain)
    check_logits = jnp.dot(final_normed, check_weight, preferred_element_type=jnp.float32)
    return (in_weight, out_weight, check_logits)
```

```python
import functools

import jax
import jax.numpy as jnp
from jax import lax
from jax.experimental import pallas as pl
from jax.experimental.pallas import tpu as pltpu
from jax.sharding import PartitionSpec as P

EPSILON = 1e-06
MESH = pl.DeviceIdType.MESH
F32, BF16 = jnp.float32, jnp.bfloat16

REPS, ROWS, COLS = 4, 4, 16
ZS, WS = 8, 8
D, FF, PATCH, CHECK = 6144, 12288, 588, 128
LAYERS = 48
FB = D // ZS
HB = FF // WS
HU = HB // 2
TB = 128
SUB = TB // WS
QUARTER = FB // REPS


def kernel(
    patches, embed_w, embed_b, old_in, old_out, rid, gains, in_b, out_b, final_g, check_w,
    new_in, new_out, logits,
    P_, We, be, IT, OT, gt, ibt, obt, fg, Wc,
    E, st, stall, bsrc, bb, PP, rh, rf, H, Yb, R, F, FR,
    lsem, psend, precv, drecv, dsend, ssend, srecv, fsend, frecv, bsend, brecv,
    rsend, rrecv, asend, arecv, ysend, yrecv, tsend, trecv, gsend, grecv,
):
    y, h, col = lax.axis_index("rep"), lax.axis_index("row"), lax.axis_index("col")
    l, w = col // 8, col % 8
    x, c = w // 2, w % 2
    z = 2 * h + l

    def at(yy, zz, ww):
        return (yy, zz // 2, (zz % 2) * 8 + ww)

    def remote(src, dst, ss, rs, dev):
        return pltpu.make_async_remote_copy(
            src_ref=src, dst_ref=dst, send_sem=ss, recv_sem=rs, device_id=dev, device_id_type=MESH
        )

    def copy_or_send(src, dst, ss, rs, dev, is_self):
        @pl.when(is_self)
        def _():
            pltpu.make_async_copy(src, dst, rs).start()

        @pl.when(jnp.logical_not(is_self))
        def _():
            remote(src, dst, ss, rs, dev).start()

    def send_done(src, dst, ss, dev, is_self):
        @pl.when(jnp.logical_not(is_self))
        def _():
            pltpu.make_async_copy(src, dst, ss).wait()

    half = pl.ds(pl.multiple_of(l * FB, 128), FB)
    loads = [
        pltpu.make_async_copy(src, dst, lsem.at[n])
        for n, (src, dst) in enumerate([
            (embed_w.at[:, half], We),
            (embed_b.at[:, half], be),
            (gains.at[:, half], gt),
            (in_b, ibt),
            (old_in.at[0], IT),
            (out_b.at[:, half], obt),
            (final_g.at[:, half], fg),
            (check_w.at[pl.ds(pl.multiple_of(l * FB, 128), FB), :], Wc),
            (old_out.at[0], OT),
        ])
    ]
    own = pltpu.make_async_copy(patches, P_.at[:, l, pl.ds(w * SUB, SUB), :], lsem.at[9])
    own.start()
    for load in loads:
        load.start()

    barrier = pltpu.get_barrier_semaphore()
    peers = [at(y, 2 * h + (l + a) % 2, (w + b) % 8) for a in range(2) for b in range(8) if a or b]
    peers += [at(y, (z + 2 * k) % 8, w) for k in range(1, 4)]
    peers += [at(y, 2 * ((h + k) % 4) + (1 - l), w) for k in range(1, 4)]
    peers += [((y + 1) % REPS, h, col), ((y + 3) % REPS, h, col)]
    for peer in peers:
        pl.semaphore_signal(barrier, inc=1, device_id=peer, device_id_type=MESH)
    pl.semaphore_wait(barrier, len(peers))

    own.wait()
    place = P_.at[:, l, pl.ds(w * SUB, SUB), :]
    patch_sends = []
    for k in range(1, 8):
        dev = at(y, 2 * h + (l + k // 4) % 2, ((x + k % 4) % 4) * 2 + c)
        send = remote(place, place, psend.at[k], precv.at[k], dev)
        send.start()
        patch_sends.append(send)
    partner = at(y, z, 2 * x + 1 - c)

    loads[3].wait()
    bsrc[...] = jnp.broadcast_to(ibt[pl.ds(rid[0], 1), :], bsrc.shape)
    bias_to = 4 * l + x
    for a in range(2):
        copy_or_send(
            bsrc, bb.at[c], bsend.at[a], brecv.at[c], at(y, 2 * h + a, bias_to),
            jnp.logical_and(l == a, w == bias_to),
        )

    for k in range(8):
        ls, xs = (l + k // 4) % 2, (x + 4 - k % 4) % 4
        piece = P_.at[:, ls, pl.ds((2 * xs + c) * SUB, SUB), :]
        if k > 0:
            remote(piece, piece, psend.at[k], precv.at[k], partner).wait_recv()
        send = remote(piece, piece, dsend.at[k], drecv.at[k], partner)
        send.start()
        patch_sends.append(send)
    for k in range(8):
        ls, xs = (l + k // 4) % 2, (x + 4 - k % 4) % 4
        piece = P_.at[:, ls, pl.ds((2 * xs + 1 - c) * SUB, SUB), :]
        remote(piece, piece, dsend.at[k], drecv.at[k], partner).wait_recv()

    loads[4].wait()
    loads[8].wait()
    quarter = pl.ds(pl.multiple_of(y * QUARTER, 64), QUARTER)
    to_l, to_x = x // 2, 2 * (x % 2) + c
    tile_moves = []
    for u in range(2):
        is_self = jnp.logical_and(jnp.logical_and(to_l == l, to_x == x), c == u)
        dev = at(y, 2 * h + to_l, 2 * to_x + u)
        tile_moves.append((
            IT.at[quarter, pl.ds(u * HU, HU)], new_in.at[l, quarter, :],
            tsend.at[0, u], trecv.at[0, l], dev, is_self,
        ))
        tile_moves.append((
            OT.at[pl.ds(pl.multiple_of(u * HU + y * QUARTER, 64), QUARTER), :], new_out.at[quarter, half],
            tsend.at[1, u], trecv.at[1, l], dev, is_self,
        ))
    for move in tile_moves:
        copy_or_send(*move)

    for n in (0, 1, 2):
        loads[n].wait()

    def lane_sum(v):
        return functools.reduce(jnp.add, [v[:, 128 * k:128 * (k + 1)] for k in range(FB // 128)])

    def embed(t, _):
        e = jnp.dot(P_[t // 2, t % 2], We[...], preferred_element_type=F32) + be[...]
        E[t] = e
        st[0, pl.ds(t, 1), :] = jnp.sum(lane_sum(e).T, axis=0, keepdims=True)
        st[1, pl.ds(t, 1), :] = jnp.sum(lane_sum(e * e).T, axis=0, keepdims=True)
        return 0

    lax.fori_loop(0, ZS, embed, 0)

    stat_sends = []
    for k in range(1, 8):
        send = remote(st, stall.at[k], ssend.at[k], srecv.at[k], at(y, (z + k) % 8, w))
        send.start()
        stat_sends.append(send)
    for send in stat_sends:
        send.wait_recv()
    total = st[...]
    for k in range(1, 8):
        total = total + stall[k]
    mean = total[0] / D
    scale = lax.rsqrt(total[1] / D - mean * mean + EPSILON)
    stall[0, 0] = mean
    stall[0, 1] = scale
    gain = gt[pl.ds(rid[0], 1), :]

    def column(row):
        return jnp.broadcast_to(row, (128, 128)).T

    def wide(v):
        return jnp.concatenate([v] * (FB // 128), axis=1)

    def first_product(t):
        m = wide(column(stall[0, 0, pl.ds(t, 1), :]))
        r = wide(column(stall[0, 1, pl.ds(t, 1), :]))
        n = ((E[t] - m) * r * gain).astype(BF16)
        PP[t] = jnp.dot(n, IT[...], preferred_element_type=F32).astype(BF16)

    def towards(d, k):
        return (z + k) % 8 if d == 0 else (z + 8 - k) % 8

    def rows_of(d):
        return pl.ds(d * (TB // 2), TB // 2)

    def lanes_of(u):
        return pl.ds(u * HU, HU)

    def reduce_copy(d, s, u):
        t = towards(d, 5 - s)
        if s == 1:
            src, dst = PP.at[t, rows_of(d), lanes_of(u)], rh.at[d, :, lanes_of(u)]
        else:
            src, dst = PP.at[t, :, lanes_of(u)], rf.at[d, s - 2, :, lanes_of(u)]
        return remote(src, dst, rsend.at[d, s - 1, u], rrecv.at[d, s - 1, u], at(y, towards(d, 1), w))

    first_product((z + 4) % 8)
    for u in range(2):
        for d in range(2):
            reduce_copy(d, 1, u).start()

    def others(k, _):
        @pl.when(k != 4)
        def _():
            first_product((z + k) % 8)
        return 0

    lax.fori_loop(0, ZS, others, 0)

    for s in range(2, 5):
        for u in range(2):
            for d in range(2):
                reduce_copy(d, s - 1, u).wait_recv()
                t = towards(d, 5 - s)
                if s == 2:
                    to, add = (t, rows_of(d), lanes_of(u)), rh[d, :, lanes_of(u)]
                else:
                    to, add = (t, slice(None), lanes_of(u)), rf[d, s - 3, :, lanes_of(u)]
                PP[to] = (PP[to].astype(F32) + add.astype(F32)).astype(BF16)
                reduce_copy(d, s, u).start()

    def spread_copy(d, a, stage):
        owner = y if stage == 0 else (y + 3 if d == 0 else y + 1) % REPS
        if stage == 0:
            rows = pl.ds(pl.multiple_of(owner * QUARTER, 64), QUARTER)
        else:
            rows = pl.ds(pl.multiple_of(owner * QUARTER + d * (QUARTER // 2), 32), QUARTER // 2)
        ref = new_in.at[:, rows, :] if a == 0 else new_out.at[rows, :]
        to = (y + 1 if d == 0 else y + 3) % REPS
        return remote(ref, ref, gsend.at[d, a, stage], grecv.at[d, a, stage], (to, h, col))

    for a in range(2):
        for s in range(2):
            ref = new_in.at[s, quarter, :] if a == 0 else new_out.at[quarter, pl.ds(s * FB, FB)]
            pltpu.make_async_copy(ref, ref, trecv.at[a, s]).wait()
        for d in range(2):
            spread_copy(d, a, 0).start()

    for u in range(2):
        ref = bb.at[u]
        pltpu.make_async_copy(ref, ref, brecv.at[u]).wait()

    def gather_copy(d, s, u):
        t = towards(1 - d, s - 1)
        ref = H.at[t, :, lanes_of(u)] if s < 4 else H.at[t, rows_of(d), lanes_of(u)]
        return remote(ref, ref, asend.at[d, s - 1, u], arecv.at[d, s - 1, u], at(y, towards(d, 1), w))

    for u in range(2):
        for d in range(2):
            reduce_copy(d, 4, u).wait_recv()
        v = PP[z, :, lanes_of(u)].astype(F32) + bb[u, 0:1, :]
        v = v + rf[0, 2, :, lanes_of(u)].astype(F32) + rf[1, 2, :, lanes_of(u)].astype(F32)
        H[z, :, lanes_of(u)] = (0.5 * v * (1.0 + lax.erf(v * 0.7071067811865476))).astype(BF16)
        for d in range(2):
            gather_copy(d, 1, u).start()

    def second_product(t):
        Yb[t] = jnp.dot(H[t], OT[...], preferred_element_type=F32).astype(BF16)
        for k in range(1, 8):
            to = (w + k) % 8
            remote(
                Yb.at[t, pl.ds(pl.multiple_of(to * SUB, SUB), SUB), :], R.at[k - 1, t], ysend, yrecv, at(y, z, to)
            ).start()

    second_product(z)
    for s in range(2, 5):
        for u in range(2):
            for d in range(2):
                gather_copy(d, s - 1, u).wait_recv()
                gather_copy(d, s, u).start()

        def pair(d, _):
            second_product((z + 8 + (2 * d - 1) * (s - 1)) % 8)
            return 0

        lax.fori_loop(0, 2, pair, 0)
        if s == 3:
            for a in range(2):
                for d in range(2):
                    spread_copy(d, a, 0).wait_recv()
                    spread_copy(d, a, 1).start()
    for u in range(2):
        for d in range(2):
            gather_copy(d, 4, u).wait_recv()
    second_product((z + 4) % 8)

    for n in (5, 6, 7):
        loads[n].wait()
    pltpu.make_async_copy(R, R, yrecv).wait()
    mine = pl.ds(pl.multiple_of(w * SUB, SUB), SUB)
    out_bias = obt[pl.ds(rid[0], 1), :]
    weights = Wc[...]
    gain_w = jnp.sum(jnp.transpose(fg[...] * jnp.ones((128, 1), F32))[:, 0:1] * weights.astype(F32), axis=0, keepdims=True)
    lane = lax.broadcasted_iota(jnp.int32, (64, 128), 1)
    row = lax.broadcasted_iota(jnp.int32, (8, 128), 0)
    columns = []
    for a in range(2):
        parts = []
        for b in range(4):
            t = 2 * b + a
            u = E[t, mine, :] + out_bias + Yb[t, mine, :].astype(F32)
            for k in range(7):
                u = u + R[k, t].astype(F32)
            parts.append(u)
        u = jnp.concatenate(parts, axis=0)
        v = u * fg[...]
        hi = v.astype(BF16)
        lo = (v - hi.astype(F32)).astype(BF16)
        F[a, 0:64, :] = jnp.dot(hi, weights, preferred_element_type=F32) + jnp.dot(lo, weights, preferred_element_type=F32)
        s1 = jnp.sum(u, axis=1, keepdims=True)
        s2 = jnp.sum(u * u, axis=1, keepdims=True)
        columns.append(jnp.where(lane == 0, s1, jnp.where(lane == 1, s2, 0.0)))
    turned = jnp.concatenate(columns, axis=0).T[0:8, :]
    turned = jnp.where(row == 2, gain_w, turned)
    F[0, 64:72, :] = turned
    F[1, 64:72, :] = turned
    last_sends = []
    for k in range(1, 8):
        send = remote(F.at[(z + k) % 2], FR.at[k - 1], fsend.at[k], frecv.at[k], at(y, (z + k) % 8, w))
        send.start()
        last_sends.append(send)
    for send in last_sends:
        send.wait_recv()
    both = F[l]
    for k in range(7):
        both = both + FR[k]
    back = jnp.concatenate([both[64:72], jnp.zeros((120, 128), F32)], axis=0).T
    E[0, :, 0:128] = back
    own_stats = E[0, pl.ds(pl.multiple_of(l * 64, 64), 64), 0:128]
    mean2 = own_stats[:, 0:1] / D
    scale2 = lax.rsqrt(own_stats[:, 1:2] / D - mean2 * mean2 + EPSILON)
    logits[...] = (both[0:64] - mean2 * both[66:67]) * scale2

    for a in range(2):
        for d in range(2):
            spread_copy(d, a, 1).wait_recv()
            spread_copy(d, a, 0).wait_send()
            spread_copy(d, a, 1).wait_send()
    for src, dst, ss, rs, dev, is_self in tile_moves:
        send_done(src, dst, ss, dev, is_self)
    for a in range(2):
        send_done(bsrc, bb.at[c], bsend.at[a], None, jnp.logical_and(l == a, w == bias_to))
    for send in patch_sends + stat_sends + last_sends:
        send.wait_send()
    for s in range(1, 5):
        for u in range(2):
            for d in range(2):
                reduce_copy(d, s, u).wait_send()
                gather_copy(d, s, u).wait_send()
    pltpu.make_async_copy(R, R, ysend).wait()


def on_device(
    patches, embed_weight, embed_bias, old_in, old_out, restore_id, norm_gains, in_biases, out_biases,
    final_gain, check_weight,
):
    anywhere = pl.BlockSpec(memory_space=pl.ANY)
    vmem = pl.BlockSpec(memory_space=pltpu.VMEM)
    dma = pltpu.SemaphoreType.DMA
    new_in, new_out, logits = pl.pallas_call(
        kernel,
        name="relayout_forward",
        out_shape=(
            jax.ShapeDtypeStruct((2, FB, HU), BF16),
            jax.ShapeDtypeStruct((HU, 2 * FB), BF16),
            jax.ShapeDtypeStruct((64, CHECK), F32),
        ),
        in_specs=[anywhere] * 5 + [pl.BlockSpec(memory_space=pltpu.SMEM)] + [anywhere] * 5,
        out_specs=(anywhere, anywhere, vmem),
        scratch_shapes=[
            pltpu.VMEM((4, 2, TB, PATCH), BF16),
            pltpu.VMEM((PATCH, FB), BF16),
            pltpu.VMEM((1, FB), F32),
            pltpu.VMEM((FB, HB), BF16),
            pltpu.VMEM((HB, FB), BF16),
            pltpu.VMEM((LAYERS, FB), F32),
            pltpu.VMEM((LAYERS, HU), F32),
            pltpu.VMEM((LAYERS, FB), F32),
            pltpu.VMEM((1, FB), F32),
            pltpu.VMEM((FB, CHECK), BF16),
            pltpu.VMEM((ZS, TB, FB), F32),
            pltpu.VMEM((2, 8, 128), F32),
            pltpu.VMEM((8, 2, 8, 128), F32),
            pltpu.VMEM((8, HU), F32),
            pltpu.VMEM((2, 8, HU), F32),
            pltpu.VMEM((ZS, TB, HB), BF16),
            pltpu.VMEM((2, TB // 2, HB), BF16),
            pltpu.VMEM((2, 3, TB, HB), BF16),
            pltpu.VMEM((ZS, TB, HB), BF16),
            pltpu.VMEM((ZS, TB, FB), BF16),
            pltpu.VMEM((7, ZS, SUB, FB), BF16),
            pltpu.VMEM((2, 72, 128), F32),
            pltpu.VMEM((7, 72, 128), F32),
            dma((10,)), dma((8,)), dma((8,)), dma((8,)), dma((8,)), dma((8,)), dma((8,)), dma((8,)), dma((8,)),
            dma((2,)), dma((2,)),
            dma((2, 4, 2)), dma((2, 4, 2)), dma((2, 4, 2)), dma((2, 4, 2)),
            dma, dma,
            dma((2, 2)), dma((2, 2)), dma((2, 2, 2)), dma((2, 2, 2)),
        ],
        compiler_params=pltpu.CompilerParams(
            collective_id=0, has_side_effects=True, vmem_limit_bytes=60 * 2**20
        ),
    )(
        patches.reshape(4, SUB, PATCH), embed_weight, embed_bias.reshape(1, -1), old_in, old_out, restore_id,
        norm_gains, in_biases, out_biases, final_gain.reshape(1, -1), check_weight,
    )
    return new_in.reshape(2 * FB, HU), new_out, logits


def solution(mesh):
    placed = (
        P(("rep", "col"), None),
        P(None, "row"),
        P("row"),
        P(("row", "col"), None, None),
        P(("row", "col"), None, None),
        P(),
        P(None, "row"),
        P(None, "col"),
        P(None, "row"),
        P("row"),
        P("row", None),
    )
    return jax.shard_map(
        on_device,
        mesh=mesh,
        in_specs=placed,
        out_specs=(P("row", "col"), P("col", "row"), P(("rep", "col"), None)),
        check_vma=False,
    )
```

```python
import functools

import jax
import jax.numpy as jnp
from jax import lax
from jax.experimental import pallas as pl
from jax.experimental.pallas import tpu as pltpu
from jax.sharding import PartitionSpec as P

EPSILON = 1e-06
MESH = pl.DeviceIdType.MESH
F32, BF16 = jnp.float32, jnp.bfloat16

REPS, ROWS, COLS = 4, 4, 16
ZS, WS = 8, 8
D, FF, PATCH, CHECK = 6144, 12288, 588, 128
LAYERS = 48
FB = D // ZS
HB = FF // WS
HU = HB // 2
TB = 128
SUB = TB // WS
QUARTER = FB // REPS


def kernel(
    patches, embed_w, embed_b, old_in, old_out, rid, gains, in_b, out_b, final_g, check_w,
    new_in, new_out, logits,
    P_, We, be, IT, OT, gt, ibt, obt, fg, Wc,
    E, st, stall, q, qall, bsrc, bb, PP, rh, rf, C, H, Yb, R, LB, LR, T, TR, XI, XO,
    lsem, psend, precv, dsend, drecv, ssend, srecv, qsend, qrecv, fsend, frecv, bsend, brecv,
    rsend, rrecv, asend, arecv, ysend, yrecv, xsend, xrecv, zsend, zrecv, gsend, grecv,
):
    y, h, col = lax.axis_index("rep"), lax.axis_index("row"), lax.axis_index("col")
    l, w = col // 8, col % 8
    x, c = w // 2, w % 2
    z = 2 * h + l

    def at(yy, zz, ww):
        return (yy, zz // 2, (zz % 2) * 8 + ww)

    def remote(src, dst, ss, rs, dev):
        return pltpu.make_async_remote_copy(
            src_ref=src, dst_ref=dst, send_sem=ss, recv_sem=rs, device_id=dev, device_id_type=MESH
        )

    def landed(ref, sem):
        pltpu.make_async_copy(ref, ref, sem).wait()

    half = pl.ds(pl.multiple_of(l * FB, 128), FB)
    loads = [
        pltpu.make_async_copy(src, dst, lsem.at[n])
        for n, (src, dst) in enumerate([
            (embed_w.at[:, half], We),
            (embed_b, be),
            (gains.at[:, half], gt),
            (in_b, ibt),
            (old_in.at[0], IT),
            (out_b.at[:, half], obt),
            (final_g, fg),
            (check_w.at[pl.ds(pl.multiple_of(l * FB, 128), FB), :], Wc),
            (old_out.at[0], OT),
        ])
    ]
    own = pltpu.make_async_copy(patches, P_.at[:, l, pl.ds(w * SUB, SUB), :], lsem.at[9])
    own.start()
    for load in loads:
        load.start()

    barrier = pltpu.get_barrier_semaphore()
    peers = [at(y, 2 * h + (l + a) % 2, (w + b) % 8) for a in range(2) for b in range(8) if a or b]
    peers += [at(y, (z + 2 * k) % 8, w) for k in range(1, 4)]
    peers += [at(y, 2 * ((h + k) % 4) + (1 - l), w) for k in range(1, 4)]
    peers += [((y + 1) % REPS, h, col), ((y + 3) % REPS, h, col)]
    for peer in peers:
        pl.semaphore_signal(barrier, inc=1, device_id=peer, device_id_type=MESH)
    own.wait()
    pl.semaphore_wait(barrier, len(peers))

    partner = at(y, z, 2 * x + 1 - c)

    def wave(v):
        return (h + (2, 1, 3, 0)[v]) % 4

    def patch_copy(v, k):
        place = P_.at[wave(v), l, pl.ds(w * SUB, SUB), :]
        dev = at(y, 2 * h + (l + k // 4) % 2, ((x + k % 4) % 4) * 2 + c)
        return remote(place, place, psend.at[v, k], precv.at[v, k], dev)

    def partner_copy(v, k, core):
        ls, xs = (l + k // 4) % 2, (x + 4 - k % 4) % 4
        piece = P_.at[wave(v), ls, pl.ds((2 * xs + core) * SUB, SUB), :]
        return remote(piece, piece, dsend.at[v, k], drecv.at[v, k], partner)

    def arrived(v, k):
        ls, xs = (l + k // 4) % 2, (x + 4 - k % 4) % 4
        landed(P_.at[wave(v), ls, pl.ds((2 * xs + c) * SUB, SUB), :], precv.at[v, k])

    for v in range(4):
        for k in range(1, 8):
            patch_copy(v, k).start()
        partner_copy(v, 0, c).start()

    loads[3].wait()
    bsrc[...] = jnp.broadcast_to(ibt[pl.ds(rid[0], 1), :], bsrc.shape)
    bias_to = 4 * l + x

    def bias_copies(act):
        for a in range(2):
            is_self = jnp.logical_and(l == a, w == bias_to)

            @pl.when(is_self)
            def _():
                if act == "start":
                    pltpu.make_async_copy(bsrc, bb.at[c], brecv.at[c]).start()

            @pl.when(jnp.logical_not(is_self))
            def _():
                copy = remote(bsrc, bb.at[c], bsend.at[a], brecv.at[c], at(y, 2 * h + a, bias_to))
                copy.start() if act == "start" else copy.wait_send()

    bias_copies("start")

    def receive(v, first, last):
        for k in range(first, last):
            if k > 0:
                arrived(v, k)
                partner_copy(v, k, c).start()
        for k in range(first, last):
            partner_copy(v, k, 1 - c).wait_recv()

    for n in (0, 1, 2, 4):
        loads[n].wait()
    gain = gt[pl.ds(rid[0], 1), :]

    def my_half(ref):
        v = ref[...].reshape(1, 2 * FB)
        return jnp.where(l == 0, v[:, :FB], v[:, FB:])

    embed_bias = my_half(be)
    lane = lax.broadcasted_iota(jnp.int32, (TB, 128), 1)

    def first_product(k):
        t = (z + k) % 8
        e = jnp.dot(P_[t // 2, t % 2], We[...], preferred_element_type=F32) + embed_bias
        E[t] = e
        m = jnp.sum(e, axis=1, keepdims=True) / FB
        s2 = jnp.sum(e * e, axis=1, keepdims=True)
        n = ((e - m) * gain).astype(BF16)
        PP[t] = jnp.dot(n, IT[...], preferred_element_type=F32).astype(BF16)
        st[t] = jnp.where(lane == 0, m, jnp.where(lane == 1, s2, 0.0)).T[0:8, :]

    def stat_copy(k):
        t = (z + k) % 8
        return remote(st.at[t], stall.at[k], ssend.at[k], srecv.at[k], at(y, t, w))

    def towards(d, k):
        return (z + k) % 8 if d == 0 else (z + 8 - k) % 8

    def rows_of(d):
        return pl.ds(d * (TB // 2), TB // 2)

    def lanes_of(u):
        return pl.ds(u * HU, HU)

    def reduce_copy(d, s, u):
        t = towards(d, 5 - s)
        if s == 1:
            src, dst = PP.at[t, rows_of(d), lanes_of(u)], rh.at[d, :, lanes_of(u)]
        else:
            src, dst = PP.at[t, :, lanes_of(u)], rf.at[d, s - 2, :, lanes_of(u)]
        return remote(src, dst, rsend.at[d, s - 1, u], rrecv.at[d, s - 1, u], at(y, towards(d, 1), w))

    def reduce_step(s):
        for u in range(2):
            for d in range(2):
                reduce_copy(d, s - 1, u).wait_recv()
                t = towards(d, 5 - s)
                if s == 2:
                    to, add = (t, rows_of(d), lanes_of(u)), rh[d, :, lanes_of(u)]
                else:
                    to, add = (t, slice(None), lanes_of(u)), rf[d, s - 3, :, lanes_of(u)]
                PP[to] = (PP[to].astype(F32) + add.astype(F32)).astype(BF16)
                reduce_copy(d, s, u).start()

    def two_products(low, high):
        def one(n, _):
            first_product(low + n * (high - low))
            return 0

        lax.fori_loop(0, 2, one, 0)

    receive(0, 0, 4)
    first_product(4)
    for u in range(2):
        for d in range(2):
            reduce_copy(d, 1, u).start()

    loads[8].wait()
    quarter = pl.ds(pl.multiple_of(y * QUARTER, 64), QUARTER)
    to_l, to_x = x // 2, 2 * (x % 2) + c

    def tile_copies(act):
        for a in range(2):
            for u in range(2):
                rows = pl.ds(pl.multiple_of(u * HU + y * QUARTER, 64), QUARTER)
                src = IT.at[quarter, lanes_of(u)] if a == 0 else OT.at[rows, :]
                is_self = jnp.logical_and(to_x == x, c == u)
                dev = at(y, z, 2 * to_x + u)
                for stays in (True, False):
                    if stays:
                        dst, n = (new_in.at[l, quarter, :] if a == 0 else new_out.at[quarter, half]), 0
                    else:
                        dst, n = (XI if a == 0 else XO), 1
                    here = (to_l == l) if stays else (to_l != l)

                    @pl.when(jnp.logical_and(here, is_self))
                    def _():
                        if act == "start":
                            pltpu.make_async_copy(src, dst, xrecv.at[a, n]).start()

                    @pl.when(jnp.logical_and(here, jnp.logical_not(is_self)))
                    def _():
                        copy = remote(src, dst, xsend.at[a, u], xrecv.at[a, n], dev)
                        copy.start() if act == "start" else copy.wait_send()

    tile_copies("start")

    receive(0, 4, 8)
    for v in (1, 2):
        receive(v, 0, 8)
    two_products(3, 5)
    reduce_step(2)
    two_products(2, 6)
    receive(3, 0, 8)
    reduce_step(3)
    two_products(1, 7)

    def cross_copy(a):
        dst = new_in.at[l, quarter, :] if a == 0 else new_out.at[quarter, half]
        return remote((XI, XO)[a], dst, zsend.at[a], zrecv.at[a], at(y, 2 * h + 1 - l, w))

    def spread_copy(d, a, stage):
        owner = y if stage == 0 else (y + 3 if d == 0 else y + 1) % REPS
        if stage == 0:
            rows = pl.ds(pl.multiple_of(owner * QUARTER, 64), QUARTER)
        else:
            rows = pl.ds(pl.multiple_of(owner * QUARTER + d * (QUARTER // 2), 32), QUARTER // 2)
        ref = new_in.at[:, rows, :] if a == 0 else new_out.at[rows, :]
        to = (y + 1 if d == 0 else y + 3) % REPS
        return remote(ref, ref, gsend.at[d, a, stage], grecv.at[d, a, stage], (to, h, col))

    def cross(a):
        landed((XI, XO)[a], xrecv.at[a, 1])
        cross_copy(a).start()

    def spread(a):
        landed(new_in.at[l, quarter, :] if a == 0 else new_out.at[quarter, half], xrecv.at[a, 0])
        cross_copy(a).wait_recv()
        for d in range(2):
            spread_copy(d, a, 0).start()

    def spread_on(a):
        for d in range(2):
            spread_copy(d, a, 0).wait_recv()
            spread_copy(d, a, 1).start()

    cross(0)
    reduce_step(4)
    cross(1)
    first_product(0)
    for k in range(1, 8):
        stat_copy(k).start()
    gains16 = jnp.broadcast_to(gain, (16, FB))
    gains_hi = gains16.astype(BF16)
    gains_lo = (gains16 - gains_hi.astype(F32)).astype(BF16)
    product = jnp.dot(gains_hi, IT[...], preferred_element_type=F32)
    product = product + jnp.dot(gains_lo, IT[...], preferred_element_type=F32)
    q[...] = product[0:1, :]

    def q_copy(k):
        return remote(q, qall.at[k], qsend.at[k], qrecv.at[k], at(y, (z + k) % 8, w))

    for k in range(1, 8):
        q_copy(k).start()
    for k in range(1, 8):
        stat_copy(k).wait_recv()
        q_copy(k).wait_recv()

    def columns_of(tiles):
        mean = functools.reduce(jnp.add, [t[0:1] for t in tiles]) / ZS
        square = functools.reduce(jnp.add, [t[1:2] for t in tiles]) / D
        scale = lax.rsqrt(square - mean * mean + EPSILON)
        rows = [t[0:1] - mean for t in tiles] + [scale, jnp.zeros((128 - ZS - 1, 128), F32)]
        return jnp.concatenate(rows, axis=0).T

    cols = columns_of([st[z]] + [stall[k] for k in range(1, 8)])
    for u in range(2):
        lanes = slice(u * HU, (u + 1) * HU)
        v = PP[z, :, lanes_of(u)].astype(F32) + cols[:, 0:1] * q[:, lanes]
        for k in range(1, 8):
            v = v + cols[:, k:k + 1] * qall[k, :, lanes]
        C[:, lanes] = v
        landed(bb.at[u], brecv.at[u])

    def gather_copy(d, s, u):
        t = towards(1 - d, s - 1)
        ref = H.at[t, :, lanes_of(u)] if s < 4 else H.at[t, rows_of(d), lanes_of(u)]
        return remote(ref, ref, asend.at[d, s - 1, u], arecv.at[d, s - 1, u], at(y, towards(d, 1), w))

    for u in range(2):
        lanes = slice(u * HU, (u + 1) * HU)
        for d in range(2):
            reduce_copy(d, 4, u).wait_recv()
        v = C[:, lanes] + rf[0, 2, :, lanes].astype(F32) + rf[1, 2, :, lanes].astype(F32)
        v = v * cols[:, ZS:ZS + 1] + bb[u, 0:1, :]
        H[z, :, lanes_of(u)] = (0.5 * v * (1.0 + lax.erf(v * 0.7071067811865476))).astype(BF16)
        for d in range(2):
            gather_copy(d, 1, u).start()

    def second_product(t):
        Yb[t] = jnp.dot(H[t], OT[...], preferred_element_type=F32).astype(BF16)
        for k in range(1, 8):
            to = (w + k) % 8
            remote(
                Yb.at[t, pl.ds(pl.multiple_of(to * SUB, SUB), SUB), :], R.at[k - 1, t], ysend, yrecv, at(y, z, to)
            ).start()

    spread(0)
    second_product(z)
    for s in range(2, 5):
        for u in range(2):
            for d in range(2):
                gather_copy(d, s - 1, u).wait_recv()
                gather_copy(d, s, u).start()

        def pair(d, _):
            second_product((z + 8 + (2 * d - 1) * (s - 1)) % 8)
            return 0

        lax.fori_loop(0, 2, pair, 0)
        if s == 2:
            spread(1)
        if s == 3:
            spread_on(0)
        if s == 4:
            spread_on(1)

    for n in (5, 6, 7):
        loads[n].wait()
    final_gain = my_half(fg)
    out_bias = obt[pl.ds(rid[0], 1), :]
    weights = Wc[...]
    gain_w = jnp.sum(
        jnp.broadcast_to(final_gain, (128, FB)).T[:, 0:1] * weights.astype(F32), axis=0, keepdims=True
    )
    for u in range(2):
        for d in range(2):
            gather_copy(d, 4, u).wait_recv()
    second_product((z + 4) % 8)

    landed(R, yrecv)
    mine = pl.ds(pl.multiple_of(w * SUB, SUB), SUB)
    row = lax.broadcasted_iota(jnp.int32, (8, 128), 0)
    columns = []
    for a in range(2):
        parts = []
        for b in range(4):
            t = 2 * b + a
            u = E[t, mine, :] + out_bias + Yb[t, mine, :].astype(F32)
            for k in range(7):
                u = u + R[k, t].astype(F32)
            parts.append(u)
        u = jnp.concatenate(parts, axis=0)
        m = jnp.sum(u, axis=1, keepdims=True) / FB
        s2 = jnp.sum(u * u, axis=1, keepdims=True)
        v = (u - m) * final_gain
        hi = v.astype(BF16)
        lo = (v - hi.astype(F32)).astype(BF16)
        part = jnp.dot(hi, weights, preferred_element_type=F32) + jnp.dot(lo, weights, preferred_element_type=F32)
        LB[a] = part.astype(BF16)
        columns.append(jnp.where(lane[0:64] == 0, m, jnp.where(lane[0:64] == 1, s2, 0.0)))
    turned = jnp.concatenate(columns, axis=0).T[0:8, :]
    T[...] = jnp.where(row == 2, gain_w, turned)

    def last_copies(k):
        dev = at(y, (z + k) % 8, w)
        return (
            remote(LB.at[(z + k) % 2], LR.at[k - 1], fsend.at[0, k], frecv.at[0, k], dev),
            remote(T, TR.at[k - 1], fsend.at[1, k], frecv.at[1, k], dev),
        )

    for k in range(1, 8):
        for copy in last_copies(k):
            copy.start()
    for k in range(1, 8):
        for copy in last_copies(k):
            copy.wait_recv()
    tiles = [T[...]] + [TR[k] for k in range(7)]
    E[0, :, 0:128] = columns_of(tiles)
    cols = E[0, pl.ds(pl.multiple_of(l * 64, 64), 64), 0:128]
    v = LB[l].astype(F32) + cols[:, 0:1] * tiles[0][2:3]
    for k in range(7):
        v = v + LR[k].astype(F32) + cols[:, k + 1:k + 2] * tiles[k + 1][2:3]
    logits[...] = v * cols[:, ZS:ZS + 1]

    for a in range(2):
        cross_copy(a).wait_send()
        for d in range(2):
            spread_copy(d, a, 1).wait_recv()
            spread_copy(d, a, 0).wait_send()
            spread_copy(d, a, 1).wait_send()
    tile_copies("wait")
    bias_copies("wait")
    for v in range(4):
        for k in range(8):
            if k > 0:
                patch_copy(v, k).wait_send()
            partner_copy(v, k, c).wait_send()
    for k in range(1, 8):
        stat_copy(k).wait_send()
        q_copy(k).wait_send()
        for copy in last_copies(k):
            copy.wait_send()
    for s in range(1, 5):
        for u in range(2):
            for d in range(2):
                reduce_copy(d, s, u).wait_send()
                gather_copy(d, s, u).wait_send()
    landed(R, ysend)


def on_device(
    patches, embed_weight, embed_bias, old_in, old_out, restore_id, norm_gains, in_biases, out_biases,
    final_gain, check_weight,
):
    def pinned(a):
        return pltpu.with_memory_space_constraint(a, pltpu.HBM)

    hbm = pl.BlockSpec(memory_space=pltpu.HBM)
    vmem = pl.BlockSpec(memory_space=pltpu.VMEM)
    dma = pltpu.SemaphoreType.DMA
    new_in, new_out, logits = pl.pallas_call(
        kernel,
        name="relayout_forward",
        out_shape=(
            jax.ShapeDtypeStruct((2, FB, HU), BF16),
            jax.ShapeDtypeStruct((HU, 2 * FB), BF16),
            jax.ShapeDtypeStruct((64, CHECK), F32),
        ),
        in_specs=[hbm] * 5 + [pl.BlockSpec(memory_space=pltpu.SMEM)] + [hbm] * 5,
        out_specs=(vmem, vmem, vmem),
        scratch_shapes=[
            pltpu.VMEM((4, 2, TB, PATCH), BF16),
            pltpu.VMEM((PATCH, FB), BF16),
            pltpu.VMEM((2 * FB,), F32),
            pltpu.VMEM((FB, HB), BF16),
            pltpu.VMEM((HB, FB), BF16),
            pltpu.VMEM((LAYERS, FB), F32),
            pltpu.VMEM((LAYERS, HU), F32),
            pltpu.VMEM((LAYERS, FB), F32),
            pltpu.VMEM((2 * FB,), F32),
            pltpu.VMEM((FB, CHECK), BF16),
            pltpu.VMEM((ZS, TB, FB), F32),
            pltpu.VMEM((ZS, 8, 128), F32),
            pltpu.VMEM((ZS, 8, 128), F32),
            pltpu.VMEM((1, HB), F32),
            pltpu.VMEM((ZS, 1, HB), F32),
            pltpu.VMEM((8, HU), F32),
            pltpu.VMEM((2, 8, HU), F32),
            pltpu.VMEM((ZS, TB, HB), BF16),
            pltpu.VMEM((2, TB // 2, HB), BF16),
            pltpu.VMEM((2, 3, TB, HB), BF16),
            pltpu.VMEM((TB, HB), F32),
            pltpu.VMEM((ZS, TB, HB), BF16),
            pltpu.VMEM((ZS, TB, FB), BF16),
            pltpu.VMEM((7, ZS, SUB, FB), BF16),
            pltpu.VMEM((2, 64, 128), BF16),
            pltpu.VMEM((7, 64, 128), BF16),
            pltpu.VMEM((8, 128), F32),
            pltpu.VMEM((7, 8, 128), F32),
            pltpu.VMEM((QUARTER, HU), BF16),
            pltpu.VMEM((QUARTER, FB), BF16),
            dma((10,)), dma((4, 8)), dma((4, 8)), dma((4, 8)), dma((4, 8)),
            dma((8,)), dma((8,)), dma((8,)), dma((8,)), dma((2, 8)), dma((2, 8)), dma((2,)), dma((2,)),
            dma((2, 4, 2)), dma((2, 4, 2)), dma((2, 4, 2)), dma((2, 4, 2)),
            dma, dma,
            dma((2, 2)), dma((2, 2)), dma((2,)), dma((2,)), dma((2, 2, 2)), dma((2, 2, 2)),
        ],
        compiler_params=pltpu.CompilerParams(
            collective_id=0, has_side_effects=True, vmem_limit_bytes=36 * 2**20
        ),
    )(
        *map(pinned, (patches.reshape(4, SUB, PATCH), embed_weight, embed_bias, old_in, old_out)), restore_id, *map(pinned, (
        norm_gains, in_biases, out_biases, final_gain, check_weight,
    )))
    return new_in.reshape(2 * FB, HU), new_out, logits


def solution(mesh):
    placed = (
        P(("rep", "col"), None),
        P(None, "row"),
        P("row"),
        P(("row", "col"), None, None),
        P(("row", "col"), None, None),
        P(),
        P(None, "row"),
        P(None, "col"),
        P(None, "row"),
        P("row"),
        P("row", None),
    )
    return jax.shard_map(
        on_device,
        mesh=mesh,
        in_specs=placed,
        out_specs=(P("row", "col"), P("col", "row"), P(("rep", "col"), None)),
        check_vma=False,
    )
```

```python
import functools

import jax
import jax.numpy as jnp
from jax import lax
from jax.experimental import pallas as pl
from jax.experimental.pallas import tpu as pltpu
from jax.sharding import PartitionSpec as P

EPSILON = 1e-06
MESH = pl.DeviceIdType.MESH
F32, BF16 = jnp.float32, jnp.bfloat16

REPS, ROWS, COLS = 4, 4, 16
ZS, WS = 8, 8
D, FF, PATCH, CHECK = 6144, 12288, 588, 128
LAYERS = 48
FB = D // ZS
HB = FF // WS
HU = HB // 2
TB = 128
SUB = TB // WS
QUARTER = FB // REPS


def kernel(
    patches, embed_w, embed_b, old_in, old_out, rid, gains, in_b, out_b, final_g, check_w,
    new_in, new_out, logits,
    P_, We, be, IT, OT, gt, ibt, obt, fg, Wc,
    E, st, stall, q, qall, bsrc, bb, PP, rf, C, H, Yb, R, LB, LR, T, TR, XI, XO,
    lsem, psend, precv, dsend, drecv, ssend, srecv, qsend, qrecv, fsend, frecv, bsend, brecv,
    rsend, rrecv, asend, arecv, ysend, yrecv, xsend, xrecv, zsend, zrecv, gsend, grecv,
):
    y, h, col = lax.axis_index("rep"), lax.axis_index("row"), lax.axis_index("col")
    l, w = col // 8, col % 8
    x, c = w // 2, w % 2
    z = 2 * h + l

    def at(yy, zz, ww):
        return (yy, zz // 2, (zz % 2) * 8 + ww)

    def remote(src, dst, ss, rs, dev):
        return pltpu.make_async_remote_copy(
            src_ref=src, dst_ref=dst, send_sem=ss, recv_sem=rs, device_id=dev, device_id_type=MESH
        )

    def landed(ref, sem):
        pltpu.make_async_copy(ref, ref, sem).wait()

    half = pl.ds(pl.multiple_of(l * FB, 128), FB)
    loads = [
        pltpu.make_async_copy(src, dst, lsem.at[n])
        for n, (src, dst) in enumerate([
            (embed_w.at[:, half], We),
            (embed_b, be),
            (gains.at[:, half], gt),
            (in_b, ibt),
            (old_in.at[0], IT),
            (out_b.at[:, half], obt),
            (final_g, fg),
            (check_w.at[pl.ds(pl.multiple_of(l * FB, 128), FB), :], Wc),
            (old_out.at[0], OT),
        ])
    ]
    own = pltpu.make_async_copy(patches, P_.at[:, l, pl.ds(w * SUB, SUB), :], lsem.at[9])
    own.start()
    for load in loads:
        load.start()

    barrier = pltpu.get_barrier_semaphore()
    peers = [at(y, 2 * h + (l + a) % 2, (w + b) % 8) for a in range(2) for b in range(8) if a or b]
    peers += [at(y, (z + 2 * k) % 8, w) for k in range(1, 4)]
    peers += [at(y, 2 * ((h + k) % 4) + (1 - l), w) for k in range(1, 4)]
    peers += [((y + 1) % REPS, h, col), ((y + 3) % REPS, h, col)]
    for peer in peers:
        pl.semaphore_signal(barrier, inc=1, device_id=peer, device_id_type=MESH)
    own.wait()
    pl.semaphore_wait(barrier, len(peers))

    partner = at(y, z, 2 * x + 1 - c)

    def wave(v):
        return (h + (2, 1, 3, 0)[v]) % 4

    def patch_copy(v, k):
        place = P_.at[wave(v), l if k < 5 else 1 - l, pl.ds(w * SUB, SUB), :]
        dev = at(y, 2 * h + 1 - l, w) if k == 4 else at(y, z, ((x + k % 4) % 4) * 2 + c)
        return remote(place, place, psend.at[v, k], precv.at[v, k], dev)

    def partner_copy(v, k, core):
        ls, xs = (l + k // 4) % 2, (x + 4 - k % 4) % 4
        piece = P_.at[wave(v), ls, pl.ds((2 * xs + core) * SUB, SUB), :]
        return remote(piece, piece, dsend.at[v, k], drecv.at[v, k], partner)

    def arrived(v, k):
        ls, xs = (l + k // 4) % 2, (x + 4 - k % 4) % 4
        landed(P_.at[wave(v), ls, pl.ds((2 * xs + c) * SUB, SUB), :], precv.at[v, k])

    for v in range(4):
        for k in range(1, 5):
            patch_copy(v, k).start()
        partner_copy(v, 0, c).start()

    loads[3].wait()
    bsrc[...] = jnp.broadcast_to(ibt[pl.ds(rid[0], 1), :], bsrc.shape)
    bias_to = 4 * l + x

    def bias_copies(act):
        for a in range(2):
            is_self = jnp.logical_and(l == a, w == bias_to)

            @pl.when(is_self)
            def _():
                if act == "start":
                    pltpu.make_async_copy(bsrc, bb.at[c], brecv.at[c]).start()

            @pl.when(jnp.logical_not(is_self))
            def _():
                copy = remote(bsrc, bb.at[c], bsend.at[a], brecv.at[c], at(y, 2 * h + a, bias_to))
                copy.start() if act == "start" else copy.wait_send()

    bias_copies("start")

    def pass_on(v):
        arrived(v, 4)
        for k in range(5, 8):
            patch_copy(v, k).start()
        partner_copy(v, 4, c).start()

    def receive(v, first, last):
        for k in range(first, last):
            if k not in (0, 4):
                arrived(v, k)
                partner_copy(v, k, c).start()
        for k in range(first, last):
            partner_copy(v, k, 1 - c).wait_recv()

    for n in (0, 1, 2, 4):
        loads[n].wait()
    gain = gt[pl.ds(rid[0], 1), :]

    def my_half(ref):
        v = ref[...].reshape(1, 2 * FB)
        return jnp.where(l == 0, v[:, :FB], v[:, FB:])

    embed_bias = my_half(be)
    gains16 = jnp.broadcast_to(gain, (16, FB))
    gains_hi = gains16.astype(BF16)
    gains_lo = (gains16 - gains_hi.astype(F32)).astype(BF16)
    product = jnp.dot(gains_hi, IT[...], preferred_element_type=F32)
    product = product + jnp.dot(gains_lo, IT[...], preferred_element_type=F32)
    q[...] = product[0:1, :]

    def q_copy(k):
        return remote(q, qall.at[k], qsend.at[k], qrecv.at[k], at(y, (z + k) % 8, w))

    for k in range(1, 8):
        q_copy(k).start()
    lane = lax.broadcasted_iota(jnp.int32, (TB, 128), 1)

    def stat_copy(k):
        t = (z + k) % 8
        return remote(st.at[t], stall.at[k], ssend.at[k], srecv.at[k], at(y, t, w))

    def first_product(k):
        t = (z + k) % 8
        e = jnp.dot(P_[t // 2, t % 2], We[...], preferred_element_type=F32) + embed_bias
        E[t] = e
        m = jnp.sum(e, axis=1, keepdims=True) / FB
        s2 = jnp.sum(e * e, axis=1, keepdims=True)
        n = ((e - m) * gain).astype(BF16)
        PP[t] = jnp.dot(n, IT[...], preferred_element_type=F32).astype(BF16)
        st[t] = jnp.where(lane == 0, m, jnp.where(lane == 1, s2, 0.0)).T[0:8, :]
        if not isinstance(k, int) or k > 0:
            stat_copy(k).start()

    def towards(d, k):
        return (z + 8 + (1 - 2 * d) * k) % 8

    outward, inward = 1 - l, l

    def lanes_of(u):
        return pl.ds(u * HU, HU)

    def reduce_copy(d, s, u):
        src = PP.at[towards(d, 5 - s), :, lanes_of(u)]
        dst = rf.at[d, s - 1, :, lanes_of(u)]
        return remote(src, dst, rsend.at[d, s - 1, u], rrecv.at[d, s - 1, u], at(y, towards(d, 1), w))

    def add_received(d, s, u):
        landed(rf.at[d, s - 2, :, lanes_of(u)], rrecv.at[d, s - 2, u])
        to = (towards(d, 5 - s), slice(None), lanes_of(u))
        PP[to] = (PP[to].astype(F32) + rf[d, s - 2, :, lanes_of(u)].astype(F32)).astype(BF16)

    def reduce_step(s):
        for u in range(2):
            if s == 2:
                reduce_copy(outward, s, u).start()
                add_received(inward, s, u)
                reduce_copy(inward, s, u).start()
            else:
                for d in range(2):
                    add_received(d, s, u)
                    reduce_copy(d, s, u).start()

    def two_products(low, high):
        def one(n, _):
            first_product(low + n * (high - low))
            return 0

        lax.fori_loop(0, 2, one, 0)

    receive(0, 0, 4)
    pass_on(0)
    first_product(4)
    for u in range(2):
        reduce_copy(outward, 1, u).start()
    for v in (1, 2, 3):
        pass_on(v)

    loads[8].wait()
    quarter = pl.ds(pl.multiple_of(y * QUARTER, 64), QUARTER)
    to_l, to_x = x // 2, 2 * (x % 2) + c

    def tile_copies(act):
        for a in range(2):
            for u in range(2):
                rows = pl.ds(pl.multiple_of(u * HU + y * QUARTER, 64), QUARTER)
                src = IT.at[quarter, lanes_of(u)] if a == 0 else OT.at[rows, :]
                is_self = jnp.logical_and(to_x == x, c == u)
                dev = at(y, z, 2 * to_x + u)
                for stays in (True, False):
                    if stays:
                        dst, n = (new_in.at[l, quarter, :] if a == 0 else new_out.at[quarter, half]), 0
                    else:
                        dst, n = (XI if a == 0 else XO), 1
                    here = (to_l == l) if stays else (to_l != l)

                    @pl.when(jnp.logical_and(here, is_self))
                    def _():
                        if act == "start":
                            pltpu.make_async_copy(src, dst, xrecv.at[a, n]).start()

                    @pl.when(jnp.logical_and(here, jnp.logical_not(is_self)))
                    def _():
                        copy = remote(src, dst, xsend.at[a, u], xrecv.at[a, n], dev)
                        copy.start() if act == "start" else copy.wait_send()

    tile_copies("start")

    receive(0, 4, 8)
    for v in (1, 2):
        receive(v, 0, 8)
    two_products(3, 5)
    reduce_step(2)
    two_products(2, 6)
    receive(3, 0, 8)
    reduce_step(3)
    two_products(1, 7)

    def cross_copy(a):
        dst = new_in.at[l, quarter, :] if a == 0 else new_out.at[quarter, half]
        return remote((XI, XO)[a], dst, zsend.at[a], zrecv.at[a], at(y, 2 * h + 1 - l, w))

    def spread_copy(d, a, stage):
        owner = y if stage == 0 else (y + 3 if d == 0 else y + 1) % REPS
        if stage == 0:
            rows = pl.ds(pl.multiple_of(owner * QUARTER, 64), QUARTER)
        else:
            rows = pl.ds(pl.multiple_of(owner * QUARTER + d * (QUARTER // 2), 32), QUARTER // 2)
        ref = new_in.at[:, rows, :] if a == 0 else new_out.at[rows, :]
        to = (y + 1 if d == 0 else y + 3) % REPS
        return remote(ref, ref, gsend.at[d, a, stage], grecv.at[d, a, stage], (to, h, col))

    def cross(a):
        landed((XI, XO)[a], xrecv.at[a, 1])
        cross_copy(a).start()

    def spread(a):
        landed(new_in.at[l, quarter, :] if a == 0 else new_out.at[quarter, half], xrecv.at[a, 0])
        cross_copy(a).wait_recv()
        for d in range(2):
            spread_copy(d, a, 0).start()

    def spread_on(a):
        for d in range(2):
            spread_copy(d, a, 0).wait_recv()
            spread_copy(d, a, 1).start()

    cross(0)
    reduce_step(4)
    cross(1)
    first_product(0)
    for k in range(1, 8):
        stat_copy(k).wait_recv()
        q_copy(k).wait_recv()

    def columns_of(tiles):
        mean = functools.reduce(jnp.add, [t[0:1] for t in tiles]) / ZS
        square = functools.reduce(jnp.add, [t[1:2] for t in tiles]) / D
        scale = lax.rsqrt(square - mean * mean + EPSILON)
        rows = [t[0:1] - mean for t in tiles] + [scale, jnp.zeros((128 - ZS - 1, 128), F32)]
        return jnp.concatenate(rows, axis=0).T

    cols = columns_of([st[z]] + [stall[k] for k in range(1, 8)])
    for u in range(2):
        lanes = slice(u * HU, (u + 1) * HU)
        v = PP[z, :, lanes_of(u)].astype(F32) + cols[:, 0:1] * q[:, lanes]
        for k in range(1, 8):
            v = v + cols[:, k:k + 1] * qall[k, :, lanes]
        C[:, lanes] = v
        landed(bb.at[u], brecv.at[u])

    def gather_copy(d, s, u):
        ref = H.at[towards(1 - d, s - 1), :, lanes_of(u)]
        return remote(ref, ref, asend.at[d, s - 1, u], arecv.at[d, s - 1, u], at(y, towards(d, 1), w))

    for u in range(2):
        lanes = slice(u * HU, (u + 1) * HU)
        for d in range(2):
            reduce_copy(d, 4, u).wait_recv()
        v = C[:, lanes] + rf[0, 3, :, lanes].astype(F32) + rf[1, 3, :, lanes].astype(F32)
        v = v * cols[:, ZS:ZS + 1] + bb[u, 0:1, :]
        H[z, :, lanes_of(u)] = (0.5 * v * (1.0 + lax.erf(v * 0.7071067811865476))).astype(BF16)
        for d in range(2):
            gather_copy(d, 1, u).start()

    def second_product(t):
        Yb[t] = jnp.dot(H[t], OT[...], preferred_element_type=F32).astype(BF16)
        for k in range(1, 8):
            to = (w + k) % 8
            remote(
                Yb.at[t, pl.ds(pl.multiple_of(to * SUB, SUB), SUB), :], R.at[k - 1, t], ysend, yrecv, at(y, z, to)
            ).start()

    spread(0)
    second_product(z)
    for s in range(2, 5):
        for u in range(2):
            for d in range(2):
                landed(H.at[towards(1 - d, s - 1), :, lanes_of(u)], arecv.at[d, s - 2, u])
                if s < 4:
                    gather_copy(d, s, u).start()
            if s == 4:
                gather_copy(outward, s, u).start()

        def pair(d, _):
            second_product((z + 8 + (2 * d - 1) * (s - 1)) % 8)
            return 0

        lax.fori_loop(0, 2, pair, 0)
        if s == 2:
            spread(1)
        if s == 3:
            spread_on(0)
        if s == 4:
            spread_on(1)

    for n in (5, 6, 7):
        loads[n].wait()
    final_gain = my_half(fg)
    out_bias = obt[pl.ds(rid[0], 1), :]
    weights = Wc[...]
    gain_w = jnp.sum(
        jnp.broadcast_to(final_gain, (128, FB)).T[:, 0:1] * weights.astype(F32), axis=0, keepdims=True
    )
    for u in range(2):
        landed(H.at[(z + 4) % 8, :, lanes_of(u)], arecv.at[inward, 3, u])
    second_product((z + 4) % 8)

    landed(R, yrecv)
    mine = pl.ds(pl.multiple_of(w * SUB, SUB), SUB)
    row = lax.broadcasted_iota(jnp.int32, (8, 128), 0)
    columns = []
    for a in range(2):
        parts = []
        for b in range(4):
            t = 2 * b + a
            u = E[t, mine, :] + out_bias + Yb[t, mine, :].astype(F32)
            for k in range(7):
                u = u + R[k, t].astype(F32)
            parts.append(u)
        u = jnp.concatenate(parts, axis=0)
        m = jnp.sum(u, axis=1, keepdims=True) / FB
        s2 = jnp.sum(u * u, axis=1, keepdims=True)
        v = (u - m) * final_gain
        hi = v.astype(BF16)
        lo = (v - hi.astype(F32)).astype(BF16)
        part = jnp.dot(hi, weights, preferred_element_type=F32) + jnp.dot(lo, weights, preferred_element_type=F32)
        LB[a] = part.astype(BF16)
        columns.append(jnp.where(lane[0:64] == 0, m, jnp.where(lane[0:64] == 1, s2, 0.0)))
    turned = jnp.concatenate(columns, axis=0).T[0:8, :]
    T[...] = jnp.where(row == 2, gain_w, turned)

    def last_copies(k):
        dev = at(y, (z + k) % 8, w)
        return (
            remote(LB.at[(z + k) % 2], LR.at[k - 1], fsend.at[0, k], frecv.at[0, k], dev),
            remote(T, TR.at[k - 1], fsend.at[1, k], frecv.at[1, k], dev),
        )

    for k in range(1, 8):
        for copy in last_copies(k):
            copy.start()
    for k in range(1, 8):
        for copy in last_copies(k):
            copy.wait_recv()
    tiles = [T[...]] + [TR[k] for k in range(7)]
    E[0, :, 0:128] = columns_of(tiles)
    cols = E[0, pl.ds(pl.multiple_of(l * 64, 64), 64), 0:128]
    v = LB[l].astype(F32) + cols[:, 0:1] * tiles[0][2:3]
    for k in range(7):
        v = v + LR[k].astype(F32) + cols[:, k + 1:k + 2] * tiles[k + 1][2:3]
    logits[...] = v * cols[:, ZS:ZS + 1]

    for a in range(2):
        cross_copy(a).wait_send()
        for d in range(2):
            spread_copy(d, a, 1).wait_recv()
            spread_copy(d, a, 0).wait_send()
            spread_copy(d, a, 1).wait_send()
    tile_copies("wait")
    bias_copies("wait")
    for v in range(4):
        for k in range(8):
            if k > 0:
                patch_copy(v, k).wait_send()
            partner_copy(v, k, c).wait_send()
    for k in range(1, 8):
        stat_copy(k).wait_send()
        q_copy(k).wait_send()
        for copy in last_copies(k):
            copy.wait_send()
    for u in range(2):
        reduce_copy(outward, 1, u).wait_send()
        gather_copy(outward, 4, u).wait_send()
        for s in range(1, 4):
            for d in range(2):
                reduce_copy(d, s + 1, u).wait_send()
                gather_copy(d, s, u).wait_send()
    landed(R, ysend)


def write_out(new_in, new_out, logits, in_w, out_w, check, sem):
    copies = [pltpu.make_async_copy(logits, check, sem.at[4])]
    for n, (src, dst) in enumerate(((new_in, in_w), (new_out, out_w))):
        rows = src.shape[0] // 2
        for half in range(2):
            part = pl.ds(half * rows, rows)
            copies.append(pltpu.make_async_copy(src.at[part, :], dst.at[part, :], sem.at[2 * n + half]))
    for copy in copies:
        copy.start()
    for copy in copies:
        copy.wait()


def on_device(
    patches, embed_weight, embed_bias, old_in, old_out, restore_id, norm_gains, in_biases, out_biases,
    final_gain, check_weight,
):
    def pinned(a):
        return pltpu.with_memory_space_constraint(a, pltpu.HBM)

    hbm = pl.BlockSpec(memory_space=pltpu.HBM)
    vmem = pl.BlockSpec(memory_space=pltpu.VMEM)
    dma = pltpu.SemaphoreType.DMA
    new_in, new_out, logits = pl.pallas_call(
        kernel,
        name="relayout_forward",
        out_shape=(
            jax.ShapeDtypeStruct((2, FB, HU), BF16),
            jax.ShapeDtypeStruct((HU, 2 * FB), BF16),
            jax.ShapeDtypeStruct((64, CHECK), F32),
        ),
        in_specs=[hbm] * 5 + [pl.BlockSpec(memory_space=pltpu.SMEM)] + [hbm] * 5,
        out_specs=(vmem, vmem, vmem),
        scratch_shapes=[
            pltpu.VMEM((4, 2, TB, PATCH), BF16),
            pltpu.VMEM((PATCH, FB), BF16),
            pltpu.VMEM((2 * FB,), F32),
            pltpu.VMEM((FB, HB), BF16),
            pltpu.VMEM((HB, FB), BF16),
            pltpu.VMEM((LAYERS, FB), F32),
            pltpu.VMEM((LAYERS, HU), F32),
            pltpu.VMEM((LAYERS, FB), F32),
            pltpu.VMEM((2 * FB,), F32),
            pltpu.VMEM((FB, CHECK), BF16),
            pltpu.VMEM((ZS, TB, FB), F32),
            pltpu.VMEM((ZS, 8, 128), F32),
            pltpu.VMEM((ZS, 8, 128), F32),
            pltpu.VMEM((1, HB), F32),
            pltpu.VMEM((ZS, 1, HB), F32),
            pltpu.VMEM((8, HU), F32),
            pltpu.VMEM((2, 8, HU), F32),
            pltpu.VMEM((ZS, TB, HB), BF16),
            pltpu.VMEM((2, 4, TB, HB), BF16),
            pltpu.VMEM((TB, HB), F32),
            pltpu.VMEM((ZS, TB, HB), BF16),
            pltpu.VMEM((ZS, TB, FB), BF16),
            pltpu.VMEM((7, ZS, SUB, FB), BF16),
            pltpu.VMEM((2, 64, 128), BF16),
            pltpu.VMEM((7, 64, 128), BF16),
            pltpu.VMEM((8, 128), F32),
            pltpu.VMEM((7, 8, 128), F32),
            pltpu.VMEM((QUARTER, HU), BF16),
            pltpu.VMEM((QUARTER, FB), BF16),
            dma((10,)), dma((4, 8)), dma((4, 8)), dma((4, 8)), dma((4, 8)),
            dma((8,)), dma((8,)), dma((8,)), dma((8,)), dma((2, 8)), dma((2, 8)), dma((2,)), dma((2,)),
            dma((2, 4, 2)), dma((2, 4, 2)), dma((2, 4, 2)), dma((2, 4, 2)),
            dma, dma,
            dma((2, 2)), dma((2, 2)), dma((2,)), dma((2,)), dma((2, 2, 2)), dma((2, 2, 2)),
        ],
        compiler_params=pltpu.CompilerParams(
            collective_id=0, has_side_effects=True, vmem_limit_bytes=36 * 2**20
        ),
    )(
        *map(pinned, (patches.reshape(4, SUB, PATCH), embed_weight, embed_bias, old_in, old_out)), restore_id, *map(pinned, (
        norm_gains, in_biases, out_biases, final_gain, check_weight,
    )))
    return pl.pallas_call(
        write_out,
        name="write_out",
        out_shape=(
            jax.ShapeDtypeStruct((2 * FB, HU), BF16),
            jax.ShapeDtypeStruct((HU, 2 * FB), BF16),
            jax.ShapeDtypeStruct((64, CHECK), F32),
        ),
        in_specs=[vmem] * 3,
        out_specs=(hbm, hbm, hbm),
        scratch_shapes=[dma((5,))],
        compiler_params=pltpu.CompilerParams(vmem_limit_bytes=2**20),
    )(new_in.reshape(2 * FB, HU), new_out, logits)


def solution(mesh):
    placed = (
        P(("rep", "col"), None),
        P(None, "row"),
        P("row"),
        P(("row", "col"), None, None),
        P(("row", "col"), None, None),
        P(),
        P(None, "row"),
        P(None, "col"),
        P(None, "row"),
        P("row"),
        P("row", None),
    )
    return jax.shard_map(
        on_device,
        mesh=mesh,
        in_specs=placed,
        out_specs=(P("row", "col"), P("col", "row"), P(("rep", "col"), None)),
        check_vma=False,
    )
```

```python
import functools

import jax
import jax.numpy as jnp
from jax import lax
from jax.experimental import pallas as pl
from jax.experimental.pallas import tpu as pltpu
from jax.sharding import PartitionSpec as P

EPSILON = 1e-06
MESH = pl.DeviceIdType.MESH
F32, BF16 = jnp.float32, jnp.bfloat16

REPS, ROWS, COLS = 4, 4, 16
ZS, WS = 8, 8
D, FF, PATCH, CHECK = 6144, 12288, 588, 128
LAYERS = 48
FB = D // ZS
HB = FF // WS
HU = HB // 2
TB = 128
SUB = TB // WS
QUARTER = FB // REPS


def kernel(
    patches, embed_w, embed_b, old_in, old_out, rid, gains, in_b, out_b, final_g, check_w,
    new_in, new_out, logits,
    P_, We, be, IT, OT, gt, ibt, obt, fg, Wc,
    E, st, stall, q, qall, bsrc, bb, PP, rf, C, H, Yb, R, LB, LR, T, TR, XI, XO,
    lsem, psend, precv, dsend, drecv, ssend, srecv, qsend, qrecv, fsend, frecv, bsend, brecv,
    rsend, rrecv, asend, arecv, ysend, yrecv, xsend, xrecv, zsend, zrecv, gsend, grecv,
):
    y, h, col = lax.axis_index("rep"), lax.axis_index("row"), lax.axis_index("col")
    l, w = col // 8, col % 8
    x, c = w // 2, w % 2
    z = 2 * h + l

    def at(yy, zz, ww):
        return (yy, zz // 2, (zz % 2) * 8 + ww)

    def remote(src, dst, ss, rs, dev):
        return pltpu.make_async_remote_copy(
            src_ref=src, dst_ref=dst, send_sem=ss, recv_sem=rs, device_id=dev, device_id_type=MESH
        )

    def landed(ref, sem):
        pltpu.make_async_copy(ref, ref, sem).wait()

    half = pl.ds(pl.multiple_of(l * FB, 128), FB)
    loads = [
        pltpu.make_async_copy(src, dst, lsem.at[n])
        for n, (src, dst) in enumerate([
            (embed_w.at[:, half], We),
            (embed_b, be),
            (gains.at[:, half], gt),
            (in_b, ibt),
            (old_in.at[0], IT),
            (out_b.at[:, half], obt),
            (final_g, fg),
            (check_w.at[pl.ds(pl.multiple_of(l * FB, 128), FB), :], Wc),
            (old_out.at[0], OT),
        ])
    ]
    own = pltpu.make_async_copy(patches, P_.at[:, l, pl.ds(w * SUB, SUB), :], lsem.at[9])
    own.start()
    for load in loads:
        load.start()

    barrier = pltpu.get_barrier_semaphore()
    peers = [at(y, 2 * h + (l + a) % 2, (w + b) % 8) for a in range(2) for b in range(8) if a or b]
    peers += [at(y, (z + 2 * k) % 8, w) for k in range(1, 4)]
    peers += [at(y, 2 * ((h + k) % 4) + (1 - l), w) for k in range(1, 4)]
    peers += [((y + 1) % REPS, h, col), ((y + 3) % REPS, h, col)]
    for peer in peers:
        pl.semaphore_signal(barrier, inc=1, device_id=peer, device_id_type=MESH)
    own.wait()
    pl.semaphore_wait(barrier, len(peers))

    partner = at(y, z, 2 * x + 1 - c)

    def wave(v):
        return (h + (2, 1, 3, 0)[v]) % 4

    def patch_copy(v, k):
        place = P_.at[wave(v), l if k < 5 else 1 - l, pl.ds(w * SUB, SUB), :]
        dev = at(y, 2 * h + 1 - l, w) if k == 4 else at(y, z, ((x + k % 4) % 4) * 2 + c)
        return remote(place, place, psend.at[v, k], precv.at[v, k], dev)

    def partner_copy(v, k, core):
        ls, xs = (l + k // 4) % 2, (x + 4 - k % 4) % 4
        piece = P_.at[wave(v), ls, pl.ds((2 * xs + core) * SUB, SUB), :]
        return remote(piece, piece, dsend.at[v, k], drecv.at[v, k], partner)

    def arrived(v, k):
        ls, xs = (l + k // 4) % 2, (x + 4 - k % 4) % 4
        landed(P_.at[wave(v), ls, pl.ds((2 * xs + c) * SUB, SUB), :], precv.at[v, k])

    for v in range(4):
        for k in range(1, 5):
            patch_copy(v, k).start()
        partner_copy(v, 0, c).start()

    loads[3].wait()
    bsrc[...] = jnp.broadcast_to(ibt[pl.ds(rid[0], 1), :], bsrc.shape)
    bias_to = 4 * l + x

    def bias_copies(act):
        for a in range(2):
            is_self = jnp.logical_and(l == a, w == bias_to)

            @pl.when(is_self)
            def _():
                if act == "start":
                    pltpu.make_async_copy(bsrc, bb.at[c], brecv.at[c]).start()

            @pl.when(jnp.logical_not(is_self))
            def _():
                copy = remote(bsrc, bb.at[c], bsend.at[a], brecv.at[c], at(y, 2 * h + a, bias_to))
                copy.start() if act == "start" else copy.wait_send()

    bias_copies("start")

    def pass_on(v):
        arrived(v, 4)
        for k in range(5, 8):
            patch_copy(v, k).start()
        partner_copy(v, 4, c).start()

    def receive(v, first, last):
        for k in range(first, last):
            if k not in (0, 4):
                arrived(v, k)
                partner_copy(v, k, c).start()
        for k in range(first, last):
            partner_copy(v, k, 1 - c).wait_recv()

    for n in (0, 1, 2, 4):
        loads[n].wait()
    gain = gt[pl.ds(rid[0], 1), :]

    def my_half(ref):
        v = ref[...].reshape(1, 2 * FB)
        return jnp.where(l == 0, v[:, :FB], v[:, FB:])

    embed_bias = my_half(be)
    gains16 = jnp.broadcast_to(gain, (16, FB))
    gains_hi = gains16.astype(BF16)
    gains_lo = (gains16 - gains_hi.astype(F32)).astype(BF16)
    product = jnp.dot(gains_hi, IT[...], preferred_element_type=F32)
    product = product + jnp.dot(gains_lo, IT[...], preferred_element_type=F32)
    q[...] = product[0:1, :]

    def q_copy(k):
        return remote(q, qall.at[k], qsend.at[k], qrecv.at[k], at(y, (z + k) % 8, w))

    for k in range(1, 8):
        q_copy(k).start()
    lane = lax.broadcasted_iota(jnp.int32, (TB, 128), 1)

    def stat_copy(k):
        t = (z + k) % 8
        return remote(st.at[t], stall.at[k], ssend.at[k], srecv.at[k], at(y, t, w))

    def first_product(k):
        t = (z + k) % 8
        e = jnp.dot(P_[t // 2, t % 2], We[...], preferred_element_type=F32) + embed_bias
        E[t] = e
        m = jnp.sum(e, axis=1, keepdims=True) / FB
        s2 = jnp.sum(e * e, axis=1, keepdims=True)
        n = ((e - m) * gain).astype(BF16)
        PP[t] = jnp.dot(n, IT[...], preferred_element_type=F32).astype(BF16)
        st[t] = jnp.where(lane == 0, m, jnp.where(lane == 1, s2, 0.0)).T[0:8, :]
        if not isinstance(k, int) or k > 0:
            stat_copy(k).start()

    def towards(d, k):
        return (z + 8 + (1 - 2 * d) * k) % 8

    outward, inward = 1 - l, l

    def lanes_of(u):
        return pl.ds(u * HU, HU)

    def reduce_copy(d, s, u):
        src = PP.at[towards(d, 5 - s), :, lanes_of(u)]
        dst = rf.at[d, s - 1, :, lanes_of(u)]
        return remote(src, dst, rsend.at[d, s - 1, u], rrecv.at[d, s - 1, u], at(y, towards(d, 1), w))

    def add_received(d, s, u):
        landed(rf.at[d, s - 2, :, lanes_of(u)], rrecv.at[d, s - 2, u])
        to = (towards(d, 5 - s), slice(None), lanes_of(u))
        PP[to] = (PP[to].astype(F32) + rf[d, s - 2, :, lanes_of(u)].astype(F32)).astype(BF16)

    def reduce_step(s):
        for u in range(2):
            if s == 2:
                reduce_copy(outward, s, u).start()
                add_received(inward, s, u)
                reduce_copy(inward, s, u).start()
            else:
                for d in range(2):
                    add_received(d, s, u)
                    reduce_copy(d, s, u).start()

    def two_products(low, high):
        def one(n, _):
            first_product(low + n * (high - low))
            return 0

        lax.fori_loop(0, 2, one, 0)

    receive(0, 0, 4)
    pass_on(0)
    first_product(4)
    for u in range(2):
        reduce_copy(outward, 1, u).start()
    for v in (1, 2, 3):
        pass_on(v)

    loads[8].wait()
    quarter = pl.ds(pl.multiple_of(y * QUARTER, 64), QUARTER)
    to_l, to_x = x // 2, 2 * (x % 2) + c

    def tile_copies(act):
        for a in range(2):
            for u in range(2):
                rows = pl.ds(pl.multiple_of(u * HU + y * QUARTER, 64), QUARTER)
                src = IT.at[quarter, lanes_of(u)] if a == 0 else OT.at[rows, :]
                is_self = jnp.logical_and(to_x == x, c == u)
                dev = at(y, z, 2 * to_x + u)
                for stays in (True, False):
                    if stays:
                        dst, n = (new_in.at[l, quarter, :] if a == 0 else new_out.at[quarter, half]), 0
                    else:
                        dst, n = (XI if a == 0 else XO), 1
                    here = (to_l == l) if stays else (to_l != l)

                    @pl.when(jnp.logical_and(here, is_self))
                    def _():
                        if act == "start":
                            pltpu.make_async_copy(src, dst, xrecv.at[a, n]).start()

                    @pl.when(jnp.logical_and(here, jnp.logical_not(is_self)))
                    def _():
                        copy = remote(src, dst, xsend.at[a, u], xrecv.at[a, n], dev)
                        copy.start() if act == "start" else copy.wait_send()

    receive(0, 4, 8)
    for v in (1, 2):
        receive(v, 0, 8)
    tile_copies("start")
    two_products(3, 5)
    reduce_step(2)
    two_products(2, 6)
    receive(3, 0, 8)
    reduce_step(3)
    two_products(1, 7)

    def cross_copy(a):
        dst = new_in.at[l, quarter, :] if a == 0 else new_out.at[quarter, half]
        return remote((XI, XO)[a], dst, zsend.at[a], zrecv.at[a], at(y, 2 * h + 1 - l, w))

    def spread_copy(d, a, p, stage):
        owner = y if stage == 0 else (y + 3 if d == 0 else y + 1) % REPS
        if stage == 0:
            rows = pl.ds(pl.multiple_of(owner * QUARTER, 64), QUARTER)
        else:
            rows = pl.ds(pl.multiple_of(owner * QUARTER + d * (QUARTER // 2), 32), QUARTER // 2)
        s = l if p == 0 else 1 - l
        ref = new_in.at[s, rows, :] if a == 0 else new_out.at[rows, pl.ds(pl.multiple_of(s * FB, 128), FB)]
        to = (y + 1 if d == 0 else y + 3) % REPS
        return remote(ref, ref, gsend.at[d, a, p, stage], grecv.at[d, a, p, stage], (to, h, col))

    def cross(a):
        landed((XI, XO)[a], xrecv.at[a, 1])
        cross_copy(a).start()

    def spread(a, p):
        if p == 0:
            landed(new_in.at[l, quarter, :] if a == 0 else new_out.at[quarter, half], xrecv.at[a, 0])
        else:
            cross_copy(a).wait_recv()
        for d in range(2):
            spread_copy(d, a, p, 0).start()

    def spread_on(a, p):
        for d in range(2):
            spread_copy(d, a, p, 0).wait_recv()
            spread_copy(d, a, p, 1).start()

    reduce_step(4)
    cross(0)
    first_product(0)
    spread(0, 0)
    spread(1, 0)
    for k in range(1, 8):
        stat_copy(k).wait_recv()
        q_copy(k).wait_recv()

    def columns_of(tiles):
        mean = functools.reduce(jnp.add, [t[0:1] for t in tiles]) / ZS
        square = functools.reduce(jnp.add, [t[1:2] for t in tiles]) / D
        scale = lax.rsqrt(square - mean * mean + EPSILON)
        rows = [t[0:1] - mean for t in tiles] + [scale, jnp.zeros((128 - ZS - 1, 128), F32)]
        return jnp.concatenate(rows, axis=0).T

    cols = columns_of([st[z]] + [stall[k] for k in range(1, 8)])
    for u in range(2):
        lanes = slice(u * HU, (u + 1) * HU)
        v = PP[z, :, lanes_of(u)].astype(F32) + cols[:, 0:1] * q[:, lanes]
        for k in range(1, 8):
            v = v + cols[:, k:k + 1] * qall[k, :, lanes]
        C[:, lanes] = v
        landed(bb.at[u], brecv.at[u])

    def gather_copy(d, s, u):
        ref = H.at[towards(1 - d, s - 1), :, lanes_of(u)]
        return remote(ref, ref, asend.at[d, s - 1, u], arecv.at[d, s - 1, u], at(y, towards(d, 1), w))

    for u in range(2):
        lanes = slice(u * HU, (u + 1) * HU)
        for d in range(2):
            reduce_copy(d, 4, u).wait_recv()
        v = C[:, lanes] + rf[0, 3, :, lanes].astype(F32) + rf[1, 3, :, lanes].astype(F32)
        v = v * cols[:, ZS:ZS + 1] + bb[u, 0:1, :]
        H[z, :, lanes_of(u)] = (0.5 * v * (1.0 + lax.erf(v * 0.7071067811865476))).astype(BF16)
        for d in range(2):
            gather_copy(d, 1, u).start()

    def second_product(t):
        Yb[t] = jnp.dot(H[t], OT[...], preferred_element_type=F32).astype(BF16)
        for k in range(1, 8):
            to = (w + k) % 8
            remote(
                Yb.at[t, pl.ds(pl.multiple_of(to * SUB, SUB), SUB), :], R.at[k - 1, t], ysend, yrecv, at(y, z, to)
            ).start()

    second_product(z)
    for s in range(2, 5):
        for u in range(2):
            for d in range(2):
                landed(H.at[towards(1 - d, s - 1), :, lanes_of(u)], arecv.at[d, s - 2, u])
                if s < 4:
                    gather_copy(d, s, u).start()
            if s == 4:
                gather_copy(outward, s, u).start()
        if s == 3:
            cross(1)

        def pair(d, _):
            second_product((z + 8 + (2 * d - 1) * (s - 1)) % 8)
            return 0

        lax.fori_loop(0, 2, pair, 0)
        if s == 2:
            spread(0, 1)
            spread_on(0, 0)
            spread_on(1, 0)
        if s == 4:
            spread_on(0, 1)

    for n in (5, 6, 7):
        loads[n].wait()
    final_gain = my_half(fg)
    out_bias = obt[pl.ds(rid[0], 1), :]
    weights = Wc[...]
    gain_w = jnp.sum(
        jnp.broadcast_to(final_gain, (128, FB)).T[:, 0:1] * weights.astype(F32), axis=0, keepdims=True
    )
    for u in range(2):
        landed(H.at[(z + 4) % 8, :, lanes_of(u)], arecv.at[inward, 3, u])
    second_product((z + 4) % 8)

    spread(1, 1)
    landed(R, yrecv)
    mine = pl.ds(pl.multiple_of(w * SUB, SUB), SUB)
    row = lax.broadcasted_iota(jnp.int32, (8, 128), 0)
    columns = []
    for a in range(2):
        parts = []
        for b in range(4):
            t = 2 * b + a
            u = E[t, mine, :] + out_bias + Yb[t, mine, :].astype(F32)
            for k in range(7):
                u = u + R[k, t].astype(F32)
            parts.append(u)
        u = jnp.concatenate(parts, axis=0)
        m = jnp.sum(u, axis=1, keepdims=True) / FB
        s2 = jnp.sum(u * u, axis=1, keepdims=True)
        v = (u - m) * final_gain
        hi = v.astype(BF16)
        lo = (v - hi.astype(F32)).astype(BF16)
        part = jnp.dot(hi, weights, preferred_element_type=F32) + jnp.dot(lo, weights, preferred_element_type=F32)
        LB[a] = part.astype(BF16)
        columns.append(jnp.where(lane[0:64] == 0, m, jnp.where(lane[0:64] == 1, s2, 0.0)))
    turned = jnp.concatenate(columns, axis=0).T[0:8, :]
    T[...] = jnp.where(row == 2, gain_w, turned)

    def last_copies(k):
        dev = at(y, (z + k) % 8, w)
        return (
            remote(LB.at[(z + k) % 2], LR.at[k - 1], fsend.at[0, k], frecv.at[0, k], dev),
            remote(T, TR.at[k - 1], fsend.at[1, k], frecv.at[1, k], dev),
        )

    for k in range(1, 8):
        for copy in last_copies(k):
            copy.start()
    spread_on(1, 1)
    for k in range(1, 8):
        for copy in last_copies(k):
            copy.wait_recv()
    tiles = [T[...]] + [TR[k] for k in range(7)]
    E[0, :, 0:128] = columns_of(tiles)
    cols = E[0, pl.ds(pl.multiple_of(l * 64, 64), 64), 0:128]
    v = LB[l].astype(F32) + cols[:, 0:1] * tiles[0][2:3]
    for k in range(7):
        v = v + LR[k].astype(F32) + cols[:, k + 1:k + 2] * tiles[k + 1][2:3]
    logits[...] = v * cols[:, ZS:ZS + 1]

    for a in range(2):
        cross_copy(a).wait_send()
        for p in range(2):
            for d in range(2):
                spread_copy(d, a, p, 1).wait_recv()
                spread_copy(d, a, p, 0).wait_send()
                spread_copy(d, a, p, 1).wait_send()
    tile_copies("wait")
    bias_copies("wait")
    for v in range(4):
        for k in range(8):
            if k > 0:
                patch_copy(v, k).wait_send()
            partner_copy(v, k, c).wait_send()
    for k in range(1, 8):
        stat_copy(k).wait_send()
        q_copy(k).wait_send()
        for copy in last_copies(k):
            copy.wait_send()
    for u in range(2):
        reduce_copy(outward, 1, u).wait_send()
        gather_copy(outward, 4, u).wait_send()
        for s in range(1, 4):
            for d in range(2):
                reduce_copy(d, s + 1, u).wait_send()
                gather_copy(d, s, u).wait_send()
    landed(R, ysend)


def write_out(new_in, new_out, logits, in_w, out_w, check, sem):
    copies = [pltpu.make_async_copy(logits, check, sem.at[4])]
    for n, (src, dst) in enumerate(((new_in, in_w), (new_out, out_w))):
        rows = src.shape[0] // 2
        for half in range(2):
            part = pl.ds(half * rows, rows)
            copies.append(pltpu.make_async_copy(src.at[part, :], dst.at[part, :], sem.at[2 * n + half]))
    for copy in copies:
        copy.start()
    for copy in copies:
        copy.wait()


def on_device(
    patches, embed_weight, embed_bias, old_in, old_out, restore_id, norm_gains, in_biases, out_biases,
    final_gain, check_weight,
):
    def pinned(a):
        return pltpu.with_memory_space_constraint(a, pltpu.HBM)

    hbm = pl.BlockSpec(memory_space=pltpu.HBM)
    vmem = pl.BlockSpec(memory_space=pltpu.VMEM)
    dma = pltpu.SemaphoreType.DMA
    new_in, new_out, logits = pl.pallas_call(
        kernel,
        name="relayout_forward",
        out_shape=(
            jax.ShapeDtypeStruct((2, FB, HU), BF16),
            jax.ShapeDtypeStruct((HU, 2 * FB), BF16),
            jax.ShapeDtypeStruct((64, CHECK), F32),
        ),
        in_specs=[hbm] * 5 + [pl.BlockSpec(memory_space=pltpu.SMEM)] + [hbm] * 5,
        out_specs=(vmem, vmem, vmem),
        scratch_shapes=[
            pltpu.VMEM((4, 2, TB, PATCH), BF16),
            pltpu.VMEM((PATCH, FB), BF16),
            pltpu.VMEM((2 * FB,), F32),
            pltpu.VMEM((FB, HB), BF16),
            pltpu.VMEM((HB, FB), BF16),
            pltpu.VMEM((LAYERS, FB), F32),
            pltpu.VMEM((LAYERS, HU), F32),
            pltpu.VMEM((LAYERS, FB), F32),
            pltpu.VMEM((2 * FB,), F32),
            pltpu.VMEM((FB, CHECK), BF16),
            pltpu.VMEM((ZS, TB, FB), F32),
            pltpu.VMEM((ZS, 8, 128), F32),
            pltpu.VMEM((ZS, 8, 128), F32),
            pltpu.VMEM((1, HB), F32),
            pltpu.VMEM((ZS, 1, HB), F32),
            pltpu.VMEM((8, HU), F32),
            pltpu.VMEM((2, 8, HU), F32),
            pltpu.VMEM((ZS, TB, HB), BF16),
            pltpu.VMEM((2, 4, TB, HB), BF16),
            pltpu.VMEM((TB, HB), F32),
            pltpu.VMEM((ZS, TB, HB), BF16),
            pltpu.VMEM((ZS, TB, FB), BF16),
            pltpu.VMEM((7, ZS, SUB, FB), BF16),
            pltpu.VMEM((2, 64, 128), BF16),
            pltpu.VMEM((7, 64, 128), BF16),
            pltpu.VMEM((8, 128), F32),
            pltpu.VMEM((7, 8, 128), F32),
            pltpu.VMEM((QUARTER, HU), BF16),
            pltpu.VMEM((QUARTER, FB), BF16),
            dma((10,)), dma((4, 8)), dma((4, 8)), dma((4, 8)), dma((4, 8)),
            dma((8,)), dma((8,)), dma((8,)), dma((8,)), dma((2, 8)), dma((2, 8)), dma((2,)), dma((2,)),
            dma((2, 4, 2)), dma((2, 4, 2)), dma((2, 4, 2)), dma((2, 4, 2)),
            dma, dma,
            dma((2, 2)), dma((2, 2)), dma((2,)), dma((2,)), dma((2, 2, 2, 2)), dma((2, 2, 2, 2)),
        ],
        compiler_params=pltpu.CompilerParams(
            collective_id=0, has_side_effects=True, vmem_limit_bytes=36 * 2**20
        ),
    )(
        *map(pinned, (patches.reshape(4, SUB, PATCH), embed_weight, embed_bias, old_in, old_out)), restore_id, *map(pinned, (
        norm_gains, in_biases, out_biases, final_gain, check_weight,
    )))
    return pl.pallas_call(
        write_out,
        name="write_out",
        out_shape=(
            jax.ShapeDtypeStruct((2 * FB, HU), BF16),
            jax.ShapeDtypeStruct((HU, 2 * FB), BF16),
            jax.ShapeDtypeStruct((64, CHECK), F32),
        ),
        in_specs=[vmem] * 3,
        out_specs=(hbm, hbm, hbm),
        scratch_shapes=[dma((5,))],
        compiler_params=pltpu.CompilerParams(vmem_limit_bytes=2**20),
    )(new_in.reshape(2 * FB, HU), new_out, logits)


def solution(mesh):
    placed = (
        P(("rep", "col"), None),
        P(None, "row"),
        P("row"),
        P(("row", "col"), None, None),
        P(("row", "col"), None, None),
        P(),
        P(None, "row"),
        P(None, "col"),
        P(None, "row"),
        P("row"),
        P("row", None),
    )
    return jax.shard_map(
        on_device,
        mesh=mesh,
        in_specs=placed,
        out_specs=(P("row", "col"), P("col", "row"), P(("rep", "col"), None)),
        check_vma=False,
    )
```

```python
import functools

import jax
import jax.numpy as jnp
from jax import lax
from jax.experimental import pallas as pl
from jax.experimental.pallas import tpu as pltpu
from jax.sharding import PartitionSpec as P

EPSILON = 1e-06
MESH = pl.DeviceIdType.MESH
F32, BF16 = jnp.float32, jnp.bfloat16

REPS, ROWS, COLS = 4, 4, 16
ZS, WS = 8, 8
D, FF, PATCH, CHECK = 6144, 12288, 588, 128
LAYERS = 48
FB = D // ZS
HB = FF // WS
HU = HB // 2
TB = 128
SUB = TB // WS
QUARTER = FB // REPS


def kernel(
    patches, embed_w, embed_b, old_in, old_out, rid, gains, in_b, out_b, final_g, check_w,
    new_in, new_out, logits,
    P_, We, be, IT, OT, gt, ibt, obt, fg, Wc,
    E, st, stall, q, qall, bsrc, bb, PP, rf, C, H, Yb, R, LB, LR, T, TR, XI, XO,
    lsem, psend, precv, dsend, drecv, ssend, srecv, qsend, qrecv, fsend, frecv, bsend, brecv,
    rsend, rrecv, asend, arecv, ysend, yrecv, xsend, xrecv, zsend, zrecv, gsend, grecv, gend,
):
    y, h, col = lax.axis_index("rep"), lax.axis_index("row"), lax.axis_index("col")
    l, w = col // 8, col % 8
    x, c = w // 2, w % 2
    z = 2 * h + l

    def at(yy, zz, ww):
        return (yy, zz // 2, (zz % 2) * 8 + ww)

    def remote(src, dst, ss, rs, dev):
        return pltpu.make_async_remote_copy(
            src_ref=src, dst_ref=dst, send_sem=ss, recv_sem=rs, device_id=dev, device_id_type=MESH
        )

    def landed(ref, sem):
        pltpu.make_async_copy(ref, ref, sem).wait()

    half = pl.ds(pl.multiple_of(l * FB, 128), FB)
    loads = [
        pltpu.make_async_copy(src, dst, lsem.at[n])
        for n, (src, dst) in enumerate([
            (embed_w.at[:, half], We),
            (embed_b, be),
            (gains.at[:, half], gt),
            (in_b, ibt),
            (old_in.at[0], IT),
            (out_b.at[:, half], obt),
            (final_g, fg),
            (check_w.at[pl.ds(pl.multiple_of(l * FB, 128), FB), :], Wc),
            (old_out.at[0], OT),
        ])
    ]
    own = pltpu.make_async_copy(patches, P_.at[:, l, pl.ds(w * SUB, SUB), :], lsem.at[9])
    own.start()
    for load in loads:
        load.start()

    barrier = pltpu.get_barrier_semaphore()
    peers = [at(y, 2 * h + (l + a) % 2, (w + b) % 8) for a in range(2) for b in range(8) if a or b]
    peers += [at(y, (z + 2 * k) % 8, w) for k in range(1, 4)]
    peers += [at(y, 2 * ((h + k) % 4) + (1 - l), w) for k in range(1, 4)]
    peers += [((y + 1) % REPS, h, col), ((y + 3) % REPS, h, col)]
    for peer in peers:
        pl.semaphore_signal(barrier, inc=1, device_id=peer, device_id_type=MESH)
    own.wait()
    pl.semaphore_wait(barrier, len(peers))

    partner = at(y, z, 2 * x + 1 - c)

    def wave(v, plane):
        return (h + 2 + (v % 2) * (1 - 2 * plane)) % 4 if v < 2 else (h + (1 + 2 * plane if v == 2 else 0)) % 4

    def patch_copy(v, k):
        plane = l if k < 5 else 1 - l
        place = P_.at[wave(v, plane), plane, pl.ds(w * SUB, SUB), :]
        dev = at(y, 2 * h + 1 - l, w) if k == 4 else at(y, z, ((x + k % 4) % 4) * 2 + c)
        return remote(place, place, psend, precv.at[v, 0 if k < 4 else 1 if k == 4 else 2], dev)

    def partner_copy(v, k, core):
        ls, xs = (l + k // 4) % 2, (x + 4 - k % 4) % 4
        piece = P_.at[wave(v, ls), ls, pl.ds((2 * xs + core) * SUB, SUB), :]
        if v == 0 and k < 4 and core is c:
            piece = P_.at[wave(v, l), l, pl.ds(w * SUB, SUB), :]
            return remote(piece, piece, dsend, drecv.at[v, 0], at(y, z, ((x + k) % 4) * 2 + 1 - c))
        return remote(piece, piece, dsend, drecv.at[v, k // 4 if v == 0 else 0], partner)

    def arrived(n, sem):
        landed(P_.at[0, 0, pl.ds(0, n * SUB), :], sem)

    for v in range(4):
        for k in range(1, 5):
            patch_copy(v, k).start()
        for k in range(4 if v == 0 else 1):
            partner_copy(v, k, c).start()

    loads[3].wait()
    bsrc[...] = jnp.broadcast_to(ibt[pl.ds(rid[0], 1), :], bsrc.shape)
    bias_to = 4 * l + x

    def bias_copies(act):
        for a in range(2):
            is_self = jnp.logical_and(l == a, w == bias_to)

            @pl.when(is_self)
            def _():
                if act == "start":
                    pltpu.make_async_copy(bsrc, bb.at[c], brecv.at[c]).start()

            @pl.when(jnp.logical_not(is_self))
            def _():
                copy = remote(bsrc, bb.at[c], bsend.at[a], brecv.at[c], at(y, 2 * h + a, bias_to))
                copy.start() if act == "start" else copy.wait_send()

    bias_copies("start")

    def pass_on(v):
        arrived(1, precv.at[v, 1])
        for k in range(5, 8):
            patch_copy(v, k).start()
        partner_copy(v, 4, c).start()

    def receive(v, first, last):
        if first == 0:
            arrived(3, precv.at[v, 0])
            for k in range(1, 4):
                if v > 0:
                    partner_copy(v, k, c).start()
        if last == 8:
            arrived(3, precv.at[v, 2])
            for k in range(5, 8):
                partner_copy(v, k, c).start()
        arrived(last - first, drecv.at[v, first // 4])

    for n in (0, 1, 2, 4):
        loads[n].wait()
    gain = gt[pl.ds(rid[0], 1), :]

    def my_half(ref):
        v = ref[...].reshape(1, 2 * FB)
        return jnp.where(l == 0, v[:, :FB], v[:, FB:])

    embed_bias = my_half(be)
    gains16 = jnp.broadcast_to(gain, (16, FB))
    gains_hi = gains16.astype(BF16)
    gains_lo = (gains16 - gains_hi.astype(F32)).astype(BF16)
    product = jnp.dot(gains_hi, IT[...], preferred_element_type=F32)
    product = product + jnp.dot(gains_lo, IT[...], preferred_element_type=F32)
    q[...] = product[0:1, :]

    def q_copy(k):
        return remote(q, qall.at[k], qsend, qrecv, at(y, (z + k) % 8, w))

    for k in range(1, 8):
        q_copy(k).start()
    lane = lax.broadcasted_iota(jnp.int32, (TB, 128), 1)

    def stat_copy(k):
        t = (z + k) % 8
        return remote(st.at[t], stall.at[k], ssend, srecv, at(y, t, w))

    def first_product(k):
        t = (z + k) % 8
        e = jnp.dot(P_[t // 2, t % 2], We[...], preferred_element_type=F32) + embed_bias
        E[t] = e
        m = jnp.sum(e, axis=1, keepdims=True) / FB
        s2 = jnp.sum(e * e, axis=1, keepdims=True)
        n = ((e - m) * gain).astype(BF16)
        PP[t] = jnp.dot(n, IT[...], preferred_element_type=F32).astype(BF16)
        st[t] = jnp.where(lane == 0, m, jnp.where(lane == 1, s2, 0.0)).T[0:8, :]
        if not isinstance(k, int) or k > 0:
            stat_copy(k).start()

    def towards(d, k):
        return (z + 8 + (1 - 2 * d) * k) % 8


    def lanes_of(u):
        return pl.ds(u * HU, HU)

    def rows_of(d, s):
        return pl.ds(d * (TB // 2), TB // 2) if s == 1 else slice(None)

    def reduce_copy(d, s, u):
        src = PP.at[towards(d, 5 - s), rows_of(d, s), lanes_of(u)]
        dst = rf.at[d, s - 1, rows_of(d, s), lanes_of(u)]
        return remote(src, dst, rsend, rrecv.at[d, s - 1, u], at(y, towards(d, 1), w))

    def add_received(d, s, u):
        rows = rows_of(d, s - 1)
        landed(rf.at[d, s - 2, rows, lanes_of(u)], rrecv.at[d, s - 2, u])
        to = (towards(d, 5 - s), rows, lanes_of(u))
        PP[to] = (PP[to].astype(F32) + rf[d, s - 2, rows, lanes_of(u)].astype(F32)).astype(BF16)

    def reduce_step(s):
        for u in range(2):
            for d in range(2):
                add_received(d, s, u)
                reduce_copy(d, s, u).start()

    def two_products(low, high):
        def one(n, _):
            first_product(low + n * (high - low))
            return 0

        lax.fori_loop(0, 2, one, 0)

    receive(0, 0, 4)
    pass_on(0)
    first_product(4)
    for u in range(2):
        for d in range(2):
            reduce_copy(d, 1, u).start()
    for v in (1, 2, 3):
        pass_on(v)

    loads[8].wait()
    quarter = pl.ds(pl.multiple_of(y * QUARTER, 64), QUARTER)
    to_l, to_x = x // 2, 2 * (x % 2) + c

    def tile_copies(act):
        for a in range(2):
            for u in range(2):
                rows = pl.ds(pl.multiple_of(u * HU + y * QUARTER, 64), QUARTER)
                src = IT.at[quarter, lanes_of(u)] if a == 0 else OT.at[rows, :]
                is_self = jnp.logical_and(to_x == x, c == u)
                dev = at(y, z, 2 * to_x + u)
                for stays in (True, False):
                    if stays:
                        dst, n = (new_in.at[l, quarter, :] if a == 0 else new_out.at[quarter, half]), 0
                    else:
                        dst, n = (XI if a == 0 else XO), 1
                    here = (to_l == l) if stays else (to_l != l)

                    @pl.when(jnp.logical_and(here, is_self))
                    def _():
                        if act == "start":
                            pltpu.make_async_copy(src, dst, xrecv.at[a, n]).start()

                    @pl.when(jnp.logical_and(here, jnp.logical_not(is_self)))
                    def _():
                        copy = remote(src, dst, xsend.at[a, u], xrecv.at[a, n], dev)
                        copy.start() if act == "start" else copy.wait_send()

    receive(0, 4, 8)
    first_product(5 - 2 * l)
    receive(1, 0, 8)
    first_product(3 + 2 * l)
    reduce_step(2)
    receive(2, 0, 8)
    tile_copies("start")
    two_products(2, 6)
    receive(3, 0, 8)
    reduce_step(3)
    two_products(1, 7)

    pieces = ((0, 0, 0, QUARTER), (1, 0, 0, QUARTER), (0, 1, 0, QUARTER), (1, 1, 0, QUARTER // 2), (1, 1, QUARTER // 2, QUARTER // 2))

    def piece_ref(i, plane, owner, skip, n):
        rows = pl.ds(pl.multiple_of(owner * QUARTER + pieces[i][2] + skip, 16), n)
        if pieces[i][0] == 0:
            return new_in.at[plane, rows, :]
        return new_out.at[rows, pl.ds(pl.multiple_of(plane * FB, 128), FB)]

    def cross_copy(i):
        n = pieces[i][3]
        src = (XI, XO)[pieces[i][0]].at[pl.ds(pieces[i][2], n), :]
        return remote(src, piece_ref(i, l, y, 0, n), zsend.at[i - 2], zrecv.at[i - 2], at(y, 2 * h + 1 - l, w))

    def spread_copy(d, i, stage):
        owner = y if stage == 0 else (y + 3 if d == 0 else y + 1) % REPS
        n = pieces[i][3] if stage == 0 else pieces[i][3] // 2
        ref = piece_ref(i, 1 - l if pieces[i][1] else l, owner, 0 if stage == 0 else d * n, n)
        to = (y + 1 if d == 0 else y + 3) % REPS
        return remote(ref, ref, gsend.at[d], grecv.at[d, i] if stage == 0 else gend, (to, h, col))

    def spread(i):
        if pieces[i][1]:
            cross_copy(i).wait_recv()
        else:
            landed(piece_ref(i, l, y, 0, QUARTER), xrecv.at[pieces[i][0], 0])
        for d in range(2):
            spread_copy(d, i, 0).start()

    def spread_on(i):
        for d in range(2):
            spread_copy(d, i, 0).wait_recv()
            spread_copy(d, i, 1).start()

    reduce_step(4)
    landed(XI, xrecv.at[0, 1])
    cross_copy(2).start()
    first_product(0)
    spread(0)
    spread(1)
    landed(stall.at[pl.ds(1, 7)], srecv)
    landed(qall.at[pl.ds(1, 7)], qrecv)

    def columns_of(tiles):
        mean = functools.reduce(jnp.add, [t[0:1] for t in tiles]) / ZS
        square = functools.reduce(jnp.add, [t[1:2] for t in tiles]) / D
        scale = lax.rsqrt(square - mean * mean + EPSILON)
        rows = [t[0:1] - mean for t in tiles] + [scale, jnp.zeros((128 - ZS - 1, 128), F32)]
        return jnp.concatenate(rows, axis=0).T

    cols = columns_of([st[z]] + [stall[k] for k in range(1, 8)])
    for u in range(2):
        lanes = slice(u * HU, (u + 1) * HU)
        v = PP[z, :, lanes_of(u)].astype(F32) + cols[:, 0:1] * q[:, lanes]
        for k in range(1, 8):
            v = v + cols[:, k:k + 1] * qall[k, :, lanes]
        C[:, lanes] = v
        landed(bb.at[u], brecv.at[u])

    outward, inward = 1 - l, l

    def gather_copy(d, s, u):
        ref = H.at[towards(1 - d, s - 1), :, lanes_of(u)]
        return remote(ref, ref, asend, arecv.at[d, s - 1, u], at(y, towards(d, 1), w))

    for u in range(2):
        lanes = slice(u * HU, (u + 1) * HU)
        for d in range(2):
            reduce_copy(d, 4, u).wait_recv()
        v = C[:, lanes] + rf[0, 3, :, lanes].astype(F32) + rf[1, 3, :, lanes].astype(F32)
        v = v * cols[:, ZS:ZS + 1] + bb[u, 0:1, :]
        H[z, :, lanes_of(u)] = (0.5 * v * (1.0 + lax.erf(v * 0.7071067811865476))).astype(BF16)
        for d in range(2):
            gather_copy(d, 1, u).start()

    def second_product(t):
        Yb[t] = jnp.dot(H[t], OT[...], preferred_element_type=F32).astype(BF16)
        for k in range(1, 8):
            to = (w + k) % 8
            remote(
                Yb.at[t, pl.ds(pl.multiple_of(to * SUB, SUB), SUB), :], R.at[k - 1, t], ysend, yrecv, at(y, z, to)
            ).start()

    second_product(z)
    for s in range(2, 5):
        for u in range(2):
            for d in range(2):
                landed(H.at[towards(1 - d, s - 1), :, lanes_of(u)], arecv.at[d, s - 2, u])
                if s < 4:
                    gather_copy(d, s, u).start()
            if s == 4:
                gather_copy(outward, s, u).start()
        if s == 3:
            landed(XO, xrecv.at[1, 1])
            cross_copy(3).start()
            cross_copy(4).start()

        def pair(d, _):
            second_product((z + 8 + (2 * d - 1) * (s - 1)) % 8)
            return 0

        lax.fori_loop(0, 2, pair, 0)
        if s == 2:
            spread(2)
            spread_on(0)
            spread_on(1)
        if s == 4:
            spread_on(2)
            spread(3)

    for n in (5, 6, 7):
        loads[n].wait()
    final_gain = my_half(fg)
    out_bias = obt[pl.ds(rid[0], 1), :]
    weights = Wc[...]
    gain_w = jnp.sum(
        jnp.broadcast_to(final_gain, (128, FB)).T[:, 0:1] * weights.astype(F32), axis=0, keepdims=True
    )
    for u in range(2):
        landed(H.at[(z + 4) % 8, :, lanes_of(u)], arecv.at[inward, 3, u])
    second_product((z + 4) % 8)

    spread(4)
    landed(R, yrecv)
    spread_on(3)
    mine = pl.ds(pl.multiple_of(w * SUB, SUB), SUB)
    row = lax.broadcasted_iota(jnp.int32, (8, 128), 0)
    columns = []
    for a in range(2):
        parts = []
        for b in range(4):
            t = 2 * b + a
            u = E[t, mine, :] + out_bias + Yb[t, mine, :].astype(F32)
            for k in range(7):
                u = u + R[k, t].astype(F32)
            parts.append(u)
        u = jnp.concatenate(parts, axis=0)
        m = jnp.sum(u, axis=1, keepdims=True) / FB
        s2 = jnp.sum(u * u, axis=1, keepdims=True)
        v = (u - m) * final_gain
        hi = v.astype(BF16)
        lo = (v - hi.astype(F32)).astype(BF16)
        part = jnp.dot(hi, weights, preferred_element_type=F32) + jnp.dot(lo, weights, preferred_element_type=F32)
        LB[a] = part.astype(BF16)
        columns.append(jnp.where(lane[0:64] == 0, m, jnp.where(lane[0:64] == 1, s2, 0.0)))
    turned = jnp.concatenate(columns, axis=0).T[0:8, :]
    T[...] = jnp.where(row == 2, gain_w, turned)

    def last_copies(k):
        dev = at(y, (z + k) % 8, w)
        return (
            remote(LB.at[(z + k) % 2], LR.at[k - 1], fsend.at[0], frecv.at[0], dev),
            remote(T, TR.at[k - 1], fsend.at[1], frecv.at[1], dev),
        )

    for k in range(1, 8):
        for copy in last_copies(k):
            copy.start()
    spread_on(4)
    landed(LR, frecv.at[0])
    landed(TR, frecv.at[1])
    tiles = [T[...]] + [TR[k] for k in range(7)]
    E[0, :, 0:128] = columns_of(tiles)
    cols = E[0, pl.ds(pl.multiple_of(l * 64, 64), 64), 0:128]
    v = LB[l].astype(F32) + cols[:, 0:1] * tiles[0][2:3]
    for k in range(7):
        v = v + LR[k].astype(F32) + cols[:, k + 1:k + 2] * tiles[k + 1][2:3]
    logits[...] = v * cols[:, ZS:ZS + 1]

    landed(OT.at[pl.ds(0, 2 * FB // 2), :], gend)
    for d in range(2):
        landed(OT.at[pl.ds(0, HB * 3 // 4), :], gsend.at[d])
    for i in range(2, 5):
        cross_copy(i).wait_send()
    tile_copies("wait")
    bias_copies("wait")
    landed(P_.at[:, 0, pl.ds(0, 7 * SUB), :], psend)
    landed(P_.at[:, 0], dsend)
    landed(stall.at[pl.ds(1, 7)], ssend)
    landed(qall.at[pl.ds(1, 7)], qsend)
    landed(LR, fsend.at[0])
    landed(TR, fsend.at[1])
    landed(PP.at[pl.ds(0, 7)], rsend)
    landed(H.at[pl.ds(0, 7)], asend)
    landed(R, ysend)


def write_out(new_in, new_out, logits, in_w, out_w, check, sem):
    copies = [pltpu.make_async_copy(logits, check, sem.at[4])]
    for n, (src, dst) in enumerate(((new_in, in_w), (new_out, out_w))):
        rows = src.shape[0] // 2
        for half in range(2):
            part = pl.ds(half * rows, rows)
            copies.append(pltpu.make_async_copy(src.at[part, :], dst.at[part, :], sem.at[2 * n + half]))
    for copy in copies:
        copy.start()
    for copy in copies:
        copy.wait()


def on_device(
    patches, embed_weight, embed_bias, old_in, old_out, restore_id, norm_gains, in_biases, out_biases,
    final_gain, check_weight,
):
    def pinned(a):
        return pltpu.with_memory_space_constraint(a, pltpu.HBM)

    hbm = pl.BlockSpec(memory_space=pltpu.HBM)
    vmem = pl.BlockSpec(memory_space=pltpu.VMEM)
    dma = pltpu.SemaphoreType.DMA
    new_in, new_out, logits = pl.pallas_call(
        kernel,
        name="relayout_forward",
        out_shape=(
            jax.ShapeDtypeStruct((2, FB, HU), BF16),
            jax.ShapeDtypeStruct((HU, 2 * FB), BF16),
            jax.ShapeDtypeStruct((64, CHECK), F32),
        ),
        in_specs=[hbm] * 5 + [pl.BlockSpec(memory_space=pltpu.SMEM)] + [hbm] * 5,
        out_specs=(vmem, vmem, vmem),
        scratch_shapes=[
            pltpu.VMEM((4, 2, TB, PATCH), BF16),
            pltpu.VMEM((PATCH, FB), BF16),
            pltpu.VMEM((2 * FB,), F32),
            pltpu.VMEM((FB, HB), BF16),
            pltpu.VMEM((HB, FB), BF16),
            pltpu.VMEM((LAYERS, FB), F32),
            pltpu.VMEM((LAYERS, HU), F32),
            pltpu.VMEM((LAYERS, FB), F32),
            pltpu.VMEM((2 * FB,), F32),
            pltpu.VMEM((FB, CHECK), BF16),
            pltpu.VMEM((ZS, TB, FB), F32),
            pltpu.VMEM((ZS, 8, 128), F32),
            pltpu.VMEM((ZS, 8, 128), F32),
            pltpu.VMEM((1, HB), F32),
            pltpu.VMEM((ZS, 1, HB), F32),
            pltpu.VMEM((8, HU), F32),
            pltpu.VMEM((2, 8, HU), F32),
            pltpu.VMEM((ZS, TB, HB), BF16),
            pltpu.VMEM((2, 4, TB, HB), BF16),
            pltpu.VMEM((TB, HB), F32),
            pltpu.VMEM((ZS, TB, HB), BF16),
            pltpu.VMEM((ZS, TB, FB), BF16),
            pltpu.VMEM((7, ZS, SUB, FB), BF16),
            pltpu.VMEM((2, 64, 128), BF16),
            pltpu.VMEM((7, 64, 128), BF16),
            pltpu.VMEM((8, 128), F32),
            pltpu.VMEM((7, 8, 128), F32),
            pltpu.VMEM((QUARTER, HU), BF16),
            pltpu.VMEM((QUARTER, FB), BF16),
            dma((10,)), dma, dma((4, 3)), dma, dma((4, 2)),
            dma, dma, dma, dma, dma((2,)), dma((2,)), dma((2,)), dma((2,)),
            dma, dma((2, 4, 2)), dma, dma((2, 4, 2)),
            dma, dma,
            dma((2, 2)), dma((2, 2)), dma((3,)), dma((3,)), dma((2,)), dma((2, 5)), dma,
        ],
        compiler_params=pltpu.CompilerParams(
            collective_id=0, has_side_effects=True, vmem_limit_bytes=36 * 2**20
        ),
    )(
        *map(pinned, (patches.reshape(4, SUB, PATCH), embed_weight, embed_bias, old_in, old_out)), restore_id, *map(pinned, (
        norm_gains, in_biases, out_biases, final_gain, check_weight,
    )))
    return pl.pallas_call(
        write_out,
        name="write_out",
        out_shape=(
            jax.ShapeDtypeStruct((2 * FB, HU), BF16),
            jax.ShapeDtypeStruct((HU, 2 * FB), BF16),
            jax.ShapeDtypeStruct((64, CHECK), F32),
        ),
        in_specs=[vmem] * 3,
        out_specs=(hbm, hbm, hbm),
        scratch_shapes=[dma((5,))],
        compiler_params=pltpu.CompilerParams(vmem_limit_bytes=2**20),
    )(new_in.reshape(2 * FB, HU), new_out, logits)


def solution(mesh):
    placed = (
        P(("rep", "col"), None),
        P(None, "row"),
        P("row"),
        P(("row", "col"), None, None),
        P(("row", "col"), None, None),
        P(),
        P(None, "row"),
        P(None, "col"),
        P(None, "row"),
        P("row"),
        P("row", None),
    )
    return jax.shard_map(
        on_device,
        mesh=mesh,
        in_specs=placed,
        out_specs=(P("row", "col"), P("col", "row"), P(("rep", "col"), None)),
        check_vma=False,
    )
```

```python
import functools

import jax
import jax.numpy as jnp
from jax import lax
from jax.experimental import pallas as pl
from jax.experimental.pallas import tpu as pltpu
from jax.sharding import PartitionSpec as P

EPSILON = 1e-06
MESH = pl.DeviceIdType.MESH
F32, BF16 = jnp.float32, jnp.bfloat16

REPS, ROWS, COLS = 4, 4, 16
ZS, WS = 8, 8
D, FF, PATCH, CHECK = 6144, 12288, 588, 128
LAYERS = 48
FB = D // ZS
HB = FF // WS
HU = HB // 2
TB = 128
SUB = TB // WS
QUARTER = FB // REPS
CHUNKS = 4
CHUNK = TB // CHUNKS


def kernel(
    patches, embed_w, embed_b, old_in, old_out, rid, gains, in_b, out_b, final_g, check_w,
    new_in, new_out, logits,
    P_, We, be, IT, OT, gt, ibt, obt, fg, Wc,
    E, st, stall, qown, qall, bsrc, bb, PP, rf, C, H, Yb, R, LB, LR, T, TR, XI, XO,
    lsem, psend, precv, dsend, drecv, ssend, srecv, qsend, qrecv, fsend, frecv, bsend, brecv,
    rsend, rrecv, asend, arecv, ysend, yrecv, xsend, xrecv, zsend, zrecv, gsend, grecv, gend,
):
    y, h, col = lax.axis_index("rep"), lax.axis_index("row"), lax.axis_index("col")
    l, w = col // 8, col % 8
    x, c = w // 2, w % 2
    z = 2 * h + l
    slot = pl.ds(pl.multiple_of((4 * c + x) * SUB, SUB), SUB)

    def at(yy, zz, ww):
        return (yy, zz // 2, (zz % 2) * 8 + ww)

    def remote(src, dst, ss, rs, dev):
        return pltpu.make_async_remote_copy(
            src_ref=src, dst_ref=dst, send_sem=ss, recv_sem=rs, device_id=dev, device_id_type=MESH
        )

    def landed(ref, sem):
        pltpu.make_async_copy(ref, ref, sem).wait()

    half = pl.ds(pl.multiple_of(l * FB, 128), FB)
    loads = [
        pltpu.make_async_copy(src, dst, lsem.at[n])
        for n, (src, dst) in enumerate([
            (embed_w.at[:, half], We),
            (embed_b, be),
            (gains.at[:, half], gt),
            (in_b, ibt),
            (old_in.at[0], IT),
            (out_b.at[:, half], obt),
            (final_g, fg),
            (check_w.at[pl.ds(pl.multiple_of(l * FB, 128), FB), :], Wc),
            (old_out.at[0], OT),
        ])
    ]
    own = pltpu.make_async_copy(patches, P_.at[:, l, slot, :], lsem.at[9])
    own.start()
    for load in loads:
        load.start()

    barrier = pltpu.get_barrier_semaphore()
    peers = [at(y, 2 * h + (l + a) % 2, (w + b) % 8) for a in range(2) for b in range(8) if a or b]
    peers += [at(y, (z + 2 * k) % 8, w) for k in range(1, 4)]
    peers += [at(y, 2 * ((h + k) % 4) + (1 - l), w) for k in range(1, 4)]
    peers += [((y + 1) % REPS, h, col), ((y + 3) % REPS, h, col)]
    for peer in peers:
        pl.semaphore_signal(barrier, inc=1, device_id=peer, device_id_type=MESH)
    own.wait()
    pl.semaphore_wait(barrier, len(peers))

    partner = at(y, z, 2 * x + 1 - c)

    def wave(v, plane):
        return (h + 2 + (v % 2) * (1 - 2 * plane)) % 4 if v < 2 else (h + (1 + 2 * plane if v == 2 else 0)) % 4

    def patch_copy(v, k):
        plane = l if k < 5 else 1 - l
        place = P_.at[wave(v, plane), plane, slot, :]
        dev = at(y, 2 * h + 1 - l, w) if k == 4 else at(y, z, ((x + k % 4) % 4) * 2 + c)
        return remote(place, place, psend, precv.at[v, 0 if k < 4 else 1 if k == 4 else 2], dev)

    def partner_copy(v, k, core):
        ls, xs = (l + k // 4) % 2, (x + 4 - k % 4) % 4
        piece = P_.at[wave(v, ls), ls, pl.ds((4 * core + xs) * SUB, SUB), :]
        if v == 0 and k < 4 and core is c:
            piece = P_.at[wave(v, l), l, slot, :]
            return remote(piece, piece, dsend, drecv.at[v, 0], at(y, z, ((x + k) % 4) * 2 + 1 - c))
        return remote(piece, piece, dsend, drecv.at[v, k // 4], partner)

    def arrived(n, sem):
        landed(P_.at[0, 0, pl.ds(0, n * SUB), :], sem)

    def send_own(v):
        for k in range(1, 4):
            patch_copy(v, k).start()
        for k in range(4 if v == 0 else 1):
            partner_copy(v, k, c).start()

    send_own(0)
    for v in range(4):
        patch_copy(v, 4).start()

    loads[3].wait()
    bsrc[...] = jnp.broadcast_to(ibt[pl.ds(rid[0], 1), :], bsrc.shape)
    bias_to = 4 * l + x

    def bias_copies(act):
        for a in range(2):
            is_self = jnp.logical_and(l == a, w == bias_to)

            @pl.when(is_self)
            def _():
                if act == "start":
                    pltpu.make_async_copy(bsrc, bb.at[c], brecv.at[c]).start()

            @pl.when(jnp.logical_not(is_self))
            def _():
                copy = remote(bsrc, bb.at[c], bsend.at[a], brecv.at[c], at(y, 2 * h + a, bias_to))
                copy.start() if act == "start" else copy.wait_send()

    bias_copies("start")

    def pass_on(v):
        arrived(1, precv.at[v, 1])
        for k in range(5, 8):
            patch_copy(v, k).start()
        partner_copy(v, 4, c).start()

    def share(v, plane):
        arrived(3, precv.at[v, 2 * plane])
        for k in range(4 * plane + 1, 4 * plane + 4):
            if v > 0 or plane > 0:
                partner_copy(v, k, c).start()

    def complete(v, plane):
        arrived(4, drecv.at[v, plane])

    for n in (0, 1, 2, 4):
        loads[n].wait()
    gain = gt[pl.ds(rid[0], 1), :]

    def my_half(ref):
        v = ref[...].reshape(1, 2 * FB)
        return jnp.where(l == 0, v[:, :FB], v[:, FB:])

    embed_bias = my_half(be)
    gains16 = jnp.broadcast_to(gain, (16, FB))
    gains_hi = gains16.astype(BF16)
    gains_lo = (gains16 - gains_hi.astype(F32)).astype(BF16)
    product = jnp.dot(gains_hi, IT[...], preferred_element_type=F32)
    product = product + jnp.dot(gains_lo, IT[...], preferred_element_type=F32)
    qown[...] = product[0:1, :]

    def q_copy(k):
        return remote(qown, qall.at[k], qsend, qrecv, at(y, (z + k) % 8, w))

    for k in range(1, 8):
        q_copy(k).start()
    lane = lax.broadcasted_iota(jnp.int32, (TB, 128), 1)

    def stat_copy(k):
        t = (z + k) % 8
        return remote(st.at[t], stall.at[k], ssend, srecv, at(y, t, w))

    def first_product(k):
        t = (z + k) % 8
        e = jnp.dot(P_[t // 2, t % 2], We[...], preferred_element_type=F32) + embed_bias
        E[t] = e
        m = jnp.sum(e, axis=1, keepdims=True) / FB
        s2 = jnp.sum(e * e, axis=1, keepdims=True)
        n = ((e - m) * gain).astype(BF16)
        PP[t] = jnp.dot(n, IT[...], preferred_element_type=F32).astype(BF16)
        st[t] = jnp.where(lane == 0, m, jnp.where(lane == 1, s2, 0.0)).T[0:8, :]
        if not isinstance(k, int) or k > 0:
            stat_copy(k).start()

    def towards(d, k):
        return (z + 8 + (1 - 2 * d) * k) % 8


    def lanes_of(u):
        return pl.ds(u * HU, HU)

    def rows_of(u):
        return pl.ds(u * (TB // 2), TB // 2)

    def chunk(q):
        return pl.ds(q * CHUNK, CHUNK)

    def reduce_copy(d, s, q):
        src = PP.at[towards(d, 5 - s), chunk(q), :]
        return remote(src, rf.at[d, s - 1, chunk(q), :], rsend, rrecv.at[d, s - 1, q], at(y, towards(d, 1), w))

    def reduce_step(s):
        for q in range(CHUNKS):
            for d in range(2):
                if s > 2 or q * 2 // CHUNKS == d:
                    landed(rf.at[d, s - 2, chunk(q), :], rrecv.at[d, s - 2, q])
                    to = (towards(d, 5 - s), chunk(q), slice(None))
                    PP[to] = (PP[to].astype(F32) + rf[d, s - 2, chunk(q), :].astype(F32)).astype(BF16)
                reduce_copy(d, s, q).start()

    def two_products(low, high):
        def one(n, _):
            first_product(low + n * (high - low))
            return 0

        lax.fori_loop(0, 2, one, 0)

    pass_on(0)
    pass_on(1)
    send_own(1)
    send_own(2)
    share(0, 0)
    complete(0, 0)
    first_product(4)
    for q in range(CHUNKS // 2):
        for d in range(2):
            reduce_copy(d, 1, d * CHUNKS // 2 + q).start()
    pass_on(2)
    pass_on(3)
    send_own(3)

    loads[8].wait()
    quarter = pl.ds(pl.multiple_of(y * QUARTER, 64), QUARTER)
    to_l, to_x = x // 2, 2 * (x % 2) + c

    def tile_copies(act):
        for a in range(2):
            for u in range(2):
                rows = pl.ds(pl.multiple_of(u * HU + y * QUARTER, 64), QUARTER)
                src = IT.at[quarter, lanes_of(u)] if a == 0 else OT.at[rows, :]
                is_self = jnp.logical_and(to_x == x, c == u)
                dev = at(y, z, 2 * to_x + u)
                for stays in (True, False):
                    if stays:
                        dst, n = (new_in.at[l, quarter, :] if a == 0 else new_out.at[quarter, half]), 0
                    else:
                        dst, n = (XI if a == 0 else XO), 1
                    here = (to_l == l) if stays else (to_l != l)

                    @pl.when(jnp.logical_and(here, is_self))
                    def _():
                        if act == "start":
                            pltpu.make_async_copy(src, dst, xrecv.at[a, n]).start()

                    @pl.when(jnp.logical_and(here, jnp.logical_not(is_self)))
                    def _():
                        copy = remote(src, dst, xsend.at[a, u], xrecv.at[a, n], dev)
                        copy.start() if act == "start" else copy.wait_send()

    share(0, 1)
    complete(0, 1)
    first_product(5 - 2 * l)
    share(1, 1)
    complete(1, 1)
    first_product(3 + 2 * l)
    share(1, 0)
    share(2, 0)
    reduce_step(2)
    complete(1, 0)
    complete(2, 0)
    two_products(2, 6)
    share(2, 1)
    share(3, 0)
    share(3, 1)
    tile_copies("start")
    reduce_step(3)
    complete(2, 1)
    complete(3, 0)
    complete(3, 1)
    two_products(1, 7)

    pieces = ((0, 0, 0, QUARTER), (1, 0, 0, QUARTER), (0, 1, 0, QUARTER), (1, 1, 0, QUARTER // 2), (1, 1, QUARTER // 2, QUARTER // 2))

    def piece_ref(i, plane, owner, skip, n):
        rows = pl.ds(pl.multiple_of(owner * QUARTER + pieces[i][2] + skip, 16), n)
        if pieces[i][0] == 0:
            return new_in.at[plane, rows, :]
        return new_out.at[rows, pl.ds(pl.multiple_of(plane * FB, 128), FB)]

    def cross_copy(i):
        n = pieces[i][3]
        src = (XI, XO)[pieces[i][0]].at[pl.ds(pieces[i][2], n), :]
        return remote(src, piece_ref(i, l, y, 0, n), zsend.at[i - 2], zrecv.at[i - 2], at(y, 2 * h + 1 - l, w))

    def spread_copy(d, i, stage):
        owner = y if stage == 0 else (y + 3 if d == 0 else y + 1) % REPS
        n = pieces[i][3] if stage == 0 else pieces[i][3] // 2
        ref = piece_ref(i, 1 - l if pieces[i][1] else l, owner, 0 if stage == 0 else d * n, n)
        to = (y + 1 if d == 0 else y + 3) % REPS
        return remote(ref, ref, gsend.at[d], grecv.at[d, i] if stage == 0 else gend, (to, h, col))

    def spread(i):
        if pieces[i][1]:
            cross_copy(i).wait_recv()
        else:
            landed(piece_ref(i, l, y, 0, QUARTER), xrecv.at[pieces[i][0], 0])
        for d in range(2):
            spread_copy(d, i, 0).start()

    def spread_on(i):
        for d in range(2):
            spread_copy(d, i, 0).wait_recv()
            spread_copy(d, i, 1).start()

    reduce_step(4)
    landed(XI, xrecv.at[0, 1])
    cross_copy(2).start()
    first_product(0)
    spread(0)
    spread(1)
    landed(stall.at[pl.ds(1, 7)], srecv)
    landed(qall.at[pl.ds(1, 7)], qrecv)

    def columns_of(tiles):
        mean = functools.reduce(jnp.add, [t[0:1] for t in tiles]) / ZS
        square = functools.reduce(jnp.add, [t[1:2] for t in tiles]) / D
        scale = lax.rsqrt(square - mean * mean + EPSILON)
        rows = [t[0:1] - mean for t in tiles] + [scale, jnp.zeros((128 - ZS - 1, 128), F32)]
        return jnp.concatenate(rows, axis=0).T

    cols = columns_of([st[z]] + [stall[k] for k in range(1, 8)])
    v = PP[z].astype(F32) + cols[:, 0:1] * qown[...]
    for k in range(1, 8):
        v = v + cols[:, k:k + 1] * qall[k]
    C[...] = v
    for u in range(2):
        landed(bb.at[u], brecv.at[u])
    in_bias = jnp.concatenate([bb[0, 0:1, :], bb[1, 0:1, :]], axis=1)

    outward, inward = 1 - l, l

    def gather_copy(d, s, q):
        ref = H.at[towards(1 - d, s - 1), chunk(q), :]
        return remote(ref, ref, asend, arecv.at[d, s - 1, q], at(y, towards(d, 1), w))

    for q in range(CHUNKS):
        rows = slice(q * CHUNK, (q + 1) * CHUNK)
        for d in range(2):
            reduce_copy(d, 4, q).wait_recv()
        v = C[rows, :] + rf[0, 3, rows, :].astype(F32) + rf[1, 3, rows, :].astype(F32)
        v = v * cols[rows, ZS:ZS + 1] + in_bias
        H[z, rows, :] = (0.5 * v * (1.0 + lax.erf(v * 0.7071067811865476))).astype(BF16)
        for d in range(2):
            gather_copy(d, 1, q).start()

    def second_product(t, u):
        Yb[t, rows_of(u), :] = jnp.dot(H[t, rows_of(u), :], OT[...], preferred_element_type=F32).astype(BF16)
        for k in range(4):
            to = (x + k) % 4
            copy = remote(
                Yb.at[t, pl.ds(pl.multiple_of((4 * u + to) * SUB, SUB), SUB), :], R.at[(2 * k + u - c + 8) % 8 - 1, t],
                ysend, yrecv, at(y, z, 2 * to + u),
            )
            if k > 0:
                copy.start()
            else:
                pl.when(c != u)(copy.start)

    for u in range(2):
        second_product(z, u)
    for s in range(2, 5):
        for u in range(2):
            for q in range(u * CHUNKS // 2, (u + 1) * CHUNKS // 2):
                for d in range(2):
                    landed(H.at[towards(1 - d, s - 1), chunk(q), :], arecv.at[d, s - 2, q])
                    if s < 4:
                        gather_copy(d, s, q).start()
                if s == 4:
                    gather_copy(outward, s, q).start()

            def pair(d, _):
                second_product((z + 8 + (2 * d - 1) * (s - 1)) % 8, u)
                return 0

            lax.fori_loop(0, 2, pair, 0)
        if s == 2:
            spread(2)
            spread_on(0)
            spread_on(1)
        if s == 3:
            landed(XO, xrecv.at[1, 1])
            cross_copy(3).start()
            cross_copy(4).start()
        if s == 4:
            spread_on(2)

    for n in (5, 6, 7):
        loads[n].wait()
    final_gain = my_half(fg)
    out_bias = obt[pl.ds(rid[0], 1), :]
    weights = Wc[...]
    gain_w = jnp.sum(
        jnp.broadcast_to(final_gain, (128, FB)).T[:, 0:1] * weights.astype(F32), axis=0, keepdims=True
    )
    for u in range(2):
        for q in range(u * CHUNKS // 2, (u + 1) * CHUNKS // 2):
            landed(H.at[(z + 4) % 8, chunk(q), :], arecv.at[inward, 3, q])
        second_product((z + 4) % 8, u)
        spread(3 + u)

    landed(R, yrecv)
    spread_on(3)
    row = lax.broadcasted_iota(jnp.int32, (8, 128), 0)
    columns = []
    for a in range(2):
        parts = []
        for b in range(4):
            t = 2 * b + a
            u = E[t, slot, :] + out_bias + Yb[t, slot, :].astype(F32)
            for k in range(7):
                u = u + R[k, t].astype(F32)
            parts.append(u)
        u = jnp.concatenate(parts, axis=0)
        m = jnp.sum(u, axis=1, keepdims=True) / FB
        s2 = jnp.sum(u * u, axis=1, keepdims=True)
        v = (u - m) * final_gain
        hi = v.astype(BF16)
        lo = (v - hi.astype(F32)).astype(BF16)
        part = jnp.dot(hi, weights, preferred_element_type=F32) + jnp.dot(lo, weights, preferred_element_type=F32)
        LB[a] = part.astype(BF16)
        columns.append(jnp.where(lane[0:64] == 0, m, jnp.where(lane[0:64] == 1, s2, 0.0)))
    turned = jnp.concatenate(columns, axis=0).T[0:8, :]
    T[...] = jnp.where(row == 2, gain_w, turned)

    def last_copies(k):
        dev = at(y, (z + k) % 8, w)
        return (
            remote(LB.at[(z + k) % 2], LR.at[k - 1], fsend.at[0], frecv.at[0], dev),
            remote(T, TR.at[k - 1], fsend.at[1], frecv.at[1], dev),
        )

    for k in range(1, 8):
        for copy in last_copies(k):
            copy.start()
    spread_on(4)
    landed(LR, frecv.at[0])
    landed(TR, frecv.at[1])
    tiles = [T[...]] + [TR[k] for k in range(7)]
    E[0, :, 0:128] = columns_of(tiles)
    cols = E[0, pl.ds(pl.multiple_of(l * 64, 64), 64), 0:128]
    v = LB[l].astype(F32) + cols[:, 0:1] * tiles[0][2:3]
    for k in range(7):
        v = v + LR[k].astype(F32) + cols[:, k + 1:k + 2] * tiles[k + 1][2:3]
    logits[...] = v * cols[:, ZS:ZS + 1]

    landed(OT.at[pl.ds(0, 2 * FB // 2), :], gend)
    for d in range(2):
        landed(OT.at[pl.ds(0, HB * 3 // 4), :], gsend.at[d])
    for i in range(2, 5):
        cross_copy(i).wait_send()
    tile_copies("wait")
    bias_copies("wait")
    landed(P_.at[:, 0, pl.ds(0, 7 * SUB), :], psend)
    landed(P_.at[:, 0], dsend)
    landed(stall.at[pl.ds(1, 7)], ssend)
    landed(qall.at[pl.ds(1, 7)], qsend)
    landed(LR, fsend.at[0])
    landed(TR, fsend.at[1])
    landed(PP.at[pl.ds(0, 7)], rsend)
    landed(H.at[pl.ds(0, 7)], asend)
    landed(R, ysend)


def write_out(new_in, new_out, logits, in_w, out_w, check, sem):
    copies = [pltpu.make_async_copy(logits, check, sem.at[4])]
    for n, (src, dst) in enumerate(((new_in, in_w), (new_out, out_w))):
        rows = src.shape[0] // 2
        for half in range(2):
            part = pl.ds(half * rows, rows)
            copies.append(pltpu.make_async_copy(src.at[part, :], dst.at[part, :], sem.at[2 * n + half]))
    for copy in copies:
        copy.start()
    for copy in copies:
        copy.wait()


def on_device(
    patches, embed_weight, embed_bias, old_in, old_out, restore_id, norm_gains, in_biases, out_biases,
    final_gain, check_weight,
):
    def pinned(a):
        return pltpu.with_memory_space_constraint(a, pltpu.HBM)

    hbm = pl.BlockSpec(memory_space=pltpu.HBM)
    vmem = pl.BlockSpec(memory_space=pltpu.VMEM)
    dma = pltpu.SemaphoreType.DMA
    new_in, new_out, logits = pl.pallas_call(
        kernel,
        name="relayout_forward",
        out_shape=(
            jax.ShapeDtypeStruct((2, FB, HU), BF16),
            jax.ShapeDtypeStruct((HU, 2 * FB), BF16),
            jax.ShapeDtypeStruct((64, CHECK), F32),
        ),
        in_specs=[hbm] * 5 + [pl.BlockSpec(memory_space=pltpu.SMEM)] + [hbm] * 5,
        out_specs=(vmem, vmem, vmem),
        scratch_shapes=[
            pltpu.VMEM((4, 2, TB, PATCH), BF16),
            pltpu.VMEM((PATCH, FB), BF16),
            pltpu.VMEM((2 * FB,), F32),
            pltpu.VMEM((FB, HB), BF16),
            pltpu.VMEM((HB, FB), BF16),
            pltpu.VMEM((LAYERS, FB), F32),
            pltpu.VMEM((LAYERS, HU), F32),
            pltpu.VMEM((LAYERS, FB), F32),
            pltpu.VMEM((2 * FB,), F32),
            pltpu.VMEM((FB, CHECK), BF16),
            pltpu.VMEM((ZS, TB, FB), F32),
            pltpu.VMEM((ZS, 8, 128), F32),
            pltpu.VMEM((ZS, 8, 128), F32),
            pltpu.VMEM((1, HB), F32),
            pltpu.VMEM((ZS, 1, HB), F32),
            pltpu.VMEM((8, HU), F32),
            pltpu.VMEM((2, 8, HU), F32),
            pltpu.VMEM((ZS, TB, HB), BF16),
            pltpu.VMEM((2, 4, TB, HB), BF16),
            pltpu.VMEM((TB, HB), F32),
            pltpu.VMEM((ZS, TB, HB), BF16),
            pltpu.VMEM((ZS, TB, FB), BF16),
            pltpu.VMEM((7, ZS, SUB, FB), BF16),
            pltpu.VMEM((2, 64, 128), BF16),
            pltpu.VMEM((7, 64, 128), BF16),
            pltpu.VMEM((8, 128), F32),
            pltpu.VMEM((7, 8, 128), F32),
            pltpu.VMEM((QUARTER, HU), BF16),
            pltpu.VMEM((QUARTER, FB), BF16),
            dma((10,)), dma, dma((4, 3)), dma, dma((4, 2)),
            dma, dma, dma, dma, dma((2,)), dma((2,)), dma((2,)), dma((2,)),
            dma, dma((2, 4, CHUNKS)), dma, dma((2, 4, CHUNKS)),
            dma, dma,
            dma((2, 2)), dma((2, 2)), dma((3,)), dma((3,)), dma((2,)), dma((2, 5)), dma,
        ],
        compiler_params=pltpu.CompilerParams(
            collective_id=0, has_side_effects=True, vmem_limit_bytes=36 * 2**20
        ),
    )(
        *map(pinned, (patches.reshape(4, SUB, PATCH), embed_weight, embed_bias, old_in, old_out)), restore_id, *map(pinned, (
        norm_gains, in_biases, out_biases, final_gain, check_weight,
    )))
    return pl.pallas_call(
        write_out,
        name="write_out",
        out_shape=(
            jax.ShapeDtypeStruct((2 * FB, HU), BF16),
            jax.ShapeDtypeStruct((HU, 2 * FB), BF16),
            jax.ShapeDtypeStruct((64, CHECK), F32),
        ),
        in_specs=[vmem] * 3,
        out_specs=(hbm, hbm, hbm),
        scratch_shapes=[dma((5,))],
        compiler_params=pltpu.CompilerParams(vmem_limit_bytes=2**20),
    )(new_in.reshape(2 * FB, HU), new_out, logits)


def solution(mesh):
    placed = (
        P(("rep", "col"), None),
        P(None, "row"),
        P("row"),
        P(("row", "col"), None, None),
        P(("row", "col"), None, None),
        P(),
        P(None, "row"),
        P(None, "col"),
        P(None, "row"),
        P("row"),
        P("row", None),
    )
    return jax.shard_map(
        on_device,
        mesh=mesh,
        in_specs=placed,
        out_specs=(P("row", "col"), P("col", "row"), P(("rep", "col"), None)),
        check_vma=False,
    )
```

```python
import functools

import jax
import jax.numpy as jnp
from jax import lax
from jax.experimental import pallas as pl
from jax.experimental.pallas import tpu as pltpu
from jax.sharding import PartitionSpec as P

EPSILON = 1e-06
MESH = pl.DeviceIdType.MESH
F32, BF16 = jnp.float32, jnp.bfloat16

REPS, ROWS, COLS = 4, 4, 16
ZS, WS = 8, 8
D, FF, PATCH, CHECK = 6144, 12288, 588, 128
LAYERS = 48
FB = D // ZS
HB = FF // WS
HU = HB // 2
TB = 128
SUB = TB // WS
QUARTER = FB // REPS
CHUNKS = 4
CHUNK = TB // CHUNKS


def kernel(
    patches, embed_w, embed_b, old_in, old_out, rid, gains, in_b, out_b, final_g, check_w,
    new_in, new_out, logits,
    P_, We, be, IT, OT, gt, ibt, obt, fg, Wc,
    E, st, stall, qown, qall, bsrc, bb, PP, rf, C, H, Yb, R, LB, LR, T, TR, XI, XO,
    lsem, psend, precv, dsend, drecv, ssend, srecv, qsend, qrecv, fsend, frecv, bsend, brecv,
    rsend, rrecv, asend, ysend, yrecv, xsend, xrecv, zsend, zrecv, gsend, grecv, gend,
):
    y, h, col = lax.axis_index("rep"), lax.axis_index("row"), lax.axis_index("col")
    l, w = col // 8, col % 8
    x, c = w // 2, w % 2
    z = 2 * h + l
    slot = pl.ds(pl.multiple_of((4 * c + x) * SUB, SUB), SUB)

    def at(yy, zz, ww):
        return (yy, zz // 2, (zz % 2) * 8 + ww)

    def remote(src, dst, ss, rs, dev):
        return pltpu.make_async_remote_copy(
            src_ref=src, dst_ref=dst, send_sem=ss, recv_sem=rs, device_id=dev, device_id_type=MESH
        )

    def landed(ref, sem):
        pltpu.make_async_copy(ref, ref, sem).wait()

    half = pl.ds(pl.multiple_of(l * FB, 128), FB)
    loads = [
        pltpu.make_async_copy(src, dst, lsem.at[n])
        for n, (src, dst) in enumerate([
            (embed_w.at[:, half], We),
            (embed_b, be),
            (gains.at[:, half], gt),
            (in_b, ibt),
            (old_in.at[0], IT),
            (out_b.at[:, half], obt),
            (final_g, fg),
            (check_w.at[pl.ds(pl.multiple_of(l * FB, 128), FB), :], Wc),
            (old_out.at[0], OT),
        ])
    ]
    own = pltpu.make_async_copy(patches, P_.at[:, l, slot, :], lsem.at[9])
    own.start()

    barrier = pltpu.get_barrier_semaphore()
    peers = [at(y, 2 * h + (l + a) % 2, (w + b) % 8) for a in range(2) for b in range(8) if a or b]
    peers += [at(y, (z + 2 * k) % 8, w) for k in range(1, 4)]
    peers += [at(y, 2 * ((h + k) % 4) + (1 - l), w) for k in range(1, 4)]
    peers += [((y + 1) % REPS, h, col), ((y + 3) % REPS, h, col)]
    for peer in peers:
        pl.semaphore_signal(barrier, inc=1, device_id=peer, device_id_type=MESH)
    own.wait()
    for load in loads:
        load.start()
    pl.semaphore_wait(barrier, len(peers))

    partner = at(y, z, 2 * x + 1 - c)

    def wave(v, plane):
        return (h + 2 + (v % 2) * (1 - 2 * plane)) % 4 if v < 2 else (h + (1 + 2 * plane if v == 2 else 0)) % 4

    def patch_copy(v, k):
        plane = l if k < 5 else 1 - l
        place = P_.at[wave(v, plane), plane, slot, :]
        dev = at(y, 2 * h + 1 - l, w) if k == 4 else at(y, z, ((x + k % 4) % 4) * 2 + c)
        return remote(place, place, psend, precv.at[v, 0 if k < 4 else 1 if k == 4 else 2], dev)

    def partner_copy(v, k, core):
        ls, xs = (l + k // 4) % 2, (x + 4 - k % 4) % 4
        piece = P_.at[wave(v, ls), ls, pl.ds((4 * core + xs) * SUB, SUB), :]
        if v == 0 and k < 4 and core is c:
            piece = P_.at[wave(v, l), l, slot, :]
            return remote(piece, piece, dsend, drecv.at[v, 0], at(y, z, ((x + k) % 4) * 2 + 1 - c))
        return remote(piece, piece, dsend, drecv.at[v, k // 4], partner)

    def arrived(n, sem):
        landed(P_.at[0, 0, pl.ds(0, n * SUB), :], sem)

    def send_own(v):
        for k in range(1, 4):
            patch_copy(v, k).start()
        for k in range(4 if v == 0 else 1):
            partner_copy(v, k, c).start()

    def pass_on(v):
        arrived(1, precv.at[v, 1])
        for k in range(5, 8):
            patch_copy(v, k).start()
        partner_copy(v, 4, c).start()

    send_own(0)
    for v in range(4):
        patch_copy(v, 4).start()

    pass_on(0)
    pass_on(1)
    send_own(1)
    send_own(2)

    loads[3].wait()
    bsrc[...] = jnp.broadcast_to(ibt[pl.ds(rid[0], 1), :], bsrc.shape)
    bias_to = 4 * l + x

    def bias_copies(act):
        for a in range(2):
            is_self = jnp.logical_and(l == a, w == bias_to)

            @pl.when(is_self)
            def _():
                if act == "start":
                    pltpu.make_async_copy(bsrc, bb.at[c], brecv.at[c]).start()

            @pl.when(jnp.logical_not(is_self))
            def _():
                copy = remote(bsrc, bb.at[c], bsend.at[a], brecv.at[c], at(y, 2 * h + a, bias_to))
                copy.start() if act == "start" else copy.wait_send()

    bias_copies("start")

    def share(v, plane):
        arrived(3, precv.at[v, 2 * plane])
        for k in range(4 * plane + 1, 4 * plane + 4):
            if v > 0 or plane > 0:
                partner_copy(v, k, c).start()

    def complete(v, plane):
        arrived(4, drecv.at[v, plane])

    for n in (0, 1, 2, 4):
        loads[n].wait()
    gain = gt[pl.ds(rid[0], 1), :]

    def my_half(ref):
        v = ref[...].reshape(1, 2 * FB)
        return jnp.where(l == 0, v[:, :FB], v[:, FB:])

    embed_bias = my_half(be)
    gains16 = jnp.broadcast_to(gain, (16, FB))
    gains_hi = gains16.astype(BF16)
    gains_lo = (gains16 - gains_hi.astype(F32)).astype(BF16)
    product = jnp.dot(gains_hi, IT[...], preferred_element_type=F32)
    product = product + jnp.dot(gains_lo, IT[...], preferred_element_type=F32)
    qown[...] = product[0:1, :]

    def q_copy(k):
        return remote(qown, qall.at[k], qsend, qrecv, at(y, (z + k) % 8, w))

    for k in range(1, 8):
        q_copy(k).start()
    lane = lax.broadcasted_iota(jnp.int32, (TB, 128), 1)

    def stat_copy(k):
        t = (z + k) % 8
        return remote(st.at[t], stall.at[k], ssend, srecv, at(y, t, w))

    def first_product(k):
        t = (z + k) % 8
        e = jnp.dot(P_[t // 2, t % 2], We[...], preferred_element_type=F32) + embed_bias
        E[t] = e
        m = jnp.sum(e, axis=1, keepdims=True) / FB
        s2 = jnp.sum(e * e, axis=1, keepdims=True)
        n = ((e - m) * gain).astype(BF16)
        PP[t] = jnp.dot(n, IT[...], preferred_element_type=F32).astype(BF16)
        st[t] = jnp.where(lane == 0, m, jnp.where(lane == 1, s2, 0.0)).T[0:8, :]
        if not isinstance(k, int) or k > 0:
            stat_copy(k).start()

    def towards(d, k):
        return (z + 8 + (1 - 2 * d) * k) % 8


    def lanes_of(u):
        return pl.ds(u * HU, HU)

    def rows_of(u):
        return pl.ds(u * (TB // 2), TB // 2)

    def chunk(q):
        return pl.ds(q * CHUNK, CHUNK)

    def reduce_copy(d, s, q):
        src = PP.at[towards(d, 5 - s), chunk(q), :]
        return remote(src, rf.at[d, s - 1, chunk(q), :], rsend, rrecv.at[d, s - 1, q], at(y, towards(d, 1), w))

    def reduce_step(s):
        for q in range(CHUNKS):
            for d in range(2):
                if s > 2 or q * 2 // CHUNKS == d:
                    landed(rf.at[d, s - 2, chunk(q), :], rrecv.at[d, s - 2, q])
                    to = (towards(d, 5 - s), chunk(q), slice(None))
                    PP[to] = (PP[to].astype(F32) + rf[d, s - 2, chunk(q), :].astype(F32)).astype(BF16)
                reduce_copy(d, s, q).start()

    def two_products(low, high):
        def one(n, _):
            first_product(low + n * (high - low))
            return 0

        lax.fori_loop(0, 2, one, 0)

    share(0, 0)
    complete(0, 0)
    first_product(4)
    for q in range(CHUNKS // 2):
        for d in range(2):
            reduce_copy(d, 1, d * CHUNKS // 2 + q).start()
    pass_on(2)
    pass_on(3)
    send_own(3)

    loads[8].wait()
    quarter = pl.ds(pl.multiple_of(y * QUARTER, 64), QUARTER)
    to_l, to_x = x // 2, 2 * (x % 2) + c

    def tile_copies(act):
        for a in range(2):
            for u in range(2):
                rows = pl.ds(pl.multiple_of(u * HU + y * QUARTER, 64), QUARTER)
                src = IT.at[quarter, lanes_of(u)] if a == 0 else OT.at[rows, :]
                is_self = jnp.logical_and(to_x == x, c == u)
                dev = at(y, z, 2 * to_x + u)
                for stays in (True, False):
                    if stays:
                        dst, n = (new_in.at[l, quarter, :] if a == 0 else new_out.at[quarter, half]), 0
                    else:
                        dst, n = (XI if a == 0 else XO), 1
                    here = (to_l == l) if stays else (to_l != l)

                    @pl.when(jnp.logical_and(here, is_self))
                    def _():
                        if act == "start":
                            pltpu.make_async_copy(src, dst, xrecv.at[a, n]).start()

                    @pl.when(jnp.logical_and(here, jnp.logical_not(is_self)))
                    def _():
                        copy = remote(src, dst, xsend.at[a, u], xrecv.at[a, n], dev)
                        copy.start() if act == "start" else copy.wait_send()

    share(0, 1)
    complete(0, 1)
    first_product(5 - 2 * l)
    share(1, 1)
    complete(1, 1)
    first_product(3 + 2 * l)
    share(1, 0)
    share(2, 0)
    reduce_step(2)
    complete(1, 0)
    complete(2, 0)
    two_products(2, 6)
    share(2, 1)
    share(3, 0)
    share(3, 1)
    tile_copies("start")
    reduce_step(3)
    complete(2, 1)
    complete(3, 0)
    complete(3, 1)
    two_products(1, 7)

    pieces = ((0, 0, 0, QUARTER), (1, 0, 0, QUARTER), (0, 1, 0, QUARTER), (1, 1, 0, QUARTER // 2), (1, 1, QUARTER // 2, QUARTER // 2))

    def piece_ref(i, plane, owner, skip, n):
        rows = pl.ds(pl.multiple_of(owner * QUARTER + pieces[i][2] + skip, 16), n)
        if pieces[i][0] == 0:
            return new_in.at[plane, rows, :]
        return new_out.at[rows, pl.ds(pl.multiple_of(plane * FB, 128), FB)]

    def cross_copy(i):
        n = pieces[i][3]
        src = (XI, XO)[pieces[i][0]].at[pl.ds(pieces[i][2], n), :]
        return remote(src, piece_ref(i, l, y, 0, n), zsend.at[i - 2], zrecv.at[i - 2], at(y, 2 * h + 1 - l, w))

    def spread_copy(d, i, stage):
        owner = y if stage == 0 else (y + 3 if d == 0 else y + 1) % REPS
        n = pieces[i][3] if stage == 0 else pieces[i][3] // 2
        ref = piece_ref(i, 1 - l if pieces[i][1] else l, owner, 0 if stage == 0 else d * n, n)
        to = (y + 1 if d == 0 else y + 3) % REPS
        return remote(ref, ref, gsend.at[d], grecv.at[d, i] if stage == 0 else gend, (to, h, col))

    def spread(i):
        if pieces[i][1]:
            cross_copy(i).wait_recv()
        else:
            landed(piece_ref(i, l, y, 0, QUARTER), xrecv.at[pieces[i][0], 0])
        for d in range(2):
            spread_copy(d, i, 0).start()

    def spread_on(i):
        for d in range(2):
            spread_copy(d, i, 0).wait_recv()
            spread_copy(d, i, 1).start()

    reduce_step(4)
    landed(XI, xrecv.at[0, 1])
    cross_copy(2).start()
    first_product(0)
    spread(0)
    spread(1)
    landed(stall.at[pl.ds(1, 7)], srecv)
    landed(qall.at[pl.ds(1, 7)], qrecv)

    def columns_of(tiles):
        mean = functools.reduce(jnp.add, [t[0:1] for t in tiles]) / ZS
        square = functools.reduce(jnp.add, [t[1:2] for t in tiles]) / D
        scale = lax.rsqrt(square - mean * mean + EPSILON)
        rows = [t[0:1] - mean for t in tiles] + [scale, jnp.zeros((128 - ZS - 1, 128), F32)]
        return jnp.concatenate(rows, axis=0).T

    cols = columns_of([st[z]] + [stall[k] for k in range(1, 8)])
    v = PP[z].astype(F32) + cols[:, 0:1] * qown[...]
    for k in range(1, 8):
        v = v + cols[:, k:k + 1] * qall[k]
    C[...] = v
    for u in range(2):
        landed(bb.at[u], brecv.at[u])
    in_bias = jnp.concatenate([bb[0, 0:1, :], bb[1, 0:1, :]], axis=1)

    outward, inward = 1 - l, l

    def gather_copy(d, s, q):
        ref = H.at[towards(1 - d, s - 1), chunk(q), :]
        return remote(ref, ref, asend, rrecv.at[d, s - 1, q], at(y, towards(d, 1), w))

    for q in range(CHUNKS):
        rows = slice(q * CHUNK, (q + 1) * CHUNK)
        for d in range(2):
            reduce_copy(d, 4, q).wait_recv()
        v = C[rows, :] + rf[0, 3, rows, :].astype(F32) + rf[1, 3, rows, :].astype(F32)
        v = v * cols[rows, ZS:ZS + 1] + in_bias
        H[z, rows, :] = (0.5 * v * (1.0 + lax.erf(v * 0.7071067811865476))).astype(BF16)
        for d in range(2):
            gather_copy(d, 1, q).start()

    def second_product(t, u):
        Yb[t, rows_of(u), :] = jnp.dot(H[t, rows_of(u), :], OT[...], preferred_element_type=F32).astype(BF16)
        for k in range(4):
            to = (x + k) % 4
            copy = remote(
                Yb.at[t, pl.ds(pl.multiple_of((4 * u + to) * SUB, SUB), SUB), :], R.at[(2 * k + u - c + 8) % 8 - 1, t],
                ysend, yrecv, at(y, z, 2 * to + u),
            )
            if k > 0:
                copy.start()
            else:
                pl.when(c != u)(copy.start)

    for u in range(2):
        second_product(z, u)
    for s in range(2, 5):
        for u in range(2):
            for q in range(u * CHUNKS // 2, (u + 1) * CHUNKS // 2):
                for d in range(2):
                    landed(H.at[towards(1 - d, s - 1), chunk(q), :], rrecv.at[d, s - 2, q])
                    if s < 4:
                        gather_copy(d, s, q).start()
                if s == 4:
                    gather_copy(outward, s, q).start()

            def pair(d, _):
                second_product((z + 8 + (2 * d - 1) * (s - 1)) % 8, u)
                return 0

            lax.fori_loop(0, 2, pair, 0)
        if s == 2:
            spread(2)
            spread_on(0)
            spread_on(1)
        if s == 3:
            landed(XO, xrecv.at[1, 1])
            cross_copy(3).start()
            cross_copy(4).start()
            spread_on(2)

    for n in (5, 6, 7):
        loads[n].wait()
    final_gain = my_half(fg)
    out_bias = obt[pl.ds(rid[0], 1), :]
    weights = Wc[...]
    gain_w = jnp.sum(
        jnp.broadcast_to(final_gain, (128, FB)).T[:, 0:1] * weights.astype(F32), axis=0, keepdims=True
    )
    for u in range(2):
        for q in range(u * CHUNKS // 2, (u + 1) * CHUNKS // 2):
            landed(H.at[(z + 4) % 8, chunk(q), :], rrecv.at[inward, 3, q])
        second_product((z + 4) % 8, u)
        spread(3 + u)

    landed(R, yrecv)
    spread_on(3)
    row = lax.broadcasted_iota(jnp.int32, (8, 128), 0)
    columns = []
    for a in range(2):
        parts = []
        for b in range(4):
            t = 2 * b + a
            u = E[t, slot, :] + out_bias + Yb[t, slot, :].astype(F32)
            for k in range(7):
                u = u + R[k, t].astype(F32)
            parts.append(u)
        u = jnp.concatenate(parts, axis=0)
        m = jnp.sum(u, axis=1, keepdims=True) / FB
        s2 = jnp.sum(u * u, axis=1, keepdims=True)
        v = (u - m) * final_gain
        hi = v.astype(BF16)
        lo = (v - hi.astype(F32)).astype(BF16)
        part = jnp.dot(hi, weights, preferred_element_type=F32) + jnp.dot(lo, weights, preferred_element_type=F32)
        LB[a] = part.astype(BF16)
        columns.append(jnp.where(lane[0:64] == 0, m, jnp.where(lane[0:64] == 1, s2, 0.0)))
    turned = jnp.concatenate(columns, axis=0).T[0:8, :]
    T[...] = jnp.where(row == 2, gain_w, turned)

    def last_copies(k):
        dev = at(y, (z + k) % 8, w)
        return (
            remote(LB.at[(z + k) % 2], LR.at[k - 1], fsend.at[0], frecv.at[0], dev),
            remote(T, TR.at[k - 1], fsend.at[1], frecv.at[1], dev),
        )

    for k in range(1, 8):
        for copy in last_copies(k):
            copy.start()
    spread_on(4)
    landed(LR, frecv.at[0])
    landed(TR, frecv.at[1])
    tiles = [T[...]] + [TR[k] for k in range(7)]
    E[0, :, 0:128] = columns_of(tiles)
    cols = E[0, pl.ds(pl.multiple_of(l * 64, 64), 64), 0:128]
    v = LB[l].astype(F32) + cols[:, 0:1] * tiles[0][2:3]
    for k in range(7):
        v = v + LR[k].astype(F32) + cols[:, k + 1:k + 2] * tiles[k + 1][2:3]
    logits[...] = v * cols[:, ZS:ZS + 1]

    landed(OT.at[pl.ds(0, 2 * FB // 2), :], gend)
    for d in range(2):
        landed(OT.at[pl.ds(0, HB * 3 // 4), :], gsend.at[d])
    for i in range(2, 5):
        cross_copy(i).wait_send()
    tile_copies("wait")
    bias_copies("wait")
    landed(P_.at[:, 0, pl.ds(0, 7 * SUB), :], psend)
    landed(P_.at[:, 0], dsend)
    landed(stall.at[pl.ds(1, 7)], ssend)
    landed(qall.at[pl.ds(1, 7)], qsend)
    landed(LR, fsend.at[0])
    landed(TR, fsend.at[1])
    landed(PP.at[pl.ds(0, 7)], rsend)
    landed(H.at[pl.ds(0, 7)], asend)
    landed(R, ysend)


def write_out(new_in, new_out, logits, in_w, out_w, check, sem):
    copies = [pltpu.make_async_copy(logits, check, sem.at[4])]
    for n, (src, dst) in enumerate(((new_in, in_w), (new_out, out_w))):
        rows = src.shape[0] // 2
        for half in range(2):
            part = pl.ds(half * rows, rows)
            copies.append(pltpu.make_async_copy(src.at[part, :], dst.at[part, :], sem.at[2 * n + half]))
    for copy in copies:
        copy.start()
    for copy in copies:
        copy.wait()


def on_device(
    patches, embed_weight, embed_bias, old_in, old_out, restore_id, norm_gains, in_biases, out_biases,
    final_gain, check_weight,
):
    def pinned(a):
        return pltpu.with_memory_space_constraint(a, pltpu.HBM)

    hbm = pl.BlockSpec(memory_space=pltpu.HBM)
    vmem = pl.BlockSpec(memory_space=pltpu.VMEM)
    dma = pltpu.SemaphoreType.DMA
    new_in, new_out, logits = pl.pallas_call(
        kernel,
        name="relayout_forward",
        out_shape=(
            jax.ShapeDtypeStruct((2, FB, HU), BF16),
            jax.ShapeDtypeStruct((HU, 2 * FB), BF16),
            jax.ShapeDtypeStruct((64, CHECK), F32),
        ),
        in_specs=[hbm] * 5 + [pl.BlockSpec(memory_space=pltpu.SMEM)] + [hbm] * 5,
        out_specs=(vmem, vmem, vmem),
        scratch_shapes=[
            pltpu.VMEM((4, 2, TB, PATCH), BF16),
            pltpu.VMEM((PATCH, FB), BF16),
            pltpu.VMEM((2 * FB,), F32),
            pltpu.VMEM((FB, HB), BF16),
            pltpu.VMEM((HB, FB), BF16),
            pltpu.VMEM((LAYERS, FB), F32),
            pltpu.VMEM((LAYERS, HU), F32),
            pltpu.VMEM((LAYERS, FB), F32),
            pltpu.VMEM((2 * FB,), F32),
            pltpu.VMEM((FB, CHECK), BF16),
            pltpu.VMEM((ZS, TB, FB), F32),
            pltpu.VMEM((ZS, 8, 128), F32),
            pltpu.VMEM((ZS, 8, 128), F32),
            pltpu.VMEM((1, HB), F32),
            pltpu.VMEM((ZS, 1, HB), F32),
            pltpu.VMEM((8, HU), F32),
            pltpu.VMEM((2, 8, HU), F32),
            pltpu.VMEM((ZS, TB, HB), BF16),
            pltpu.VMEM((2, 4, TB, HB), BF16),
            pltpu.VMEM((TB, HB), F32),
            pltpu.VMEM((ZS, TB, HB), BF16),
            pltpu.VMEM((ZS, TB, FB), BF16),
            pltpu.VMEM((7, ZS, SUB, FB), BF16),
            pltpu.VMEM((2, 64, 128), BF16),
            pltpu.VMEM((7, 64, 128), BF16),
            pltpu.VMEM((8, 128), F32),
            pltpu.VMEM((7, 8, 128), F32),
            pltpu.VMEM((QUARTER, HU), BF16),
            pltpu.VMEM((QUARTER, FB), BF16),
            dma((10,)), dma, dma((4, 3)), dma, dma((4, 2)),
            dma, dma, dma, dma, dma((2,)), dma((2,)), dma((2,)), dma((2,)),
            dma, dma((2, 4, CHUNKS)), dma,
            dma, dma,
            dma((2, 2)), dma((2, 2)), dma((3,)), dma((3,)), dma((2,)), dma((2, 5)), dma,
        ],
        compiler_params=pltpu.CompilerParams(
            collective_id=0, has_side_effects=True, vmem_limit_bytes=36 * 2**20
        ),
    )(
        *map(pinned, (patches.reshape(4, SUB, PATCH), embed_weight, embed_bias, old_in, old_out)), restore_id, *map(pinned, (
        norm_gains, in_biases, out_biases, final_gain, check_weight,
    )))
    return pl.pallas_call(
        write_out,
        name="write_out",
        out_shape=(
            jax.ShapeDtypeStruct((2 * FB, HU), BF16),
            jax.ShapeDtypeStruct((HU, 2 * FB), BF16),
            jax.ShapeDtypeStruct((64, CHECK), F32),
        ),
        in_specs=[vmem] * 3,
        out_specs=(hbm, hbm, hbm),
        scratch_shapes=[dma((5,))],
        compiler_params=pltpu.CompilerParams(vmem_limit_bytes=2**20),
    )(new_in.reshape(2 * FB, HU), new_out, logits)


def solution(mesh):
    placed = (
        P(("rep", "col"), None),
        P(None, "row"),
        P("row"),
        P(("row", "col"), None, None),
        P(("row", "col"), None, None),
        P(),
        P(None, "row"),
        P(None, "col"),
        P(None, "row"),
        P("row"),
        P("row", None),
    )
    return jax.shard_map(
        on_device,
        mesh=mesh,
        in_specs=placed,
        out_specs=(P("row", "col"), P("col", "row"), P(("rep", "col"), None)),
        check_vma=False,
    )
```

```python
import functools

import jax
import jax.numpy as jnp
from jax import lax
from jax.experimental import pallas as pl
from jax.experimental.pallas import tpu as pltpu
from jax.sharding import PartitionSpec as P

EPSILON = 1e-06
MESH = pl.DeviceIdType.MESH
F32, BF16 = jnp.float32, jnp.bfloat16

REPS, ROWS, COLS = 4, 4, 16
ZS, WS = 8, 8
D, FF, PATCH, CHECK = 6144, 12288, 588, 128
LAYERS = 48
FB = D // ZS
HB = FF // WS
HU = HB // 2
TB = 128
SUB = TB // WS
QUARTER = FB // REPS
CHUNKS = 4
CHUNK = TB // CHUNKS


def kernel(
    patches, embed_w, embed_b, old_in, old_out, rid, gains, in_b, out_b, final_g, check_w,
    new_in, new_out, logits,
    P_, We, be, IT, OT, gt, ibt, obt, fg, Wc,
    E, st, stall, qown, qall, bsrc, bb, PP, rf, C, H, Yb, R, LB, LR, T, TR, XI, XO,
    lsem, psend, precv, dsend, drecv, ssend, srecv, qsend, qrecv, fsend, frecv, bsend, brecv,
    rsend, rrecv, asend, ysend, yrecv, xsend, xrecv, zsend, zrecv, gsend, grecv, gend,
):
    y, h, col = lax.axis_index("rep"), lax.axis_index("row"), lax.axis_index("col")
    l, w = col // 8, col % 8
    x, c = w // 2, w % 2
    z = 2 * h + l
    slot = pl.ds(pl.multiple_of((4 * c + x) * SUB, SUB), SUB)

    def at(yy, zz, ww):
        return (yy, zz // 2, (zz % 2) * 8 + ww)

    def remote(src, dst, ss, rs, dev):
        return pltpu.make_async_remote_copy(
            src_ref=src, dst_ref=dst, send_sem=ss, recv_sem=rs, device_id=dev, device_id_type=MESH
        )

    def landed(ref, sem):
        pltpu.make_async_copy(ref, ref, sem).wait()

    half = pl.ds(pl.multiple_of(l * FB, 128), FB)
    loads = [
        pltpu.make_async_copy(src, dst, lsem.at[n])
        for n, (src, dst) in enumerate([
            (embed_w.at[:, half], We),
            (embed_b, be),
            (gains.at[:, half], gt),
            (in_b, ibt),
            (old_in.at[0], IT),
            (out_b.at[:, half], obt),
            (final_g, fg),
            (check_w.at[pl.ds(pl.multiple_of(l * FB, 128), FB), :], Wc),
            (old_out.at[0], OT),
        ])
    ]
    own = pltpu.make_async_copy(patches, P_.at[:, l, slot, :], lsem.at[9])
    own.start()

    barrier = pltpu.get_barrier_semaphore()
    peers = [at(y, 2 * h + (l + a) % 2, (w + b) % 8) for a in range(2) for b in range(8) if a or b]
    peers += [at(y, (z + 2 * k) % 8, w) for k in range(1, 4)]
    peers += [at(y, 2 * ((h + k) % 4) + (1 - l), w) for k in range(1, 4)]
    peers += [((y + 1) % REPS, h, col), ((y + 3) % REPS, h, col)]
    for peer in peers:
        pl.semaphore_signal(barrier, inc=1, device_id=peer, device_id_type=MESH)
    own.wait()
    for load in loads:
        load.start()
    pl.semaphore_wait(barrier, len(peers))

    partner = at(y, z, 2 * x + 1 - c)

    def wave(v, plane):
        return (h + 2 + (v % 2) * (1 - 2 * plane)) % 4 if v < 2 else (h + (1 + 2 * plane if v == 2 else 0)) % 4

    def patch_copy(v, k):
        plane = l if k < 5 else 1 - l
        place = P_.at[wave(v, plane), plane, slot, :]
        dev = at(y, 2 * h + 1 - l, w) if k == 4 else at(y, z, ((x + k % 4) % 4) * 2 + c)
        return remote(place, place, psend, precv.at[v, 0 if k < 4 else 1 if k == 4 else 2], dev)

    def partner_copy(v, k, core):
        ls, xs = (l + k // 4) % 2, (x + 4 - k % 4) % 4
        piece = P_.at[wave(v, ls), ls, pl.ds((4 * core + xs) * SUB, SUB), :]
        if v == 0 and k < 4 and core is c:
            piece = P_.at[wave(v, l), l, slot, :]
            return remote(piece, piece, dsend, drecv.at[v, 0], at(y, z, ((x + k) % 4) * 2 + 1 - c))
        return remote(piece, piece, dsend, drecv.at[v, k // 4], partner)

    def arrived(n, sem):
        landed(P_.at[0, 0, pl.ds(0, n * SUB), :], sem)

    def send_own(v):
        for k in range(1, 4):
            patch_copy(v, k).start()
        for k in range(4 if v == 0 else 1):
            partner_copy(v, k, c).start()

    def pass_on(v):
        arrived(1, precv.at[v, 1])
        for k in range(5, 8):
            patch_copy(v, k).start()
        partner_copy(v, 4, c).start()

    send_own(0)
    for v in range(4):
        patch_copy(v, 4).start()

    pass_on(0)
    pass_on(1)
    send_own(1)
    send_own(2)

    loads[3].wait()
    bsrc[...] = jnp.broadcast_to(ibt[pl.ds(rid[0], 1), :], bsrc.shape)
    bias_to = 4 * l + x

    def bias_copies(act):
        for a in range(2):
            is_self = jnp.logical_and(l == a, w == bias_to)

            @pl.when(is_self)
            def _():
                if act == "start":
                    pltpu.make_async_copy(bsrc, bb.at[c], brecv.at[c]).start()

            @pl.when(jnp.logical_not(is_self))
            def _():
                copy = remote(bsrc, bb.at[c], bsend.at[a], brecv.at[c], at(y, 2 * h + a, bias_to))
                copy.start() if act == "start" else copy.wait_send()

    bias_copies("start")

    def share(v, plane):
        arrived(3, precv.at[v, 2 * plane])
        for k in range(4 * plane + 1, 4 * plane + 4):
            if v > 0 or plane > 0:
                partner_copy(v, k, c).start()

    def complete(v, plane):
        arrived(4, drecv.at[v, plane])

    for n in (0, 1, 2, 4):
        loads[n].wait()
    gain = gt[pl.ds(rid[0], 1), :]

    def my_half(ref):
        v = ref[...].reshape(1, 2 * FB)
        return jnp.where(l == 0, v[:, :FB], v[:, FB:])

    embed_bias = my_half(be)
    gains16 = jnp.broadcast_to(gain, (16, FB))
    gains_hi = gains16.astype(BF16)
    gains_lo = (gains16 - gains_hi.astype(F32)).astype(BF16)
    product = jnp.dot(gains_hi, IT[...], preferred_element_type=F32)
    product = product + jnp.dot(gains_lo, IT[...], preferred_element_type=F32)
    qown[...] = product[0:1, :]

    def q_copy(k):
        return remote(qown, qall.at[k], qsend, qrecv, at(y, (z + k) % 8, w))

    for k in range(1, 8):
        q_copy(k).start()
    lane = lax.broadcasted_iota(jnp.int32, (TB, 128), 1)

    def stat_copy(k):
        t = (z + k) % 8
        return remote(st.at[t], stall.at[k], ssend, srecv, at(y, t, w))

    def first_product(k):
        t = (z + k) % 8
        e = jnp.dot(P_[t // 2, t % 2], We[...], preferred_element_type=F32) + embed_bias
        E[t] = e
        m = jnp.sum(e, axis=1, keepdims=True) / FB
        s2 = jnp.sum(e * e, axis=1, keepdims=True)
        n = ((e - m) * gain).astype(BF16)
        PP[t] = jnp.dot(n, IT[...], preferred_element_type=F32).astype(BF16)
        st[t] = jnp.where(lane == 0, m, jnp.where(lane == 1, s2, 0.0)).T[0:8, :]
        if not isinstance(k, int) or k > 0:
            stat_copy(k).start()

    def towards(d, k):
        return (z + 8 + (1 - 2 * d) * k) % 8


    def lanes_of(u):
        return pl.ds(u * HU, HU)

    def rows_of(u):
        return pl.ds(u * (TB // 2), TB // 2)

    def chunk(q):
        return pl.ds(q * CHUNK, CHUNK)

    def reduce_copy(d, s, q):
        src = PP.at[towards(d, 5 - s), chunk(q), :]
        return remote(src, rf.at[d, s - 1, chunk(q), :], rsend, rrecv.at[d, s - 1, q], at(y, towards(d, 1), w))

    def reduce_step(s):
        for q in range(CHUNKS):
            for d in range(2):
                if s > 2 or q * 2 // CHUNKS == d:
                    landed(rf.at[d, s - 2, chunk(q), :], rrecv.at[d, s - 2, q])
                    to = (towards(d, 5 - s), chunk(q), slice(None))
                    PP[to] = (PP[to].astype(F32) + rf[d, s - 2, chunk(q), :].astype(F32)).astype(BF16)
                reduce_copy(d, s, q).start()

    def two_products(low, high):
        def one(n, _):
            first_product(low + n * (high - low))
            return 0

        lax.fori_loop(0, 2, one, 0)

    share(0, 0)
    complete(0, 0)
    first_product(4)
    for q in range(CHUNKS // 2):
        for d in range(2):
            reduce_copy(d, 1, d * CHUNKS // 2 + q).start()
    pass_on(2)
    pass_on(3)
    send_own(3)

    loads[8].wait()
    quarter = pl.ds(pl.multiple_of(y * QUARTER, 64), QUARTER)
    to_l, to_x = x // 2, 2 * (x % 2) + c

    def tile_copies(act):
        for a in range(2):
            for u in range(2):
                rows = pl.ds(pl.multiple_of(u * HU + y * QUARTER, 64), QUARTER)
                src = IT.at[quarter, lanes_of(u)] if a == 0 else OT.at[rows, :]
                is_self = jnp.logical_and(to_x == x, c == u)
                dev = at(y, z, 2 * to_x + u)
                for stays in (True, False):
                    if stays:
                        dst, n = (new_in.at[l, quarter, :] if a == 0 else new_out.at[quarter, half]), 0
                    else:
                        dst, n = (XI if a == 0 else XO), 1
                    here = (to_l == l) if stays else (to_l != l)

                    @pl.when(jnp.logical_and(here, is_self))
                    def _():
                        if act == "start":
                            pltpu.make_async_copy(src, dst, xrecv.at[a, n]).start()

                    @pl.when(jnp.logical_and(here, jnp.logical_not(is_self)))
                    def _():
                        copy = remote(src, dst, xsend.at[a, u], xrecv.at[a, n], dev)
                        copy.start() if act == "start" else copy.wait_send()

    share(0, 1)
    share(1, 1)
    complete(0, 1)
    first_product(5 - 2 * l)
    complete(1, 1)
    first_product(3 + 2 * l)
    share(1, 0)
    share(2, 0)
    reduce_step(2)
    complete(1, 0)
    complete(2, 0)
    two_products(2, 6)
    share(2, 1)
    share(3, 0)
    share(3, 1)
    tile_copies("start")
    reduce_step(3)
    complete(2, 1)
    complete(3, 0)
    complete(3, 1)
    two_products(1, 7)

    pieces = ((0, 0, 0, QUARTER), (1, 0, 0, QUARTER), (0, 1, 0, QUARTER), (1, 1, 0, QUARTER // 2), (1, 1, QUARTER // 2, QUARTER // 2))

    def piece_ref(i, plane, owner, skip, n):
        rows = pl.ds(pl.multiple_of(owner * QUARTER + pieces[i][2] + skip, 16), n)
        if pieces[i][0] == 0:
            return new_in.at[plane, rows, :]
        return new_out.at[rows, pl.ds(pl.multiple_of(plane * FB, 128), FB)]

    def cross_copy(i):
        n = pieces[i][3]
        src = (XI, XO)[pieces[i][0]].at[pl.ds(pieces[i][2], n), :]
        return remote(src, piece_ref(i, l, y, 0, n), zsend.at[i - 2], zrecv.at[i - 2], at(y, 2 * h + 1 - l, w))

    def spread_copy(d, i, stage):
        owner = y if stage == 0 else (y + 3 if d == 0 else y + 1) % REPS
        n = pieces[i][3] if stage == 0 else pieces[i][3] // 2
        ref = piece_ref(i, 1 - l if pieces[i][1] else l, owner, 0 if stage == 0 else d * n, n)
        to = (y + 1 if d == 0 else y + 3) % REPS
        return remote(ref, ref, gsend.at[d], grecv.at[d, i] if stage == 0 else gend, (to, h, col))

    def spread(i):
        if pieces[i][1]:
            cross_copy(i).wait_recv()
        else:
            landed(piece_ref(i, l, y, 0, QUARTER), xrecv.at[pieces[i][0], 0])
        for d in range(2):
            spread_copy(d, i, 0).start()

    def spread_on(i):
        for d in range(2):
            spread_copy(d, i, 0).wait_recv()
            spread_copy(d, i, 1).start()

    reduce_step(4)
    landed(XI, xrecv.at[0, 1])
    cross_copy(2).start()
    first_product(0)
    spread(0)
    spread(1)
    landed(stall.at[pl.ds(1, 7)], srecv)
    landed(qall.at[pl.ds(1, 7)], qrecv)

    def columns_of(tiles):
        mean = functools.reduce(jnp.add, [t[0:1] for t in tiles]) / ZS
        square = functools.reduce(jnp.add, [t[1:2] for t in tiles]) / D
        scale = lax.rsqrt(square - mean * mean + EPSILON)
        rows = [t[0:1] - mean for t in tiles] + [scale, jnp.zeros((128 - ZS - 1, 128), F32)]
        return jnp.concatenate(rows, axis=0).T

    cols = columns_of([st[z]] + [stall[k] for k in range(1, 8)])
    v = PP[z].astype(F32) + cols[:, 0:1] * qown[...]
    for k in range(1, 8):
        v = v + cols[:, k:k + 1] * qall[k]
    C[...] = v
    for u in range(2):
        landed(bb.at[u], brecv.at[u])
    in_bias = jnp.concatenate([bb[0, 0:1, :], bb[1, 0:1, :]], axis=1)

    outward, inward = 1 - l, l

    def gather_copy(d, s, q):
        ref = H.at[towards(1 - d, s - 1), chunk(q), :]
        return remote(ref, ref, asend, rrecv.at[d, s - 1, q], at(y, towards(d, 1), w))

    for q in range(CHUNKS):
        rows = slice(q * CHUNK, (q + 1) * CHUNK)
        for d in range(2):
            reduce_copy(d, 4, q).wait_recv()
        v = C[rows, :] + rf[0, 3, rows, :].astype(F32) + rf[1, 3, rows, :].astype(F32)
        v = v * cols[rows, ZS:ZS + 1] + in_bias
        H[z, rows, :] = (0.5 * v * (1.0 + lax.erf(v * 0.7071067811865476))).astype(BF16)
        for d in range(2):
            gather_copy(d, 1, q).start()

    def second_product(t, u):
        Yb[t, rows_of(u), :] = jnp.dot(H[t, rows_of(u), :], OT[...], preferred_element_type=F32).astype(BF16)
        for k in range(4):
            to = (x + k) % 4
            copy = remote(
                Yb.at[t, pl.ds(pl.multiple_of((4 * u + to) * SUB, SUB), SUB), :], R.at[(2 * k + u - c + 8) % 8 - 1, t],
                ysend, yrecv, at(y, z, 2 * to + u),
            )
            if k > 0:
                copy.start()
            else:
                pl.when(c != u)(copy.start)

    for u in range(2):
        second_product(z, u)
    for s in range(2, 5):
        for u in range(2):
            for q in range(u * CHUNKS // 2, (u + 1) * CHUNKS // 2):
                for d in range(2):
                    landed(H.at[towards(1 - d, s - 1), chunk(q), :], rrecv.at[d, s - 2, q])
                    if s < 4:
                        gather_copy(d, s, q).start()
                if s == 4:
                    gather_copy(outward, s, q).start()

            def pair(d, _):
                second_product((z + 8 + (2 * d - 1) * (s - 1)) % 8, u)
                return 0

            lax.fori_loop(0, 2, pair, 0)
        if s == 2:
            spread(2)
            spread_on(0)
            spread_on(1)
        if s == 3:
            landed(XO, xrecv.at[1, 1])
            cross_copy(3).start()
            cross_copy(4).start()
            spread_on(2)

    for n in (5, 6, 7):
        loads[n].wait()
    final_gain = my_half(fg)
    out_bias = obt[pl.ds(rid[0], 1), :]
    weights = Wc[...]
    gain_w = jnp.sum(
        jnp.broadcast_to(final_gain, (128, FB)).T[:, 0:1] * weights.astype(F32), axis=0, keepdims=True
    )
    for u in range(2):
        for q in range(u * CHUNKS // 2, (u + 1) * CHUNKS // 2):
            landed(H.at[(z + 4) % 8, chunk(q), :], rrecv.at[inward, 3, q])
        second_product((z + 4) % 8, u)
        spread(3 + u)

    landed(R, yrecv)
    spread_on(3)
    row = lax.broadcasted_iota(jnp.int32, (8, 128), 0)
    columns = []
    for a in range(2):
        parts = []
        for b in range(4):
            t = 2 * b + a
            u = E[t, slot, :] + out_bias + Yb[t, slot, :].astype(F32)
            for k in range(7):
                u = u + R[k, t].astype(F32)
            parts.append(u)
        u = jnp.concatenate(parts, axis=0)
        m = jnp.sum(u, axis=1, keepdims=True) / FB
        s2 = jnp.sum(u * u, axis=1, keepdims=True)
        v = (u - m) * final_gain
        hi = v.astype(BF16)
        lo = (v - hi.astype(F32)).astype(BF16)
        part = jnp.dot(hi, weights, preferred_element_type=F32) + jnp.dot(lo, weights, preferred_element_type=F32)
        LB[a] = part.astype(BF16)
        columns.append(jnp.where(lane[0:64] == 0, m, jnp.where(lane[0:64] == 1, s2, 0.0)))
    turned = jnp.concatenate(columns, axis=0).T[0:8, :]
    T[...] = jnp.where(row == 2, gain_w, turned)

    def last_copies(k):
        dev = at(y, (z + k) % 8, w)
        return (
            remote(LB.at[(z + k) % 2], LR.at[k - 1], fsend.at[0], frecv.at[0], dev),
            remote(T, TR.at[k - 1], fsend.at[1], frecv.at[1], dev),
        )

    for k in range(1, 8):
        for copy in last_copies(k):
            copy.start()
    spread_on(4)
    landed(LR, frecv.at[0])
    landed(TR, frecv.at[1])
    tiles = [T[...]] + [TR[k] for k in range(7)]
    E[0, :, 0:128] = columns_of(tiles)
    cols = E[0, pl.ds(pl.multiple_of(l * 64, 64), 64), 0:128]
    v = LB[l].astype(F32) + cols[:, 0:1] * tiles[0][2:3]
    for k in range(7):
        v = v + LR[k].astype(F32) + cols[:, k + 1:k + 2] * tiles[k + 1][2:3]
    logits[...] = v * cols[:, ZS:ZS + 1]

    landed(OT.at[pl.ds(0, 2 * FB // 2), :], gend)
    for d in range(2):
        landed(OT.at[pl.ds(0, HB * 3 // 4), :], gsend.at[d])
    for i in range(2, 5):
        cross_copy(i).wait_send()
    tile_copies("wait")
    bias_copies("wait")
    landed(P_.at[:, 0, pl.ds(0, 7 * SUB), :], psend)
    landed(P_.at[:, 0], dsend)
    landed(stall.at[pl.ds(1, 7)], ssend)
    landed(qall.at[pl.ds(1, 7)], qsend)
    landed(LR, fsend.at[0])
    landed(TR, fsend.at[1])
    landed(PP.at[pl.ds(0, 7)], rsend)
    landed(H.at[pl.ds(0, 7)], asend)
    landed(R, ysend)


def write_out(new_in, new_out, logits, in_w, out_w, check, sem):
    copies = [pltpu.make_async_copy(logits, check, sem.at[4])]
    for n, (src, dst) in enumerate(((new_in, in_w), (new_out, out_w))):
        rows = src.shape[0] // 2
        for half in range(2):
            part = pl.ds(half * rows, rows)
            copies.append(pltpu.make_async_copy(src.at[part, :], dst.at[part, :], sem.at[2 * n + half]))
    for copy in copies:
        copy.start()
    for copy in copies:
        copy.wait()


def on_device(
    patches, embed_weight, embed_bias, old_in, old_out, restore_id, norm_gains, in_biases, out_biases,
    final_gain, check_weight,
):
    def pinned(a):
        return pltpu.with_memory_space_constraint(a, pltpu.HBM)

    hbm = pl.BlockSpec(memory_space=pltpu.HBM)
    vmem = pl.BlockSpec(memory_space=pltpu.VMEM)
    dma = pltpu.SemaphoreType.DMA
    new_in, new_out, logits = pl.pallas_call(
        kernel,
        name="relayout_forward",
        out_shape=(
            jax.ShapeDtypeStruct((2, FB, HU), BF16),
            jax.ShapeDtypeStruct((HU, 2 * FB), BF16),
            jax.ShapeDtypeStruct((64, CHECK), F32),
        ),
        in_specs=[hbm] * 5 + [pl.BlockSpec(memory_space=pltpu.SMEM)] + [hbm] * 5,
        out_specs=(vmem, vmem, vmem),
        scratch_shapes=[
            pltpu.VMEM((4, 2, TB, PATCH), BF16),
            pltpu.VMEM((PATCH, FB), BF16),
            pltpu.VMEM((2 * FB,), F32),
            pltpu.VMEM((FB, HB), BF16),
            pltpu.VMEM((HB, FB), BF16),
            pltpu.VMEM((LAYERS, FB), F32),
            pltpu.VMEM((LAYERS, HU), F32),
            pltpu.VMEM((LAYERS, FB), F32),
            pltpu.VMEM((2 * FB,), F32),
            pltpu.VMEM((FB, CHECK), BF16),
            pltpu.VMEM((ZS, TB, FB), F32),
            pltpu.VMEM((ZS, 8, 128), F32),
            pltpu.VMEM((ZS, 8, 128), F32),
            pltpu.VMEM((1, HB), F32),
            pltpu.VMEM((ZS, 1, HB), F32),
            pltpu.VMEM((8, HU), F32),
            pltpu.VMEM((2, 8, HU), F32),
            pltpu.VMEM((ZS, TB, HB), BF16),
            pltpu.VMEM((2, 4, TB, HB), BF16),
            pltpu.VMEM((TB, HB), F32),
            pltpu.VMEM((ZS, TB, HB), BF16),
            pltpu.VMEM((ZS, TB, FB), BF16),
            pltpu.VMEM((7, ZS, SUB, FB), BF16),
            pltpu.VMEM((2, 64, 128), BF16),
            pltpu.VMEM((7, 64, 128), BF16),
            pltpu.VMEM((8, 128), F32),
            pltpu.VMEM((7, 8, 128), F32),
            pltpu.VMEM((QUARTER, HU), BF16),
            pltpu.VMEM((QUARTER, FB), BF16),
            dma((10,)), dma, dma((4, 3)), dma, dma((4, 2)),
            dma, dma, dma, dma, dma((2,)), dma((2,)), dma((2,)), dma((2,)),
            dma, dma((2, 4, CHUNKS)), dma,
            dma, dma,
            dma((2, 2)), dma((2, 2)), dma((3,)), dma((3,)), dma((2,)), dma((2, 5)), dma,
        ],
        compiler_params=pltpu.CompilerParams(
            collective_id=0, has_side_effects=True, vmem_limit_bytes=36 * 2**20
        ),
    )(
        *map(pinned, (patches.reshape(4, SUB, PATCH), embed_weight, embed_bias, old_in, old_out)), restore_id, *map(pinned, (
        norm_gains, in_biases, out_biases, final_gain, check_weight,
    )))
    return pl.pallas_call(
        write_out,
        name="write_out",
        out_shape=(
            jax.ShapeDtypeStruct((2 * FB, HU), BF16),
            jax.ShapeDtypeStruct((HU, 2 * FB), BF16),
            jax.ShapeDtypeStruct((64, CHECK), F32),
        ),
        in_specs=[vmem] * 3,
        out_specs=(hbm, hbm, hbm),
        scratch_shapes=[dma((5,))],
        compiler_params=pltpu.CompilerParams(vmem_limit_bytes=2**20),
    )(new_in.reshape(2 * FB, HU), new_out, logits)


def solution(mesh):
    placed = (
        P(("rep", "col"), None),
        P(None, "row"),
        P("row"),
        P(("row", "col"), None, None),
        P(("row", "col"), None, None),
        P(),
        P(None, "row"),
        P(None, "col"),
        P(None, "row"),
        P("row"),
        P("row", None),
    )
    return jax.shard_map(
        on_device,
        mesh=mesh,
        in_specs=placed,
        out_specs=(P("row", "col"), P("col", "row"), P(("rep", "col"), None)),
        check_vma=False,
    )
```

```python
import functools

import jax
import jax.numpy as jnp
from jax import lax
from jax.experimental import pallas as pl
from jax.experimental.pallas import tpu as pltpu
from jax.sharding import PartitionSpec as P

EPSILON = 1e-06
MESH = pl.DeviceIdType.MESH
F32, BF16 = jnp.float32, jnp.bfloat16

REPS, ROWS, COLS = 4, 4, 16
ZS, WS = 8, 8
D, FF, PATCH, CHECK = 6144, 12288, 588, 128
LAYERS = 48
FB = D // ZS
HB = FF // WS
HU = HB // 2
TB = 128
SUB = TB // WS
QUARTER = FB // REPS
CHUNKS = 4
CHUNK = TB // CHUNKS


def kernel(
    patches, embed_w, embed_b, old_in, old_out, rid, gains, in_b, out_b, final_g, check_w,
    new_in, new_out, logits,
    P_, We, be, IT, OT, gt, ibt, obt, fg, Wc,
    E, st, stall, qown, qall, bsrc, bb, PP, rf, C, H, Yb, R, LB, LR, T, TR, XI, XO,
    lsem, psend, precv, dsend, drecv, ssend, srecv, qsend, qrecv, fsend, frecv, bsend, brecv,
    rsend, rrecv, asend, ysend, yrecv, xsend, xrecv, zsend, zrecv, gsend, grecv, gend,
):
    y, h, col = lax.axis_index("rep"), lax.axis_index("row"), lax.axis_index("col")
    l, w = col // 8, col % 8
    x, c = w // 2, w % 2
    z = 2 * h + l
    slot = pl.ds(pl.multiple_of((4 * c + x) * SUB, SUB), SUB)

    def at(yy, zz, ww):
        return (yy, zz // 2, (zz % 2) * 8 + ww)

    def remote(src, dst, ss, rs, dev):
        return pltpu.make_async_remote_copy(
            src_ref=src, dst_ref=dst, send_sem=ss, recv_sem=rs, device_id=dev, device_id_type=MESH
        )

    def landed(ref, sem):
        pltpu.make_async_copy(ref, ref, sem).wait()

    half = pl.ds(pl.multiple_of(l * FB, 128), FB)
    loads = [
        pltpu.make_async_copy(src, dst, lsem.at[n])
        for n, (src, dst) in enumerate([
            (embed_w.at[:, half], We),
            (embed_b, be),
            (gains.at[:, half], gt),
            (in_b, ibt),
            (old_in.at[0], IT),
            (out_b.at[:, half], obt),
            (final_g, fg),
            (check_w.at[pl.ds(pl.multiple_of(l * FB, 128), FB), :], Wc),
            (old_out.at[0], OT),
        ])
    ]
    own = pltpu.make_async_copy(patches, P_.at[:, l, slot, :], lsem.at[9])
    own.start()

    barrier = pltpu.get_barrier_semaphore()
    peers = [at(y, 2 * h + (l + a) % 2, (w + b) % 8) for a in range(2) for b in range(8) if a or b]
    peers += [at(y, (z + 2 * k) % 8, w) for k in range(1, 4)]
    peers += [at(y, 2 * ((h + k) % 4) + (1 - l), w) for k in range(1, 4)]
    peers += [((y + 1) % REPS, h, col), ((y + 3) % REPS, h, col)]
    for peer in peers:
        pl.semaphore_signal(barrier, inc=1, device_id=peer, device_id_type=MESH)
    own.wait()
    for load in loads:
        load.start()
    pl.semaphore_wait(barrier, len(peers))

    partner = at(y, z, 2 * x + 1 - c)

    def wave(v, plane):
        return (h + 2 + (v % 2) * (1 - 2 * plane)) % 4 if v < 2 else (h + (1 + 2 * plane if v == 2 else 0)) % 4

    def patch_copy(v, k):
        plane = l if k < 5 else 1 - l
        place = P_.at[wave(v, plane), plane, slot, :]
        dev = at(y, 2 * h + 1 - l, w) if k == 4 else at(y, z, ((x + k % 4) % 4) * 2 + c)
        return remote(place, place, psend, precv.at[v, 0 if k < 4 else 1 if k == 4 else 2], dev)

    def partner_copy(v, k, core):
        ls, xs = (l + k // 4) % 2, (x + 4 - k % 4) % 4
        piece = P_.at[wave(v, ls), ls, pl.ds((4 * core + xs) * SUB, SUB), :]
        if v == 0 and k < 4 and core is c:
            piece = P_.at[wave(v, l), l, slot, :]
            return remote(piece, piece, dsend, drecv.at[v, 0], at(y, z, ((x + k) % 4) * 2 + 1 - c))
        return remote(piece, piece, dsend, drecv.at[v, k // 4], partner)

    def arrived(n, sem):
        landed(P_.at[0, 0, pl.ds(0, n * SUB), :], sem)

    def send_own(v):
        for k in range(1, 4):
            patch_copy(v, k).start()
        for k in range(4 if v == 0 else 1):
            partner_copy(v, k, c).start()

    def pass_on(v):
        arrived(1, precv.at[v, 1])
        for k in range(5, 8):
            patch_copy(v, k).start()
        partner_copy(v, 4, c).start()

    send_own(0)
    for v in range(4):
        patch_copy(v, 4).start()

    pass_on(0)
    pass_on(1)
    send_own(1)
    send_own(2)

    loads[3].wait()
    bsrc[...] = jnp.broadcast_to(ibt[pl.ds(rid[0], 1), :], bsrc.shape)
    bias_to = 4 * l + x

    def bias_copies(act):
        for a in range(2):
            is_self = jnp.logical_and(l == a, w == bias_to)

            @pl.when(is_self)
            def _():
                if act == "start":
                    pltpu.make_async_copy(bsrc, bb.at[c], brecv.at[c]).start()

            @pl.when(jnp.logical_not(is_self))
            def _():
                copy = remote(bsrc, bb.at[c], bsend.at[a], brecv.at[c], at(y, 2 * h + a, bias_to))
                copy.start() if act == "start" else copy.wait_send()

    bias_copies("start")

    def share(v, plane):
        arrived(3, precv.at[v, 2 * plane])
        for k in range(4 * plane + 1, 4 * plane + 4):
            if v > 0 or plane > 0:
                partner_copy(v, k, c).start()

    def complete(v, plane):
        arrived(4, drecv.at[v, plane])

    for n in (0, 1, 2, 4):
        loads[n].wait()
    gain = gt[pl.ds(rid[0], 1), :]

    def my_half(ref):
        v = ref[...].reshape(1, 2 * FB)
        return jnp.where(l == 0, v[:, :FB], v[:, FB:])

    embed_bias = my_half(be)
    lane = lax.broadcasted_iota(jnp.int32, (TB, 128), 1)

    def stat_copy(k):
        t = (z + k) % 8
        return remote(st.at[t], stall.at[k], ssend, srecv, at(y, t, w))

    def first_product(k):
        t = (z + k) % 8
        e = jnp.dot(P_[t // 2, t % 2], We[...], preferred_element_type=F32) + embed_bias
        E[t] = e
        m = jnp.sum(e, axis=1, keepdims=True) / FB
        s2 = jnp.sum(e * e, axis=1, keepdims=True)
        n = ((e - m) * gain).astype(BF16)
        PP[t] = jnp.dot(n, IT[...], preferred_element_type=F32).astype(BF16)
        st[t] = jnp.where(lane == 0, m, jnp.where(lane == 1, s2, 0.0)).T[0:8, :]
        if not isinstance(k, int) or k > 0:
            stat_copy(k).start()

    def towards(d, k):
        return (z + 8 + (1 - 2 * d) * k) % 8


    def lanes_of(u):
        return pl.ds(u * HU, HU)

    def rows_of(u):
        return pl.ds(u * (TB // 2), TB // 2)

    def chunk(q):
        return pl.ds(q * CHUNK, CHUNK)

    def reduce_copy(d, s, q):
        src = PP.at[towards(d, 5 - s), chunk(q), :]
        return remote(src, rf.at[d, s - 1, chunk(q), :], rsend, rrecv.at[d, s - 1, q], at(y, towards(d, 1), w))

    def reduce_step(s):
        for q in range(CHUNKS):
            for d in range(2):
                if s > 2 or q * 2 // CHUNKS == d:
                    landed(rf.at[d, s - 2, chunk(q), :], rrecv.at[d, s - 2, q])
                    to = (towards(d, 5 - s), chunk(q), slice(None))
                    PP[to] = (PP[to].astype(F32) + rf[d, s - 2, chunk(q), :].astype(F32)).astype(BF16)
                reduce_copy(d, s, q).start()

    def two_products(low, high):
        def one(n, _):
            first_product(low + n * (high - low))
            return 0

        lax.fori_loop(0, 2, one, 0)

    share(0, 0)
    complete(0, 0)
    first_product(4)
    for q in range(CHUNKS // 2):
        for d in range(2):
            reduce_copy(d, 1, d * CHUNKS // 2 + q).start()
    pass_on(2)
    pass_on(3)
    send_own(3)

    loads[8].wait()
    quarter = pl.ds(pl.multiple_of(y * QUARTER, 64), QUARTER)
    to_l, to_x = x // 2, 2 * (x % 2) + c

    def tile_copies(act):
        for a in range(2):
            for u in range(2):
                rows = pl.ds(pl.multiple_of(u * HU + y * QUARTER, 64), QUARTER)
                src = IT.at[quarter, lanes_of(u)] if a == 0 else OT.at[rows, :]
                is_self = jnp.logical_and(to_x == x, c == u)
                dev = at(y, z, 2 * to_x + u)
                for stays in (True, False):
                    if stays:
                        dst, n = (new_in.at[l, quarter, :] if a == 0 else new_out.at[quarter, half]), 0
                    else:
                        dst, n = (XI if a == 0 else XO), 1
                    here = (to_l == l) if stays else (to_l != l)

                    @pl.when(jnp.logical_and(here, is_self))
                    def _():
                        if act == "start":
                            pltpu.make_async_copy(src, dst, xrecv.at[a, n]).start()

                    @pl.when(jnp.logical_and(here, jnp.logical_not(is_self)))
                    def _():
                        copy = remote(src, dst, xsend.at[a, u], xrecv.at[a, n], dev)
                        copy.start() if act == "start" else copy.wait_send()

    gains16 = jnp.broadcast_to(gain, (16, FB))
    gains_hi = gains16.astype(BF16)
    gains_lo = (gains16 - gains_hi.astype(F32)).astype(BF16)
    product = jnp.dot(gains_hi, IT[...], preferred_element_type=F32)
    product = product + jnp.dot(gains_lo, IT[...], preferred_element_type=F32)
    qown[...] = product[0:1, :]

    def q_copy(k):
        return remote(qown, qall.at[k], qsend, qrecv, at(y, (z + k) % 8, w))

    for k in range(1, 8):
        q_copy(k).start()
    share(0, 1)
    share(1, 1)
    complete(0, 1)
    first_product(5 - 2 * l)
    complete(1, 1)
    first_product(3 + 2 * l)
    share(1, 0)
    share(2, 0)
    reduce_step(2)
    complete(1, 0)
    complete(2, 0)
    two_products(2, 6)
    share(2, 1)
    share(3, 0)
    share(3, 1)
    tile_copies("start")
    reduce_step(3)
    complete(2, 1)
    complete(3, 0)
    complete(3, 1)
    two_products(1, 7)

    pieces = ((0, 0, 0, QUARTER), (1, 0, 0, QUARTER), (0, 1, 0, QUARTER), (1, 1, 0, QUARTER // 2), (1, 1, QUARTER // 2, QUARTER // 2))

    def piece_ref(i, plane, owner, skip, n):
        rows = pl.ds(pl.multiple_of(owner * QUARTER + pieces[i][2] + skip, 16), n)
        if pieces[i][0] == 0:
            return new_in.at[plane, rows, :]
        return new_out.at[rows, pl.ds(pl.multiple_of(plane * FB, 128), FB)]

    def cross_copy(i):
        n = pieces[i][3]
        src = (XI, XO)[pieces[i][0]].at[pl.ds(pieces[i][2], n), :]
        return remote(src, piece_ref(i, l, y, 0, n), zsend.at[i - 2], zrecv.at[i - 2], at(y, 2 * h + 1 - l, w))

    def spread_copy(d, i, stage):
        owner = y if stage == 0 else (y + 3 if d == 0 else y + 1) % REPS
        n = pieces[i][3] if stage == 0 else pieces[i][3] // 2
        ref = piece_ref(i, 1 - l if pieces[i][1] else l, owner, 0 if stage == 0 else d * n, n)
        to = (y + 1 if d == 0 else y + 3) % REPS
        return remote(ref, ref, gsend.at[d], grecv.at[d, i] if stage == 0 else gend, (to, h, col))

    def spread(i):
        if pieces[i][1]:
            cross_copy(i).wait_recv()
        else:
            landed(piece_ref(i, l, y, 0, QUARTER), xrecv.at[pieces[i][0], 0])
        for d in range(2):
            spread_copy(d, i, 0).start()

    def spread_on(i):
        for d in range(2):
            spread_copy(d, i, 0).wait_recv()
            spread_copy(d, i, 1).start()

    reduce_step(4)
    landed(XI, xrecv.at[0, 1])
    cross_copy(2).start()
    first_product(0)
    spread(0)
    spread(1)
    landed(stall.at[pl.ds(1, 7)], srecv)
    landed(qall.at[pl.ds(1, 7)], qrecv)

    def columns_of(tiles):
        mean = functools.reduce(jnp.add, [t[0:1] for t in tiles]) / ZS
        square = functools.reduce(jnp.add, [t[1:2] for t in tiles]) / D
        scale = lax.rsqrt(square - mean * mean + EPSILON)
        rows = [t[0:1] - mean for t in tiles] + [scale, jnp.zeros((128 - ZS - 1, 128), F32)]
        return jnp.concatenate(rows, axis=0).T

    cols = columns_of([st[z]] + [stall[k] for k in range(1, 8)])
    v = PP[z].astype(F32) + cols[:, 0:1] * qown[...]
    for k in range(1, 8):
        v = v + cols[:, k:k + 1] * qall[k]
    C[...] = v
    for u in range(2):
        landed(bb.at[u], brecv.at[u])
    in_bias = jnp.concatenate([bb[0, 0:1, :], bb[1, 0:1, :]], axis=1)

    outward, inward = 1 - l, l

    def gather_copy(d, s, q):
        ref = H.at[towards(1 - d, s - 1), chunk(q), :]
        return remote(ref, ref, asend, rrecv.at[d, s - 1, q], at(y, towards(d, 1), w))

    for q in range(CHUNKS):
        rows = slice(q * CHUNK, (q + 1) * CHUNK)
        for d in range(2):
            reduce_copy(d, 4, q).wait_recv()
        v = C[rows, :] + rf[0, 3, rows, :].astype(F32) + rf[1, 3, rows, :].astype(F32)
        v = v * cols[rows, ZS:ZS + 1] + in_bias
        H[z, rows, :] = (0.5 * v * (1.0 + lax.erf(v * 0.7071067811865476))).astype(BF16)
        for d in range(2):
            gather_copy(d, 1, q).start()

    def second_product(t, u):
        Yb[t, rows_of(u), :] = jnp.dot(H[t, rows_of(u), :], OT[...], preferred_element_type=F32).astype(BF16)
        for k in range(4):
            to = (x + k) % 4
            copy = remote(
                Yb.at[t, pl.ds(pl.multiple_of((4 * u + to) * SUB, SUB), SUB), :], R.at[(2 * k + u - c + 8) % 8 - 1, t],
                ysend, yrecv, at(y, z, 2 * to + u),
            )
            if k > 0:
                copy.start()
            else:
                pl.when(c != u)(copy.start)

    for u in range(2):
        second_product(z, u)
    for s in range(2, 5):
        for u in range(2):
            for q in range(u * CHUNKS // 2, (u + 1) * CHUNKS // 2):
                for d in range(2):
                    landed(H.at[towards(1 - d, s - 1), chunk(q), :], rrecv.at[d, s - 2, q])
                    if s < 4:
                        gather_copy(d, s, q).start()
                if s == 4:
                    gather_copy(outward, s, q).start()

            def pair(d, _):
                second_product((z + 8 + (2 * d - 1) * (s - 1)) % 8, u)
                return 0

            lax.fori_loop(0, 2, pair, 0)
        if s == 2:
            spread(2)
            spread_on(0)
            spread_on(1)
        if s == 3:
            landed(XO, xrecv.at[1, 1])
            cross_copy(3).start()
            cross_copy(4).start()
            spread_on(2)

    for n in (5, 6, 7):
        loads[n].wait()
    final_gain = my_half(fg)
    out_bias = obt[pl.ds(rid[0], 1), :]
    weights = Wc[...]
    gain_w = jnp.sum(
        jnp.broadcast_to(final_gain, (128, FB)).T[:, 0:1] * weights.astype(F32), axis=0, keepdims=True
    )
    for u in range(2):
        for q in range(u * CHUNKS // 2, (u + 1) * CHUNKS // 2):
            landed(H.at[(z + 4) % 8, chunk(q), :], rrecv.at[inward, 3, q])
        second_product((z + 4) % 8, u)
        spread(3 + u)

    landed(R, yrecv)
    spread_on(3)
    row = lax.broadcasted_iota(jnp.int32, (8, 128), 0)
    columns = []
    for a in range(2):
        parts = []
        for b in range(4):
            t = 2 * b + a
            u = E[t, slot, :] + out_bias + Yb[t, slot, :].astype(F32)
            for k in range(7):
                u = u + R[k, t].astype(F32)
            parts.append(u)
        u = jnp.concatenate(parts, axis=0)
        m = jnp.sum(u, axis=1, keepdims=True) / FB
        s2 = jnp.sum(u * u, axis=1, keepdims=True)
        v = (u - m) * final_gain
        hi = v.astype(BF16)
        lo = (v - hi.astype(F32)).astype(BF16)
        part = jnp.dot(hi, weights, preferred_element_type=F32) + jnp.dot(lo, weights, preferred_element_type=F32)
        LB[a] = part.astype(BF16)
        columns.append(jnp.where(lane[0:64] == 0, m, jnp.where(lane[0:64] == 1, s2, 0.0)))
    turned = jnp.concatenate(columns, axis=0).T[0:8, :]
    T[...] = jnp.where(row == 2, gain_w, turned)

    def last_copies(k):
        dev = at(y, (z + k) % 8, w)
        return (
            remote(LB.at[(z + k) % 2], LR.at[k - 1], fsend.at[0], frecv.at[0], dev),
            remote(T, TR.at[k - 1], fsend.at[1], frecv.at[1], dev),
        )

    for k in range(1, 8):
        for copy in last_copies(k):
            copy.start()
    spread_on(4)
    landed(LR, frecv.at[0])
    landed(TR, frecv.at[1])
    tiles = [T[...]] + [TR[k] for k in range(7)]
    E[0, :, 0:128] = columns_of(tiles)
    cols = E[0, pl.ds(pl.multiple_of(l * 64, 64), 64), 0:128]
    v = LB[l].astype(F32) + cols[:, 0:1] * tiles[0][2:3]
    for k in range(7):
        v = v + LR[k].astype(F32) + cols[:, k + 1:k + 2] * tiles[k + 1][2:3]
    logits[...] = v * cols[:, ZS:ZS + 1]

    landed(OT.at[pl.ds(0, 2 * FB // 2), :], gend)
    for d in range(2):
        landed(OT.at[pl.ds(0, HB * 3 // 4), :], gsend.at[d])
    for i in range(2, 5):
        cross_copy(i).wait_send()
    tile_copies("wait")
    bias_copies("wait")
    landed(P_.at[:, 0, pl.ds(0, 7 * SUB), :], psend)
    landed(P_.at[:, 0], dsend)
    landed(stall.at[pl.ds(1, 7)], ssend)
    landed(qall.at[pl.ds(1, 7)], qsend)
    landed(LR, fsend.at[0])
    landed(TR, fsend.at[1])
    landed(PP.at[pl.ds(0, 7)], rsend)
    landed(H.at[pl.ds(0, 7)], asend)
    landed(R, ysend)


def write_out(new_in, new_out, logits, in_w, out_w, check, sem):
    copies = [pltpu.make_async_copy(logits, check, sem.at[4])]
    for n, (src, dst) in enumerate(((new_in, in_w), (new_out, out_w))):
        rows = src.shape[0] // 2
        for half in range(2):
            part = pl.ds(half * rows, rows)
            copies.append(pltpu.make_async_copy(src.at[part, :], dst.at[part, :], sem.at[2 * n + half]))
    for copy in copies:
        copy.start()
    for copy in copies:
        copy.wait()


def on_device(
    patches, embed_weight, embed_bias, old_in, old_out, restore_id, norm_gains, in_biases, out_biases,
    final_gain, check_weight,
):
    def pinned(a):
        return pltpu.with_memory_space_constraint(a, pltpu.HBM)

    hbm = pl.BlockSpec(memory_space=pltpu.HBM)
    vmem = pl.BlockSpec(memory_space=pltpu.VMEM)
    dma = pltpu.SemaphoreType.DMA
    new_in, new_out, logits = pl.pallas_call(
        kernel,
        name="relayout_forward",
        out_shape=(
            jax.ShapeDtypeStruct((2, FB, HU), BF16),
            jax.ShapeDtypeStruct((HU, 2 * FB), BF16),
            jax.ShapeDtypeStruct((64, CHECK), F32),
        ),
        in_specs=[hbm] * 5 + [pl.BlockSpec(memory_space=pltpu.SMEM)] + [hbm] * 5,
        out_specs=(vmem, vmem, vmem),
        scratch_shapes=[
            pltpu.VMEM((4, 2, TB, PATCH), BF16),
            pltpu.VMEM((PATCH, FB), BF16),
            pltpu.VMEM((2 * FB,), F32),
            pltpu.VMEM((FB, HB), BF16),
            pltpu.VMEM((HB, FB), BF16),
            pltpu.VMEM((LAYERS, FB), F32),
            pltpu.VMEM((LAYERS, HU), F32),
            pltpu.VMEM((LAYERS, FB), F32),
            pltpu.VMEM((2 * FB,), F32),
            pltpu.VMEM((FB, CHECK), BF16),
            pltpu.VMEM((ZS, TB, FB), F32),
            pltpu.VMEM((ZS, 8, 128), F32),
            pltpu.VMEM((ZS, 8, 128), F32),
            pltpu.VMEM((1, HB), F32),
            pltpu.VMEM((ZS, 1, HB), F32),
            pltpu.VMEM((8, HU), F32),
            pltpu.VMEM((2, 8, HU), F32),
            pltpu.VMEM((ZS, TB, HB), BF16),
            pltpu.VMEM((2, 4, TB, HB), BF16),
            pltpu.VMEM((TB, HB), F32),
            pltpu.VMEM((ZS, TB, HB), BF16),
            pltpu.VMEM((ZS, TB, FB), BF16),
            pltpu.VMEM((7, ZS, SUB, FB), BF16),
            pltpu.VMEM((2, 64, 128), BF16),
            pltpu.VMEM((7, 64, 128), BF16),
            pltpu.VMEM((8, 128), F32),
            pltpu.VMEM((7, 8, 128), F32),
            pltpu.VMEM((QUARTER, HU), BF16),
            pltpu.VMEM((QUARTER, FB), BF16),
            dma((10,)), dma, dma((4, 3)), dma, dma((4, 2)),
            dma, dma, dma, dma, dma((2,)), dma((2,)), dma((2,)), dma((2,)),
            dma, dma((2, 4, CHUNKS)), dma,
            dma, dma,
            dma((2, 2)), dma((2, 2)), dma((3,)), dma((3,)), dma((2,)), dma((2, 5)), dma,
        ],
        compiler_params=pltpu.CompilerParams(
            collective_id=0, has_side_effects=True, vmem_limit_bytes=36 * 2**20
        ),
    )(
        *map(pinned, (patches.reshape(4, SUB, PATCH), embed_weight, embed_bias, old_in, old_out)), restore_id, *map(pinned, (
        norm_gains, in_biases, out_biases, final_gain, check_weight,
    )))
    return pl.pallas_call(
        write_out,
        name="write_out",
        out_shape=(
            jax.ShapeDtypeStruct((2 * FB, HU), BF16),
            jax.ShapeDtypeStruct((HU, 2 * FB), BF16),
            jax.ShapeDtypeStruct((64, CHECK), F32),
        ),
        in_specs=[vmem] * 3,
        out_specs=(hbm, hbm, hbm),
        scratch_shapes=[dma((5,))],
        compiler_params=pltpu.CompilerParams(vmem_limit_bytes=2**20),
    )(new_in.reshape(2 * FB, HU), new_out, logits)


def solution(mesh):
    placed = (
        P(("rep", "col"), None),
        P(None, "row"),
        P("row"),
        P(("row", "col"), None, None),
        P(("row", "col"), None, None),
        P(),
        P(None, "row"),
        P(None, "col"),
        P(None, "row"),
        P("row"),
        P("row", None),
    )
    return jax.shard_map(
        on_device,
        mesh=mesh,
        in_specs=placed,
        out_specs=(P("row", "col"), P("col", "row"), P(("rep", "col"), None)),
        check_vma=False,
    )
```
